32 devices in a mesh: grp: 2 (over y), sp: 4 (over z), sub: 2 (over x), rep: 2 (over core).
Axes of the slice: x: 2, y: 2, z: 4, core: 2. Of those that a mesh axis runs over, the one named last changes fastest.
Arguments:
- field: float32 [512, 32, 32, 128], P(('grp', 'sp', 'rep'), 'sub'), parts along dimension 0, may hold values from -40 to 40, as said below
- mix_weight: float32 [256, 256], replicated, may hold values from -0.375 to 0.375
- factor_x: float32 [256, 32], replicated, may hold values from -6 to 6
- factor_y: float32 [256, 32], replicated, may hold values from -6 to 6
- factor_z: float32 [256, 32], replicated, may hold values from -6 to 6
- norm_gain: float32 [256], replicated, may hold values from 0.5 to 1.5
- norm_bias: float32 [256], replicated, may hold values from -3 to 3
- w_in: float32 [256, 256], replicated, may hold values from -0.375 to 0.375
- b_in: float32 [256], replicated, may hold values from -3 to 3
- w_out: float32 [256, 256], replicated, may hold values from -0.375 to 0.375
- b_out: float32 [256], replicated, may hold values from -3 to 3
Outputs:
- block_out: float32 [512, 32, 32, 128], P('grp', 'sub', ('sp', 'rep')), parts along dimension 0
The draws below stay inside these ranges and needn't reach their ends.
There are 2 independent parts, one for each index of `grp`. The reference program is written for one: setup_inputs(seed, part) draws one part's arguments, and reference() takes and returns one part's arrays. A program takes and returns all parts, laid end to end along the dimension named above; an argument that names none is the same for every part. Nothing has to cross between parts.
Inputs may be any that keep to these rules, and one draw needn't show every extreme that they name: `field`: real values of order one in each channel, with scales that differ between channels.
All inputs are finite; a program needn't handle non-finite values.
Results may differ from the reference program's by a relative error of at most 0.000078.
Values sent between devices are 32-bit elements; how exact they have to be, the bound alone decides.
A program may use at most 128 MiB of HBM per device.

```python
import math
import jax
import jax.numpy as jnp
from jax import lax

C = 256
HID = 256
KX = 32
KY = 32
KZ = 32
GROUPS = 32
NX = 32
NY = 32
NZ = 128


def draw_field(key, part):
    first, second = jax.random.split(key, 2)
    chan_scale = jnp.exp(jax.random.uniform(second, (C, 1, 1, 1), jnp.float32, math.log(0.3), math.log(3.0)))
    along_x = jnp.arange(NX, dtype=jnp.float32) / (NX - 1)
    along_y = jnp.arange(NY, dtype=jnp.float32) / (NY - 1)
    ramp = jnp.exp(math.log(3.0) * (along_x[:, None, None] + along_y[None, :, None]) - math.log(3.0))
    base = jnp.clip(jax.random.normal(first, (C, NX, NY, NZ), jnp.float32), -4.0, 4.0)
    return base * chan_scale * ramp[None]


def noise(own_key, shape, spread, reach, kind=jnp.bfloat16):
    drawn = jax.random.normal(own_key, shape, jnp.float32) * spread
    return jnp.minimum(jnp.maximum(drawn, -reach), reach).astype(kind)


def setup_inputs(seed: int = 0, part: int = 0) -> dict:
    splits = jax.random.split(jax.random.key(seed), 12)
    part_splits = jax.random.split(jax.random.fold_in(splits[11], part), 12)
    field = draw_field(jax.random.fold_in(jax.random.fold_in(splits[11], part), 71), part)
    mix_weight = noise(splits[1], (C, C), C ** -0.5, 0.375, jnp.float32)
    factor_x = noise(splits[2], (C, KX), 1.3, 6.0, jnp.float32)
    factor_y = noise(splits[3], (C, KY), 1.3, 6.0, jnp.float32)
    factor_z = noise(splits[4], (C, KZ), 1.3, 6.0, jnp.float32)
    norm_gain = jnp.clip(jax.random.uniform(splits[5], (C,), jnp.float32, 0.5, 1.5), 0.5, 1.5)
    norm_bias = noise(splits[6], (C,), 0.5, 3.0, jnp.float32)
    w_in = noise(splits[7], (HID, C), C ** -0.5, 0.375, jnp.float32)
    b_in = noise(splits[8], (HID,), 0.5, 3.0, jnp.float32)
    w_out = noise(splits[9], (C, HID), HID ** -0.5, 0.375, jnp.float32)
    b_out = noise(splits[10], (C,), 0.5, 3.0, jnp.float32)
    return dict(field=field, mix_weight=mix_weight, factor_x=factor_x, factor_y=factor_y, factor_z=factor_z, norm_gain=norm_gain, norm_bias=norm_bias, w_in=w_in, b_in=b_in, w_out=w_out, b_out=b_out)


def contract(formula, left, right):
    return jnp.einsum(formula, left, right, precision=lax.Precision.HIGHEST)

def tables(length, kept_count):
    indices = jnp.arange(kept_count, dtype=jnp.int32)
    kept_freq = jnp.where(indices < kept_count // 2, indices, length - kept_count + indices)
    positions = jnp.arange(length, dtype=jnp.int32)
    phases = kept_freq[:, None] * positions[None, :] % length
    angles = 2.0 * math.pi / length * phases.astype(jnp.float32)
    return (jnp.cos(angles), jnp.sin(angles))

def transform(planes, cosine, sine, formula):
    real_part = contract(formula, planes[0], cosine) + contract(formula, planes[1], sine)
    imag_part = contract(formula, planes[1], cosine) - contract(formula, planes[0], sine)
    return jnp.stack([real_part, imag_part])

def reference(field, mix_weight, factor_x, factor_y, factor_z, norm_gain, norm_bias, w_in, b_in, w_out, b_out):
    cos_x, sin_x = tables(NX, KX)
    cos_y, sin_y = tables(NY, KY)
    cos_z, sin_z = tables(NZ, KZ)
    planes = jnp.stack([contract('cxyz,kz->cxyk', field, cos_z / NZ), -contract('cxyz,kz->cxyk', field, sin_z / NZ)])
    planes = transform(planes, cos_y / NY, sin_y / NY, 'cxyk,jy->cxjk')
    spectra = transform(planes, cos_x / NX, sin_x / NX, 'cxjk,ix->cijk')
    weighting = factor_x[:, :, None, None] * factor_y[:, None, :, None] * factor_z[:, None, None, :]
    mixed_modes = jnp.einsum('oc,rcijk->roijk', mix_weight, spectra * weighting[None], precision=lax.Precision.HIGHEST)
    returned = transform(mixed_modes, cos_x, -sin_x, 'cijk,ix->cxjk')
    returned = transform(returned, cos_y, -sin_y, 'cxjk,jy->cxyk')
    spectral = contract('cxyk,kz->cxyz', returned[0], cos_z) - contract('cxyk,kz->cxyz', returned[1], sin_z)
    summed = field + spectral
    cells_group = C // GROUPS * NX * NY * NZ
    grouped = summed.reshape(GROUPS, -1)
    group_mean = lax.optimization_barrier(jnp.sum(grouped, axis=1)) / cells_group
    centered = grouped - group_mean[:, None]
    group_var = lax.optimization_barrier(jnp.sum(centered * centered, axis=1)) / cells_group
    inv_scale = jnp.repeat(lax.rsqrt(group_var + 1e-05), C // GROUPS) * norm_gain
    mean_chan = jnp.repeat(group_mean, C // GROUPS)
    columns = summed.reshape(C, -1)
    normed = (columns - mean_chan[:, None]) * inv_scale[:, None] + norm_bias[:, None]
    hidden = jax.nn.gelu(jnp.dot(w_in, normed, precision=lax.Precision.HIGHEST) + b_in[:, None])
    result = columns + jnp.dot(w_out, hidden, precision=lax.Precision.HIGHEST) + b_out[:, None]
    return result.reshape(C, NX, NY, NZ)
```

```python
import math
import functools

import jax
import jax.numpy as jnp
from jax import lax
from jax.experimental import pallas as pl
from jax.experimental.pallas import tpu as pltpu
from jax.sharding import PartitionSpec as P

GROUPS = 32
HIGH = lax.Precision.HIGH
WIDE = ("sp", "rep")


def trig(length, freq, positions):
    phases = (freq[:, None] * positions[None, :]) % length
    angles = 2.0 * math.pi / length * phases.astype(jnp.float32)
    return jnp.cos(angles), jnp.sin(angles)


def kron_pair(cos_a, sin_a, cos_b, sin_b):
    ca, sa = cos_a.T[:, None, :, None], sin_a.T[:, None, :, None]
    cb, sb = cos_b.T[None, :, None, :], sin_b.T[None, :, None, :]
    return ca * cb - sa * sb, sa * cb + ca * sb


def split(value):
    high = value.astype(jnp.bfloat16)
    low = (value - high.astype(jnp.float32)).astype(jnp.bfloat16)
    return high, low


def dot3(left, right):
    lh, ll = left
    rh, rl = right
    d = functools.partial(jnp.dot, preferred_element_type=jnp.float32)
    return d(lh, rh) + (d(lh, rl) + d(ll, rh))


def sum_kernel(
    sizes, field_ref, modes_ref, table_ref, summed_ref, total_ref, acc1, acc2, held, send_sem, recv_sem
):
    step = pl.program_id(0)
    n_sp, n_sub, n_rep = sizes
    count = n_sp * n_sub * n_rep
    me = (lax.axis_index("sp") * n_sub + lax.axis_index("sub")) * n_rep + lax.axis_index("rep")

    def place(index):
        return {
            "sp": index // (n_sub * n_rep),
            "sub": (index // n_rep) % n_sub,
            "rep": index % n_rep,
        }

    @pl.when(step == 0)
    def _():
        barrier = pltpu.get_barrier_semaphore()

        def greet(k, carry):
            pl.semaphore_signal(
                barrier,
                inc=1,
                device_id=place((me + k) % count),
                device_id_type=pl.DeviceIdType.MESH,
            )
            return carry

        lax.fori_loop(1, count, greet, 0)

    chans, cells, width = field_ref.shape
    rank = modes_ref.shape[2]

    @pl.when(step == 0)
    def _():
        acc1[...] = jnp.zeros_like(acc1)
        acc2[...] = jnp.zeros_like(acc2)

    table = split(table_ref[...])
    chunk = 32 if chans % 32 == 0 else chans

    def body(index, carry):
        rows = pl.ds(pl.multiple_of(index * chunk, chunk), chunk)
        modes = modes_ref[rows].reshape(chunk * cells, rank)
        value = dot3(split(modes), table).reshape(chunk, cells, width) + field_ref[rows]
        summed_ref[rows] = value
        acc1[rows] += value
        acc2[rows] += value * value
        return carry

    lax.fori_loop(0, chans // chunk, body, 0)

    @pl.when(step == pl.num_programs(0) - 1)
    def _():
        def row(acc):
            per = jnp.sum(acc[...], axis=1)
            per = jnp.sum(per.reshape(GROUPS, chans // GROUPS, width), axis=1)
            per = jnp.broadcast_to(jnp.sum(per, axis=1, keepdims=True), (GROUPS, 128))
            lanes = lax.broadcasted_iota(jnp.int32, (GROUPS, 128), 1)
            rows = lax.broadcasted_iota(jnp.int32, (GROUPS, 128), 0)
            return jnp.sum(jnp.where(lanes == rows, per, 0.0), axis=0, keepdims=True)

        tile = lax.broadcasted_iota(jnp.int32, (8, 128), 0)
        held[0] = jnp.where(tile == 0, row(acc1), jnp.where(tile == 1, row(acc2), 0.0))
        pl.semaphore_wait(pltpu.get_barrier_semaphore(), count - 1)

        def copy(k):
            return pltpu.make_async_remote_copy(
                src_ref=held.at[0],
                dst_ref=held.at[k],
                send_sem=send_sem.at[k],
                recv_sem=recv_sem.at[k],
                device_id=place((me + k) % count),
                device_id_type=pl.DeviceIdType.MESH,
            )

        def launch(k, carry):
            copy(k).start()
            return carry

        def finish(k, carry):
            copy(k).wait()
            return carry

        lax.fori_loop(1, count, launch, 0)
        lax.fori_loop(1, count, finish, 0)
        total_ref[...] = jnp.sum(held[...], axis=0)


def mlp_kernel(summed_ref, vec_ref, w_in_ref, w_out_ref, out_ref):
    cells = summed_ref.shape[1]
    w_in = split(w_in_ref[...])
    w_out = split(w_out_ref[...])
    vec = vec_ref[...]
    mean, scale, bias = vec[:, 0:1], vec[:, 1:2], vec[:, 2:3]
    b_in, b_out = vec[:, 3:4], vec[:, 4:5]
    pair = 2 if cells % 2 == 0 else 1
    for start in range(0, cells, pair):
        parts = [summed_ref[:, p, :] for p in range(start, start + pair)]
        value = jnp.concatenate(parts, axis=1) if pair > 1 else parts[0]
        normed = (value - mean) * scale + bias
        hidden = dot3(w_in, split(normed)) + b_in
        inner = math.sqrt(2.0 / math.pi) * (hidden + 0.044715 * (hidden * hidden * hidden))
        hidden = hidden * (0.5 * (1.0 + jnp.tanh(inner)))
        result = value + dot3(w_out, split(hidden)) + b_out
        width = summed_ref.shape[2]
        for k in range(pair):
            out_ref[:, start + k, :] = result[:, k * width : (k + 1) * width]


def general(
    field, mix_weight, factor_x, factor_y, factor_z, norm_gain, norm_bias, w_in, b_in, w_out, b_out
):
    wide_count = lax.axis_size(WIDE)
    narrow_count = lax.axis_size("sub")
    own_chans, x_local, ny, nz = field.shape
    chans = own_chans * wide_count
    nx = x_local * narrow_count
    kx, ky, kz = factor_x.shape[1], factor_y.shape[1], factor_z.shape[1]
    y_local = ny // wide_count
    half = kz // 2
    kept = half + 1
    me_sub = lax.axis_index("sub")
    cells = x_local * y_local

    spatial = field.reshape(own_chans, x_local, wide_count, y_local, nz)
    spatial = spatial.transpose(2, 0, 1, 3, 4).reshape(wide_count, own_chans, cells, nz)
    spatial = lax.all_to_all(spatial, WIDE, split_axis=0, concat_axis=0, tiled=True)

    cos_z, sin_z = trig(nz, jnp.arange(kept), jnp.arange(nz))
    forward = jnp.concatenate([cos_z, -sin_z]) / nz
    planes = jnp.einsum("rz,cxyz->rcxy", forward, field, precision=HIGH)
    planes = planes.reshape(2 * kept * own_chans, x_local * ny)

    def freqs(length, count):
        index = jnp.arange(count)
        return jnp.where(index < count // 2, index, length - count + index)

    cos_y, sin_y = trig(ny, freqs(ny, ky), jnp.arange(ny))

    def forward_xy(values, owner):
        cos_x, sin_x = trig(nx, freqs(nx, kx), owner * x_local + jnp.arange(x_local))
        c, s = kron_pair(cos_x, sin_x, cos_y, sin_y)
        c = (c / (nx * ny)).reshape(x_local * ny, kx * ky)
        s = (s / (nx * ny)).reshape(x_local * ny, kx * ky)
        a = jnp.dot(values, jnp.concatenate([c, s], axis=1), precision=HIGH)
        a = a.reshape(2, kept * own_chans, 2, kx * ky)
        return a[0, :, 0] + a[1, :, 1], a[1, :, 0] - a[0, :, 1]

    held = planes
    real, imag = forward_xy(held, me_sub)
    for hop in range(1, narrow_count):
        held = lax.ppermute(held, "sub", [(i, (i + 1) % narrow_count) for i in range(narrow_count)])
        owner = (me_sub - hop + narrow_count) % narrow_count
        more_real, more_imag = forward_xy(held, owner)
        real, imag = real + more_real, imag + more_imag

    start = lax.axis_index(WIDE) * own_chans
    fx = lax.dynamic_slice_in_dim(factor_x, start, own_chans, 0)
    fy = lax.dynamic_slice_in_dim(factor_y, start, own_chans, 0)
    fz = lax.dynamic_slice_in_dim(factor_z, start, own_chans, 0)
    mirror_x = (-jnp.arange(kx)) % kx
    mirror_y = (-jnp.arange(ky)) % ky
    plane_a = (fx[:, :, None] * fy[:, None, :]).reshape(own_chans, kx * ky)
    plane_b = (fx[:, mirror_x][:, :, None] * fy[:, mirror_y][:, None, :]).reshape(own_chans, kx * ky)
    zero = jnp.zeros((own_chans, 1), jnp.float32)
    z_plus = jnp.concatenate([fz[:, :half], zero], axis=1).T
    z_minus = jnp.concatenate([zero, fz[:, half:][:, ::-1]], axis=1).T
    weight = z_plus[:, :, None] * plane_a[None] + z_minus[:, :, None] * plane_b[None]
    weight = weight.reshape(kept * own_chans, kx * ky)
    real, imag = real * weight, imag * weight

    cos_x, sin_x = trig(nx, freqs(nx, kx), me_sub * x_local + jnp.arange(x_local))
    c, s = kron_pair(cos_x, sin_x, cos_y, sin_y)

    def columns(t):
        t = t.reshape(x_local, wide_count, y_local, kx * ky)
        return t.transpose(3, 1, 0, 2).reshape(kx * ky, wide_count * cells)

    c, s = columns(c), columns(s)
    table_re = jnp.concatenate([c, -s])
    table_im = jnp.concatenate([s, c])
    both = jnp.concatenate([real, imag], axis=1)
    back = jnp.stack(
        [jnp.dot(both, table_re, precision=HIGH), jnp.dot(both, table_im, precision=HIGH)]
    )
    back = back.reshape(2 * kept, own_chans, wide_count, cells)
    back = back.transpose(2, 1, 0, 3).reshape(wide_count * own_chans, 2 * kept * cells)
    back, spatial = lax.optimization_barrier((back, spatial))
    back = lax.all_to_all(back, WIDE, split_axis=0, concat_axis=0, tiled=True)
    back = back.reshape(chans, 2 * kept, cells)
    mixed = jnp.einsum("oi,irp->opr", mix_weight, back, precision=HIGH)

    inverse_z = jnp.concatenate([cos_z, -sin_z])
    spatial = spatial.reshape(chans, cells, nz)
    block = 8 if cells % 8 == 0 else cells
    steps = cells // block
    cube = pl.BlockSpec((chans, block, nz), lambda i: (0, i, 0))
    whole = lambda *shape: pl.BlockSpec(shape, lambda i: (0,) * len(shape))
    sizes = (lax.axis_size("sp"), narrow_count, lax.axis_size("rep"))
    count = sizes[0] * sizes[1] * sizes[2]
    summed, stats = pl.pallas_call(
        functools.partial(sum_kernel, sizes),
        grid=(steps,),
        out_shape=(
            jax.ShapeDtypeStruct(spatial.shape, jnp.float32),
            jax.ShapeDtypeStruct((8, 128), jnp.float32),
        ),
        in_specs=[
            cube,
            pl.BlockSpec((chans, block, 2 * kept), lambda i: (0, i, 0)),
            whole(2 * kept, nz),
        ],
        out_specs=(cube, whole(8, 128)),
        scratch_shapes=[pltpu.VMEM((chans, block, nz), jnp.float32)] * 2
        + [
            pltpu.VMEM((count, 8, 128), jnp.float32),
            pltpu.SemaphoreType.DMA((count,)),
            pltpu.SemaphoreType.DMA((count,)),
        ],
        compiler_params=pltpu.CompilerParams(collective_id=0, has_side_effects=True),
        name="sum_stats",
    )(spatial, mixed, inverse_z)

    size = chans // GROUPS
    stats = stats[:2, :GROUPS]
    cells_group = size * nx * ny * nz
    group_mean = stats[0] / cells_group
    group_var = stats[1] / cells_group - group_mean * group_mean
    scale = jnp.repeat(lax.rsqrt(group_var + 1e-05), size) * norm_gain
    mean = jnp.repeat(group_mean, size)
    vec = jnp.stack([mean, scale, norm_bias, b_in, b_out] + [b_out] * 3, axis=1)

    result = pl.pallas_call(
        mlp_kernel,
        grid=(steps,),
        out_shape=jax.ShapeDtypeStruct(spatial.shape, jnp.float32),
        in_specs=[cube, whole(chans, 8), whole(*w_in.shape), whole(*w_out.shape)],
        out_specs=cube,
        name="mlp",
    )(summed, vec, w_in, w_out)
    return result.reshape(chans, x_local, y_local, nz)


MESH = pl.DeviceIdType.MESH
LANES = 128


def cosine(index, length):
    fold = jnp.abs(index.astype(jnp.float32) * (2.0 / length) - 1.0)
    near = jnp.minimum(fold, 1.0 - fold) * math.pi
    square = near * near
    total = jnp.full_like(square, 1.0 / math.factorial(14))
    for power in range(6, -1, -1):
        term = 1.0 / math.factorial(2 * power)
        total = term - square * total
    return jnp.where(fold > 0.5, total, -total)


def log2(value):
    return value.bit_length() - 1


def split3(value):
    high = value.astype(jnp.bfloat16)
    rest = value - high.astype(jnp.float32)
    mid = rest.astype(jnp.bfloat16)
    low = (rest - mid.astype(jnp.float32)).astype(jnp.bfloat16)
    return high, mid, low


def pick(left, right):
    d = functools.partial(jnp.dot, preferred_element_type=jnp.float32)
    a, b, c = split3(right)
    return d(left, a) + (d(left, b) + d(left, c))


def pick_right(left, right):
    d = functools.partial(jnp.dot, preferred_element_type=jnp.float32)
    a, b, c = split3(left)
    return d(a, right) + (d(b, right) + d(c, right))


def iota(shape, axis):
    return lax.broadcasted_iota(jnp.int32, shape, axis)


def fused_kernel(
    dims,
    field_ref, mix_ref, w_in_ref, w_out_ref, fx_ref, fy_ref, fz_ref, gain_ref, bias_ref, b_in_ref, b_out_ref,
    out_ref,
    fld, mats, facs, vecs, g_hi, g_lo, gi_hi, gi_lo, yf_hi, yf_lo, yi_hi, yi_lo, xt_hi, xt_lo, fxs, uv, fy_t, fz_t,
    se, sh, lf, re, rh, pin, mid, bs, lb, ls, rb, rl, held, cols, obuf,
    fld_sem, par_sem, own_sem, e_send, e_recv, h_send, h_recv, x_send, x_recv, b_send, b_recv, l_send, l_recv,
    t_send, t_recv, o_sem,
):
    n_sp, n_sub, n_rep, n_freq = dims
    wide = n_sp * n_rep
    count = wide * n_sub
    own, xy_rows, nz = field_ref.shape
    chans = own * wide
    parts, x_local, _, _ = se.shape[1:]
    y_local = LANES // (nz // (2 * parts))
    width = LANES // y_local
    nx = pin.shape[1]
    ny = xy_rows // x_local
    kz = n_freq
    half = kz // 2
    chain = own // n_sub
    sub8 = chain // 8
    tiles = wide + 1
    ltile = half * ny // LANES
    per_tile = LANES // ny
    lane_y, lane_n = log2(y_local), log2(ny)

    me_sub = lax.axis_index("sub")
    me_wide = lax.axis_index("sp") * n_rep + lax.axis_index("rep")
    me = me_wide * n_sub + me_sub

    def place(w, s):
        return {"sp": w // n_rep, "sub": s, "rep": w % n_rep}

    def place_flat(index):
        return place(index // n_sub, index % n_sub)

    def loop(n, body):
        def step(i, carry):
            body(i)
            return carry

        lax.fori_loop(0, n, step, 0)

    barrier = pltpu.get_barrier_semaphore()

    def greet(k, carry):
        pl.semaphore_signal(barrier, inc=1, device_id=place_flat((me + k) % count), device_id_type=MESH)
        return carry

    lax.fori_loop(1, count, greet, 0)

    xchunks = fld_sem.shape[0]
    xc_size = x_local // xchunks

    def fetch(i):
        rows = pl.ds(i * (xc_size * ny), xc_size * ny)
        return pltpu.make_async_copy(field_ref.at[:, rows], fld.at[:, rows], fld_sem.at[i])

    for i in range(xchunks):
        fetch(i).start()
    params = [(mix_ref, mats.at[0]), (w_in_ref, mats.at[1]), (w_out_ref, mats.at[2])]
    params += [(fx_ref, facs.at[0]), (fy_ref, facs.at[1]), (fz_ref, facs.at[2])]
    params += [(gain_ref, vecs.at[0]), (bias_ref, vecs.at[1]), (b_in_ref, vecs.at[2]), (b_out_ref, vecs.at[3])]
    param_copies = [pltpu.make_async_copy(a, b, par_sem.at[i]) for i, (a, b) in enumerate(params)]
    for copy in param_copies:
        copy.start()

    def coef(j):
        low_k = jnp.where(j == 1, half, j >> 1)
        low_s = jnp.where(j == 1, 0, j & 1)
        high_k = (j + 1) >> 1
        high_s = 1 - (j & 1)
        return jnp.where(j < kz, low_k, high_k), jnp.where(j < kz, low_s, high_s)

    def basis(j, z):
        k, s = coef(j)
        value = cosine((k * z + s * (3 * nz // 4)) & (nz - 1), nz)
        edge = (k == 0) | (k == nz // 2)
        return value * jnp.where(edge, math.sqrt(1.0 / nz), math.sqrt(2.0 / nz))

    def g_entry(rows, columns):
        y_in, z = rows >> log2(nz), rows & (nz - 1)
        j, y_out = columns >> lane_y, columns & (y_local - 1)
        return jnp.where(y_in == y_out, basis(j, z), 0.0)

    size = nz * y_local
    stepr = LANES

    def build_g(i):
        rows = pl.ds(pl.multiple_of(i * stepr, stepr), stepr)
        a = iota((stepr, size), 0) + i * stepr
        b = iota((stepr, size), 1)
        g_hi[rows], g_lo[rows] = split(g_entry(a, b))
        gi_hi[rows], gi_lo[rows] = split(g_entry(b, a))

    loop(size // stepr, build_g)

    lane = iota((1, LANES), 1)

    def e_copy(xc, k):
        w = (me_wide + k) % wide
        xs = pl.ds(xc * xc_size, xc_size)
        return pltpu.make_async_remote_copy(
            src_ref=se.at[w, :, xs],
            dst_ref=re.at[:, xs, pl.ds(pl.multiple_of(me_wide * own, own), own)],
            send_sem=e_send.at[xc, k],
            recv_sem=e_recv.at[xc, k],
            device_id=place(w, me_sub),
            device_id_type=MESH,
        )

    hchunks = h_send.shape[0]
    hc_size = x_local // hchunks

    def h_copy(hc, k):
        w = (me_wide + k) % wide
        xs = pl.ds(hc * hc_size, hc_size)
        return pltpu.make_async_remote_copy(
            src_ref=sh.at[w, xs],
            dst_ref=rh.at[xs, :, pl.ds(pl.multiple_of(me_wide * own, own), own)],
            send_sem=h_send.at[hc, k],
            recv_sem=h_recv.at[hc, k],
            device_id=place(w, me_sub),
            device_id_type=MESH,
        )

    def peers(make, what, n=wide):
        def step(k, carry):
            getattr(make(k), what)()
            return carry

        lax.fori_loop(1, n, step, 0)

    zero = jnp.zeros((own, LANES), jnp.float32)

    def transform(xc, squares):
        fetch(xc).wait()

        def one(d, carry):
            left, sq = carry
            groups = []
            for xi in range(xc_size):
                row = (xc * xc_size + xi) * ny + d * y_local
                groups.append(jnp.concatenate([fld[:, row + y, :] for y in range(y_local)], axis=1))
            value = jnp.concatenate(groups, axis=0)
            res = dot3(split(value), (g_hi[...], g_lo[...]))
            cube = res.reshape(xc_size, own, size)
            xs = pl.ds(xc * xc_size, xc_size)
            for g in range(parts):
                se[d, g, xs] = cube[:, :, g * LANES : (g + 1) * LANES]
                part = cube[:, :, (parts + g) * LANES : (parts + g + 1) * LANES]
                sh[d, xs, g] = part
                sq = sq + jnp.sum(part * part, axis=0)
            more = pltpu.roll(res[:, LANES : 2 * LANES], d * y_local, axis=1)
            left = jnp.where((lane >> lane_y) == d, more, left)
            return left, sq

        left = jnp.zeros((xc_size * own, LANES), jnp.float32)
        left, squares = lax.fori_loop(0, wide, one, (left, squares))
        lf[pl.ds(xc * xc_size, xc_size)] = left.reshape(xc_size, own, LANES)

        @pl.when(xc == 1)
        def _():
            pl.semaphore_wait(barrier, count - 1)

        @pl.when(xc >= 1)
        def _():
            peers(lambda k: e_copy(xc - 1, k), "start")

        return squares

    squares = lax.fori_loop(0, xchunks, transform, zero)
    for copy in param_copies:
        copy.wait()

    def x_src(t, s):
        cs = pl.ds(pl.multiple_of(s * chain, 8), chain)
        return se.at[t, 0, :, cs] if t < wide else lf.at[:, cs]

    def x_dst(t):
        return pin.at[t, pl.ds(me_sub * x_local, x_local)]

    x_copies = []
    for t in range(tiles):
        for k in range(1, n_sub):
            s = (me_sub + k) % n_sub
            x_copies.append(
                pltpu.make_async_remote_copy(
                    src_ref=x_src(t, s),
                    dst_ref=x_dst(t),
                    send_sem=x_send.at[t, k],
                    recv_sem=x_recv.at[t, k],
                    device_id=place(me_wide, s),
                    device_id_type=MESH,
                )
            )
    own_chan = pl.ds(pl.multiple_of(me_wide * own, own), own)
    own_copies = [pltpu.make_async_copy(x_src(t, me_sub), x_dst(t), own_sem.at[t]) for t in range(tiles)]
    own_copies.append(pltpu.make_async_copy(se.at[me_wide], re.at[:, :, own_chan], own_sem.at[tiles]))
    own_copies.append(pltpu.make_async_copy(sh.at[me_wide], rh.at[:, :, own_chan], own_sem.at[tiles + 1]))

    def p_meta(t, r):
        jj = r >> lane_y
        k = jnp.where(jj == 1, half, jj >> 1)
        s = jnp.where(jj == 1, 0, jj & 1)
        y = t * y_local + (r & (y_local - 1))
        rest = t == wide
        k = jnp.where(rest, jnp.where(r < ny, half, -1), k)
        return k, jnp.where(rest, 1, s), jnp.where(rest, r, y)

    def m_meta(t, c):
        part = jnp.where(t >= ltile, 1, 0)
        k = (t - part * ltile) * per_tile + (c >> lane_n)
        rest = t == 2 * ltile
        seat = c & (LANES // 2 - 1)
        k = jnp.where(rest, jnp.where(seat < ny, half, -2), k)
        part = jnp.where(rest, c >> log2(LANES // 2), part)
        return k, part, c & (ny - 1)

    def y_entry(pt, mt, p, m, power):
        kp, s, y = p_meta(pt, p)
        km, part, b = m_meta(mt, m)
        value = cosine((y * b + (ny // 4) * (s + part)) & (ny - 1), ny)
        norm = jnp.where(km == 0, math.sqrt(1.0 / nz), math.sqrt(2.0 / nz))
        scale = norm if power else 1.0 / norm
        if not power:
            scale = scale * (1.0 / nz)
        else:
            scale = 1.0 / scale
        return jnp.where(kp == km, value * scale, 0.0)

    square = (LANES, LANES)
    mtiles = 2 * ltile + 1

    def build_y(i):
        rows = pl.ds(pl.multiple_of(i * LANES, LANES), LANES)
        for t in range(mtiles):
            cut = slice(t * LANES, (t + 1) * LANES)
            a, b = iota(square, 0), iota(square, 1)
            yf_hi[rows, cut], yf_lo[rows, cut] = split(y_entry(i, t, a, b, False))
            yi_hi[rows, cut], yi_lo[rows, cut] = split(y_entry(t, i, b, a, True))

    def build_x(i):
        shape = (LANES, nx * 8)
        row = iota(shape, 0) + i * LANES
        col = iota(shape, 1)
        part = row >> log2(nx * 8)
        a = (row >> 3) & (nx - 1)
        value = cosine(((a * (col >> 3)) + part * (3 * nx // 4)) & (nx - 1), nx)
        value = jnp.where((row & 7) == (col & 7), value, 0.0)
        rows = pl.ds(pl.multiple_of(i * LANES, LANES), LANES)
        xt_hi[rows], xt_lo[rows] = split(value)

    peers(lambda k: e_copy(xchunks - 1, k), "start")
    for copy in x_copies:
        copy.start()
    for copy in own_copies:
        copy.start()
    loop(tiles, build_y)
    loop(2 * nx * 8 // LANES, build_x)

    fy_t[...] = jnp.transpose(facs[1])
    fz_t[...] = jnp.transpose(facs[2])
    first = me_wide * own + me_sub * chain
    bf = jnp.bfloat16
    one_hot = lambda mask: jnp.where(mask, 1.0, 0.0).astype(bf)
    for h in range(sub8):
        base = pl.multiple_of(first + 8 * h, 8)
        a = iota((nx * 8, nx), 0) >> 3
        b = iota((nx * 8, nx), 1)
        mask = iota((nx * 8, chans), 1) == first + 8 * h + (iota((nx * 8, chans), 0) & 7)
        for sign in range(2):
            want = a if sign == 0 else (nx - a) & (nx - 1)
            spread = pick(one_hot(b == want), facs[0])
            column = jnp.sum(jnp.where(mask, spread, 0.0), axis=1, keepdims=True)
            fxs[h, sign] = jnp.broadcast_to(column * (1.0 / (nx * ny)), (nx * 8, LANES))
        fz8, fy8 = fz_t[pl.ds(base, 8), :], fy_t[pl.ds(base, 8), :]
        for t in range(ltile + 1):
            i = iota((kz, LANES), 0)
            seat = iota((kz, LANES), 1)
            k = t * per_tile + (seat >> lane_n) if t < ltile else half
            bb = seat & (ny - 1)
            plus = one_hot(i == (k if t < ltile else -1))
            minus = one_hot((i == kz - k) & (k > 0)) if t < ltile else one_hot(i == half)
            yp, ym = one_hot(i == bb), one_hot(i == ((ny - bb) & (ny - 1)))
            uv[h, 0, t] = pick_right(fz8, plus) * pick_right(fy8, yp)
            uv[h, 1, t] = pick_right(fz8, minus) * pick_right(fy8, ym)

    for copy in own_copies:
        copy.wait()
    for copy in x_copies:
        copy.wait()

    rows8 = nx * 8

    def forward_y(h):
        cs = pl.ds(pl.multiple_of(h * 8, 8), 8)
        value = jnp.concatenate([pin[t, :, cs, :].reshape(rows8, LANES) for t in range(tiles)], axis=1)
        res = dot3(split(value), (yf_hi[...], yf_lo[...]))
        for t in range(mtiles):
            mid[h, t] = res[:, t * LANES : (t + 1) * LANES]

    loop(sub8, forward_y)

    def weights(h, t):
        u = jnp.broadcast_to(uv[h, 0, t][None], (nx, 8, LANES)).reshape(rows8, LANES)
        v = jnp.broadcast_to(uv[h, 1, t][None], (nx, 8, LANES)).reshape(rows8, LANES)
        return fxs[h, 0] * u + fxs[h, 1] * v

    def along_x(value):
        return dot3((xt_hi[...], xt_lo[...]), split(value))

    def pair_x(i):
        h, t = i // ltile, i % ltile
        res = along_x(jnp.concatenate([mid[h, t], mid[h, ltile + t]], axis=1))
        c_re, c_im = res[:rows8, :LANES], res[:rows8, LANES:]
        s_re, s_im = res[rows8:, :LANES], res[rows8:, LANES:]
        w = weights(h, t)
        res = along_x(jnp.concatenate([(c_re + s_im) * w, (c_im - s_re) * w], axis=1))
        c_re, c_im = res[:rows8, :LANES], res[:rows8, LANES:]
        s_re, s_im = res[rows8:, :LANES], res[rows8:, LANES:]
        mid[h, t] = c_re - s_im
        mid[h, ltile + t] = c_im + s_re

    loop(sub8 * ltile, pair_x)

    def rest_x(h):
        sign = jnp.where(lane < LANES // 2, 1.0, -1.0)
        res = along_x(mid[h, 2 * ltile])
        modes = res[:rows8] + sign * pltpu.roll(res[rows8:], LANES // 2, axis=1)
        res = along_x(modes * weights(h, ltile))
        mid[h, 2 * ltile] = res[:rows8] - sign * pltpu.roll(res[rows8:], LANES // 2, axis=1)

    loop(sub8, rest_x)

    def back_y(h):
        cs = pl.ds(pl.multiple_of(h * 8, 8), 8)
        value = jnp.concatenate([mid[h, t] for t in range(mtiles)], axis=1)
        res = dot3(split(value), (yi_hi[...], yi_lo[...]))
        for t in range(tiles):
            cut = res[:, t * LANES : (t + 1) * LANES].reshape(nx, 8, LANES)
            if t < wide:
                bs[t, :, cs, :] = cut
            else:
                lb[:, cs, :] = cut

    loop(sub8, back_y)

    def gather_rest(s):
        def one(x, carry):
            value = lb[s * x_local + x]
            new = []
            for d in range(wide):
                moved = pltpu.roll(value, ((x - d) * y_local + LANES) & (LANES - 1), axis=1)
                new.append(jnp.where((lane >> lane_y) == x, moved, carry[d]))
            return tuple(new)

        start = tuple(jnp.zeros((chain, LANES), jnp.float32) for _ in range(wide))
        done = lax.fori_loop(0, x_local, one, start)
        for d in range(wide):
            ls[s, d] = done[d]

    loop(n_sub, gather_rest)

    b_rows = pl.ds(pl.multiple_of(first, 8), chain)

    def b_copy(k):
        index = (me + k) % count
        w, s = index // n_sub, index % n_sub
        return pltpu.make_async_remote_copy(
            src_ref=bs.at[w, pl.ds(s * x_local, x_local)],
            dst_ref=rb.at[:, b_rows],
            send_sem=b_send.at[k],
            recv_sem=b_recv.at[k],
            device_id=place(w, s),
            device_id_type=MESH,
        )

    def l_copy(k):
        index = (me + k) % count
        w, s = index // n_sub, index % n_sub
        return pltpu.make_async_remote_copy(
            src_ref=ls.at[s, w],
            dst_ref=rl.at[b_rows],
            send_sem=l_send.at[k],
            recv_sem=l_recv.at[k],
            device_id=place(w, s),
            device_id_type=MESH,
        )

    peers(b_copy, "start", count)
    own_b = pltpu.make_async_copy(bs.at[me_wide, pl.ds(me_sub * x_local, x_local)], rb.at[:, b_rows], b_send.at[0])
    own_l = pltpu.make_async_copy(ls.at[me_sub, me_wide], rl.at[b_rows], l_send.at[0])
    own_b.start()
    own_l.start()
    peers(l_copy, "start", count)
    loop(hchunks, lambda hc: peers(lambda k: h_copy(hc, k), "start"))

    eye = iota((chans, chans), 0) == iota((chans, chans), 1)
    for i in range(4):
        column = jnp.sum(jnp.where(eye, vecs[i], 0.0), axis=1, keepdims=True)
        cols[i] = jnp.broadcast_to(column, (chans, LANES))

    own_b.wait()
    own_l.wait()
    peers(b_copy, "wait", count)
    peers(l_copy, "wait", count)
    loop(xchunks, lambda xc: peers(lambda k: e_copy(xc, k), "wait"))
    mix = split(mats[0])
    rest = dot3(mix, split(rl[...]))
    lows = lane < y_local
    blank = jnp.zeros((chans, LANES), jnp.float32)

    def low(i, carry):
        one, two = carry
        spectral = dot3(mix, split(jnp.concatenate([rb[2 * i], rb[2 * i + 1]], axis=1)))
        for j in range(2):
            x = 2 * i + j
            value = re[0, x] + spectral[:, j * LANES : (j + 1) * LANES]
            re[0, x] = value
            one = one + jnp.where(lows, value, 0.0)
            two = two + value * value
            moved = pltpu.roll(rest, (LANES - x * y_local) & (LANES - 1), axis=1)
            value = re[1, x] + jnp.where(lows, moved, 0.0)
            re[1, x] = value
            two = two + value * value
        return one, two

    one, two = lax.fori_loop(0, x_local // 2, low, (blank, blank))

    per_group = chans // GROUPS

    def row(acc, base):
        groups = acc.shape[0] // per_group
        per = jnp.sum(acc.reshape(groups, per_group, LANES), axis=1)
        per = jnp.broadcast_to(jnp.sum(per, axis=1, keepdims=True), (groups, LANES))
        seat = iota((groups, LANES), 1) == iota((groups, LANES), 0) + base
        return jnp.sum(jnp.where(seat, per, 0.0), axis=0, keepdims=True)

    tile = iota((8, LANES), 0)
    sum_one = row(one, 0) * math.sqrt(nz)
    sum_two = row(two, 0) + row(squares, me_wide * (own // per_group))
    held[0] = jnp.where(tile == 0, sum_one, jnp.where(tile == 1, sum_two, 0.0))

    def t_copy(k):
        return pltpu.make_async_remote_copy(
            src_ref=held.at[0],
            dst_ref=held.at[k],
            send_sem=t_send.at[k],
            recv_sem=t_recv.at[k],
            device_id=place_flat((me + k) % count),
            device_id_type=MESH,
        )

    peers(t_copy, "start", count)
    peers(t_copy, "wait", count)
    total = jnp.sum(held[...], axis=0)
    cells_group = per_group * nx * ny * nz
    group_mean = total[0:1] / cells_group
    group_var = total[1:2] / cells_group - group_mean * group_mean
    group_scale = lax.rsqrt(group_var + 1e-05)
    seat = iota((chans, LANES), 1) == iota((chans, LANES), 0) // per_group

    def column_of(value):
        return jnp.sum(jnp.where(seat, value, 0.0), axis=1, keepdims=True)

    scale = column_of(group_scale) * cols[0, :, 0:1]
    shift = cols[1, :, 0:1] - column_of(group_mean) * scale
    cols[4] = jnp.broadcast_to(scale, (chans, LANES))
    cols[5] = jnp.broadcast_to(shift, (chans, LANES))

    def out_copy(hc, slot):
        rows = pl.ds(pl.multiple_of(hc * (hc_size * y_local), 8), hc_size * y_local)
        return pltpu.make_async_copy(obuf.at[slot], out_ref.at[:, rows], o_sem.at[slot])

    def late(hc, carry):
        slot = hc % 2
        peers(lambda k: h_copy(hc, k), "wait")

        @pl.when(hc >= 2)
        def _():
            out_copy(hc - 2, slot).wait()

        w_in, w_out = split(mats[1]), split(mats[2])
        factor, offset = cols[4, :, 0:1], cols[5, :, 0:1]
        b_in, b_out = cols[2, :, 0:1], cols[3, :, 0:1]
        for j in range(hc_size):
            x = hc * hc_size + j
            value = jnp.concatenate([re[g, x] for g in range(parts)] + [rh[x, g] for g in range(parts)], axis=1)
            value = dot3(split(value), (gi_hi[...], gi_lo[...]))
            normed = value * factor + offset
            hidden = dot3(w_in, split(normed)) + b_in
            inner = math.sqrt(2.0 / math.pi) * (hidden + 0.044715 * (hidden * hidden * hidden))
            hidden = hidden * (0.5 * (1.0 + jnp.tanh(inner)))
            result = value + dot3(w_out, split(hidden)) + b_out
            for y in range(y_local):
                obuf[slot, :, j * y_local + y, :] = result[:, y * nz : (y + 1) * nz]
        out_copy(hc, slot).start()
        return carry

    lax.fori_loop(0, hchunks, late, 0)
    out_copy(hchunks - 2, (hchunks - 2) % 2).wait()
    out_copy(hchunks - 1, (hchunks - 1) % 2).wait()


def fused(
    field, mix_weight, factor_x, factor_y, factor_z, norm_gain, norm_bias, w_in, b_in, w_out, b_out
):
    n_sp, n_sub, n_rep = (lax.axis_size(a) for a in ("sp", "sub", "rep"))
    wide, count = n_sp * n_rep, n_sp * n_rep * n_sub
    own, x_local, ny, nz = field.shape
    chans, nx, y_local = own * wide, x_local * n_sub, ny // wide
    kz = factor_z.shape[1]
    chain = own // n_sub
    sub8 = chain // 8
    tiles = wide + 1
    ltile = kz // 2 * ny // LANES
    mtiles = 2 * ltile + 1
    parts = nz * y_local // LANES // 2
    size = nz * y_local
    xchunks, hchunks = 4, x_local * y_local // 8
    f32, bf = jnp.float32, jnp.bfloat16
    vmem = lambda *shape: pltpu.VMEM(shape, f32)
    table = lambda *shape: pltpu.VMEM(shape, bf)
    dma = lambda *shape: pltpu.SemaphoreType.DMA(shape)
    scratch = [
        vmem(own, x_local * ny, nz), vmem(3, chans, chans), vmem(3, kz, chans), vmem(4, 1, chans),
        table(size, size), table(size, size), table(size, size), table(size, size),
        table(tiles * LANES, mtiles * LANES), table(tiles * LANES, mtiles * LANES),
        table(mtiles * LANES, tiles * LANES), table(mtiles * LANES, tiles * LANES),
        table(2 * nx * 8, nx * 8), table(2 * nx * 8, nx * 8),
        vmem(sub8, 2, nx * 8, LANES), vmem(sub8, 2, ltile + 1, 8, LANES), vmem(chans, kz), vmem(chans, kz),
        vmem(wide, parts, x_local, own, LANES), vmem(wide, x_local, parts, own, LANES), vmem(x_local, own, LANES),
        vmem(parts, x_local, chans, LANES), vmem(x_local, parts, chans, LANES),
        vmem(tiles, nx, chain, LANES), vmem(sub8, mtiles, nx * 8, LANES),
        vmem(wide, nx, chain, LANES), vmem(nx, chain, LANES), vmem(n_sub, wide, chain, LANES),
        vmem(x_local, chans, LANES), vmem(chans, LANES), vmem(count, 8, LANES), vmem(6, chans, LANES),
        vmem(2, chans, 8, nz),
        dma(xchunks), dma(10), dma(tiles + 2), dma(xchunks, wide), dma(xchunks, wide), dma(hchunks, wide),
        dma(hchunks, wide), dma(tiles, n_sub), dma(tiles, n_sub), dma(count), dma(count), dma(count), dma(count),
        dma(count), dma(count), dma(2),
    ]
    any_spec = pl.BlockSpec(memory_space=pl.ANY)
    line = lambda v: v.reshape(1, chans)
    result = pl.pallas_call(
        functools.partial(fused_kernel, (n_sp, n_sub, n_rep, kz)),
        out_shape=jax.ShapeDtypeStruct((chans, x_local * y_local, nz), f32),
        in_specs=[any_spec] * 11,
        out_specs=any_spec,
        scratch_shapes=scratch,
        compiler_params=pltpu.CompilerParams(
            collective_id=0, has_side_effects=True, vmem_limit_bytes=VMEM_LIMIT
        ),
        name="fused",
    )(
        field.reshape(own, x_local * ny, nz), mix_weight, w_in, w_out, factor_x.T, factor_y.T, factor_z.T,
        line(norm_gain), line(norm_bias), line(b_in), line(b_out),
    )
    return result.reshape(chans, x_local, y_local, nz)


VMEM_LIMIT = 64 * 1024 * 1024 - 65536


def fits(field, factor_x, factor_y, factor_z):
    n_sub, wide = lax.axis_size("sub"), lax.axis_size(WIDE)
    own, x_local, ny, nz = field.shape
    nx, kz = x_local * n_sub, factor_z.shape[1]
    power = all(v & (v - 1) == 0 for v in (nx, ny, nz, kz))
    if not power or nz != LANES or factor_x.shape[1] != nx or factor_y.shape[1] != ny or ny % wide:
        return False
    y_local = ny // wide
    return (
        kz * y_local == LANES
        and nz == 4 * kz
        and nx == kz == ny
        and own % (8 * n_sub) == 0
        and own % (own * wide // GROUPS) == 0
        and x_local * y_local <= LANES
        and x_local % 4 == 0
        and 8 % y_local == 0
        and (kz // 2 * ny) % LANES == 0
    )


def local(
    field, mix_weight, factor_x, factor_y, factor_z, norm_gain, norm_bias, w_in, b_in, w_out, b_out
):
    run = fused if fits(field, factor_x, factor_y, factor_z) else general
    return run(
        field, mix_weight, factor_x, factor_y, factor_z, norm_gain, norm_bias, w_in, b_in, w_out, b_out
    )


def solution(mesh):
    placed = (P(("grp", "sp", "rep"), "sub", None, None),) + (P(),) * 10
    return jax.shard_map(
        local,
        mesh=mesh,
        in_specs=placed,
        out_specs=P("grp", "sub", ("sp", "rep"), None),
        check_vma=False,
    )
```

```python
import math
import functools

import jax
import jax.numpy as jnp
from jax import lax
from jax.experimental import pallas as pl
from jax.experimental.pallas import tpu as pltpu
from jax.sharding import PartitionSpec as P

GROUPS = 32
HIGH = lax.Precision.HIGH
WIDE = ("sp", "rep")


def trig(length, freq, positions):
    phases = (freq[:, None] * positions[None, :]) % length
    angles = 2.0 * math.pi / length * phases.astype(jnp.float32)
    return jnp.cos(angles), jnp.sin(angles)


def kron_pair(cos_a, sin_a, cos_b, sin_b):
    ca, sa = cos_a.T[:, None, :, None], sin_a.T[:, None, :, None]
    cb, sb = cos_b.T[None, :, None, :], sin_b.T[None, :, None, :]
    return ca * cb - sa * sb, sa * cb + ca * sb


def split(value):
    high = value.astype(jnp.bfloat16)
    low = (value - high.astype(jnp.float32)).astype(jnp.bfloat16)
    return high, low


def dot3(left, right):
    lh, ll = left
    rh, rl = right
    d = functools.partial(jnp.dot, preferred_element_type=jnp.float32)
    return d(lh, rh) + (d(lh, rl) + d(ll, rh))


def sum_kernel(
    sizes, field_ref, modes_ref, table_ref, summed_ref, total_ref, acc1, acc2, held, send_sem, recv_sem
):
    step = pl.program_id(0)
    n_sp, n_sub, n_rep = sizes
    count = n_sp * n_sub * n_rep
    me = (lax.axis_index("sp") * n_sub + lax.axis_index("sub")) * n_rep + lax.axis_index("rep")

    def place(index):
        return {
            "sp": index // (n_sub * n_rep),
            "sub": (index // n_rep) % n_sub,
            "rep": index % n_rep,
        }

    @pl.when(step == 0)
    def _():
        barrier = pltpu.get_barrier_semaphore()

        def greet(k, carry):
            pl.semaphore_signal(
                barrier,
                inc=1,
                device_id=place((me + k) % count),
                device_id_type=pl.DeviceIdType.MESH,
            )
            return carry

        lax.fori_loop(1, count, greet, 0)

    chans, cells, width = field_ref.shape
    rank = modes_ref.shape[2]

    @pl.when(step == 0)
    def _():
        acc1[...] = jnp.zeros_like(acc1)
        acc2[...] = jnp.zeros_like(acc2)

    table = split(table_ref[...])
    chunk = 32 if chans % 32 == 0 else chans

    def body(index, carry):
        rows = pl.ds(pl.multiple_of(index * chunk, chunk), chunk)
        modes = modes_ref[rows].reshape(chunk * cells, rank)
        value = dot3(split(modes), table).reshape(chunk, cells, width) + field_ref[rows]
        summed_ref[rows] = value
        acc1[rows] += value
        acc2[rows] += value * value
        return carry

    lax.fori_loop(0, chans // chunk, body, 0)

    @pl.when(step == pl.num_programs(0) - 1)
    def _():
        def row(acc):
            per = jnp.sum(acc[...], axis=1)
            per = jnp.sum(per.reshape(GROUPS, chans // GROUPS, width), axis=1)
            per = jnp.broadcast_to(jnp.sum(per, axis=1, keepdims=True), (GROUPS, 128))
            lanes = lax.broadcasted_iota(jnp.int32, (GROUPS, 128), 1)
            rows = lax.broadcasted_iota(jnp.int32, (GROUPS, 128), 0)
            return jnp.sum(jnp.where(lanes == rows, per, 0.0), axis=0, keepdims=True)

        tile = lax.broadcasted_iota(jnp.int32, (8, 128), 0)
        held[0] = jnp.where(tile == 0, row(acc1), jnp.where(tile == 1, row(acc2), 0.0))
        pl.semaphore_wait(pltpu.get_barrier_semaphore(), count - 1)

        def copy(k):
            return pltpu.make_async_remote_copy(
                src_ref=held.at[0],
                dst_ref=held.at[k],
                send_sem=send_sem.at[k],
                recv_sem=recv_sem.at[k],
                device_id=place((me + k) % count),
                device_id_type=pl.DeviceIdType.MESH,
            )

        def launch(k, carry):
            copy(k).start()
            return carry

        def finish(k, carry):
            copy(k).wait()
            return carry

        lax.fori_loop(1, count, launch, 0)
        lax.fori_loop(1, count, finish, 0)
        total_ref[...] = jnp.sum(held[...], axis=0)


def mlp_kernel(summed_ref, vec_ref, w_in_ref, w_out_ref, out_ref):
    cells = summed_ref.shape[1]
    w_in = split(w_in_ref[...])
    w_out = split(w_out_ref[...])
    vec = vec_ref[...]
    mean, scale, bias = vec[:, 0:1], vec[:, 1:2], vec[:, 2:3]
    b_in, b_out = vec[:, 3:4], vec[:, 4:5]
    pair = 2 if cells % 2 == 0 else 1
    for start in range(0, cells, pair):
        parts = [summed_ref[:, p, :] for p in range(start, start + pair)]
        value = jnp.concatenate(parts, axis=1) if pair > 1 else parts[0]
        normed = (value - mean) * scale + bias
        hidden = dot3(w_in, split(normed)) + b_in
        inner = math.sqrt(2.0 / math.pi) * (hidden + 0.044715 * (hidden * hidden * hidden))
        hidden = hidden * (0.5 * (1.0 + jnp.tanh(inner)))
        result = value + dot3(w_out, split(hidden)) + b_out
        width = summed_ref.shape[2]
        for k in range(pair):
            out_ref[:, start + k, :] = result[:, k * width : (k + 1) * width]


def general(
    field, mix_weight, factor_x, factor_y, factor_z, norm_gain, norm_bias, w_in, b_in, w_out, b_out
):
    wide_count = lax.axis_size(WIDE)
    narrow_count = lax.axis_size("sub")
    own_chans, x_local, ny, nz = field.shape
    chans = own_chans * wide_count
    nx = x_local * narrow_count
    kx, ky, kz = factor_x.shape[1], factor_y.shape[1], factor_z.shape[1]
    y_local = ny // wide_count
    half = kz // 2
    kept = half + 1
    me_sub = lax.axis_index("sub")
    cells = x_local * y_local

    spatial = field.reshape(own_chans, x_local, wide_count, y_local, nz)
    spatial = spatial.transpose(2, 0, 1, 3, 4).reshape(wide_count, own_chans, cells, nz)
    spatial = lax.all_to_all(spatial, WIDE, split_axis=0, concat_axis=0, tiled=True)

    cos_z, sin_z = trig(nz, jnp.arange(kept), jnp.arange(nz))
    forward = jnp.concatenate([cos_z, -sin_z]) / nz
    planes = jnp.einsum("rz,cxyz->rcxy", forward, field, precision=HIGH)
    planes = planes.reshape(2 * kept * own_chans, x_local * ny)

    def freqs(length, count):
        index = jnp.arange(count)
        return jnp.where(index < count // 2, index, length - count + index)

    cos_y, sin_y = trig(ny, freqs(ny, ky), jnp.arange(ny))

    def forward_xy(values, owner):
        cos_x, sin_x = trig(nx, freqs(nx, kx), owner * x_local + jnp.arange(x_local))
        c, s = kron_pair(cos_x, sin_x, cos_y, sin_y)
        c = (c / (nx * ny)).reshape(x_local * ny, kx * ky)
        s = (s / (nx * ny)).reshape(x_local * ny, kx * ky)
        a = jnp.dot(values, jnp.concatenate([c, s], axis=1), precision=HIGH)
        a = a.reshape(2, kept * own_chans, 2, kx * ky)
        return a[0, :, 0] + a[1, :, 1], a[1, :, 0] - a[0, :, 1]

    held = planes
    real, imag = forward_xy(held, me_sub)
    for hop in range(1, narrow_count):
        held = lax.ppermute(held, "sub", [(i, (i + 1) % narrow_count) for i in range(narrow_count)])
        owner = (me_sub - hop + narrow_count) % narrow_count
        more_real, more_imag = forward_xy(held, owner)
        real, imag = real + more_real, imag + more_imag

    start = lax.axis_index(WIDE) * own_chans
    fx = lax.dynamic_slice_in_dim(factor_x, start, own_chans, 0)
    fy = lax.dynamic_slice_in_dim(factor_y, start, own_chans, 0)
    fz = lax.dynamic_slice_in_dim(factor_z, start, own_chans, 0)
    mirror_x = (-jnp.arange(kx)) % kx
    mirror_y = (-jnp.arange(ky)) % ky
    plane_a = (fx[:, :, None] * fy[:, None, :]).reshape(own_chans, kx * ky)
    plane_b = (fx[:, mirror_x][:, :, None] * fy[:, mirror_y][:, None, :]).reshape(own_chans, kx * ky)
    zero = jnp.zeros((own_chans, 1), jnp.float32)
    z_plus = jnp.concatenate([fz[:, :half], zero], axis=1).T
    z_minus = jnp.concatenate([zero, fz[:, half:][:, ::-1]], axis=1).T
    weight = z_plus[:, :, None] * plane_a[None] + z_minus[:, :, None] * plane_b[None]
    weight = weight.reshape(kept * own_chans, kx * ky)
    real, imag = real * weight, imag * weight

    cos_x, sin_x = trig(nx, freqs(nx, kx), me_sub * x_local + jnp.arange(x_local))
    c, s = kron_pair(cos_x, sin_x, cos_y, sin_y)

    def columns(t):
        t = t.reshape(x_local, wide_count, y_local, kx * ky)
        return t.transpose(3, 1, 0, 2).reshape(kx * ky, wide_count * cells)

    c, s = columns(c), columns(s)
    table_re = jnp.concatenate([c, -s])
    table_im = jnp.concatenate([s, c])
    both = jnp.concatenate([real, imag], axis=1)
    back = jnp.stack(
        [jnp.dot(both, table_re, precision=HIGH), jnp.dot(both, table_im, precision=HIGH)]
    )
    back = back.reshape(2 * kept, own_chans, wide_count, cells)
    back = back.transpose(2, 1, 0, 3).reshape(wide_count * own_chans, 2 * kept * cells)
    back, spatial = lax.optimization_barrier((back, spatial))
    back = lax.all_to_all(back, WIDE, split_axis=0, concat_axis=0, tiled=True)
    back = back.reshape(chans, 2 * kept, cells)
    mixed = jnp.einsum("oi,irp->opr", mix_weight, back, precision=HIGH)

    inverse_z = jnp.concatenate([cos_z, -sin_z])
    spatial = spatial.reshape(chans, cells, nz)
    block = 8 if cells % 8 == 0 else cells
    steps = cells // block
    cube = pl.BlockSpec((chans, block, nz), lambda i: (0, i, 0))
    whole = lambda *shape: pl.BlockSpec(shape, lambda i: (0,) * len(shape))
    sizes = (lax.axis_size("sp"), narrow_count, lax.axis_size("rep"))
    count = sizes[0] * sizes[1] * sizes[2]
    summed, stats = pl.pallas_call(
        functools.partial(sum_kernel, sizes),
        grid=(steps,),
        out_shape=(
            jax.ShapeDtypeStruct(spatial.shape, jnp.float32),
            jax.ShapeDtypeStruct((8, 128), jnp.float32),
        ),
        in_specs=[
            cube,
            pl.BlockSpec((chans, block, 2 * kept), lambda i: (0, i, 0)),
            whole(2 * kept, nz),
        ],
        out_specs=(cube, whole(8, 128)),
        scratch_shapes=[pltpu.VMEM((chans, block, nz), jnp.float32)] * 2
        + [
            pltpu.VMEM((count, 8, 128), jnp.float32),
            pltpu.SemaphoreType.DMA((count,)),
            pltpu.SemaphoreType.DMA((count,)),
        ],
        compiler_params=pltpu.CompilerParams(collective_id=0, has_side_effects=True),
        name="sum_stats",
    )(spatial, mixed, inverse_z)

    size = chans // GROUPS
    stats = stats[:2, :GROUPS]
    cells_group = size * nx * ny * nz
    group_mean = stats[0] / cells_group
    group_var = stats[1] / cells_group - group_mean * group_mean
    scale = jnp.repeat(lax.rsqrt(group_var + 1e-05), size) * norm_gain
    mean = jnp.repeat(group_mean, size)
    vec = jnp.stack([mean, scale, norm_bias, b_in, b_out] + [b_out] * 3, axis=1)

    result = pl.pallas_call(
        mlp_kernel,
        grid=(steps,),
        out_shape=jax.ShapeDtypeStruct(spatial.shape, jnp.float32),
        in_specs=[cube, whole(chans, 8), whole(*w_in.shape), whole(*w_out.shape)],
        out_specs=cube,
        name="mlp",
    )(summed, vec, w_in, w_out)
    return result.reshape(chans, x_local, y_local, nz)


MESH = pl.DeviceIdType.MESH
LANES = 128
AHEAD = 3


def cosine(index, length):
    fold = jnp.abs(index.astype(jnp.float32) * (2.0 / length) - 1.0)
    near = jnp.minimum(fold, 1.0 - fold) * math.pi
    square = near * near
    total = jnp.full_like(square, 1.0 / math.factorial(14))
    for power in range(6, -1, -1):
        term = 1.0 / math.factorial(2 * power)
        total = term - square * total
    return jnp.where(fold > 0.5, total, -total)


def log2(value):
    return value.bit_length() - 1


def split3(value):
    high = value.astype(jnp.bfloat16)
    rest = value - high.astype(jnp.float32)
    mid = rest.astype(jnp.bfloat16)
    low = (rest - mid.astype(jnp.float32)).astype(jnp.bfloat16)
    return high, mid, low


def pick(left, right):
    d = functools.partial(jnp.dot, preferred_element_type=jnp.float32)
    a, b, c = split3(right)
    return d(left, a) + (d(left, b) + d(left, c))


def pick_right(left, right):
    d = functools.partial(jnp.dot, preferred_element_type=jnp.float32)
    a, b, c = split3(left)
    return d(a, right) + (d(b, right) + d(c, right))


def iota(shape, axis):
    return lax.broadcasted_iota(jnp.int32, shape, axis)


def fused_kernel(
    dims,
    field_ref, mix_ref, w_in_ref, w_out_ref, fx_ref, fy_ref, fz_ref, gain_ref, bias_ref, b_in_ref, b_out_ref,
    out_ref,
    fld, mats, facs, vecs, g_hi, g_lo, gi_hi, gi_lo, yf_hi, yf_lo, yi_hi, yi_lo, xt_hi, xt_lo, fxs, uv, fy_t, fz_t,
    se, sh, lf, re, rh, pin, mid, bs, lb, ls, rb, rl, held, cols,
    fld_sem, par_sem, own_sem, e_send, e_recv, h_send, h_recv, x_send, x_recv, b_send, b_recv, l_send, l_recv,
    t_send, t_recv,
):
    n_sp, n_sub, n_rep, n_freq = dims
    wide = n_sp * n_rep
    count = wide * n_sub
    own, xy_rows, nz = field_ref.shape
    chans = own * wide
    parts, x_local, _, _ = se.shape[1:]
    y_local = LANES // (nz // (2 * parts))
    width = LANES // y_local
    nx = pin.shape[1]
    ny = xy_rows // x_local
    kz = n_freq
    half = kz // 2
    chain = own // n_sub
    sub8 = chain // 8
    tiles = wide + 1
    ltile = half * ny // LANES
    per_tile = LANES // ny
    lane_y, lane_n = log2(y_local), log2(ny)

    me_sub = lax.axis_index("sub")
    me_wide = lax.axis_index("sp") * n_rep + lax.axis_index("rep")
    me = me_wide * n_sub + me_sub

    def place(w, s):
        return {"sp": w // n_rep, "sub": s, "rep": w % n_rep}

    def place_flat(index):
        return place(index // n_sub, index % n_sub)

    def loop(n, body):
        def step(i, carry):
            body(i)
            return carry

        lax.fori_loop(0, n, step, 0)

    barrier = pltpu.get_barrier_semaphore()

    def greet(k, carry):
        pl.semaphore_signal(barrier, inc=1, device_id=place_flat((me + k) % count), device_id_type=MESH)
        return carry

    lax.fori_loop(1, count, greet, 0)

    xchunks = fld_sem.shape[0]
    xc_size = x_local // xchunks

    def fetch(i):
        rows = pl.ds(i * (xc_size * ny), xc_size * ny)
        return pltpu.make_async_copy(field_ref.at[:, rows], fld.at[:, rows], fld_sem.at[i])

    for i in range(xchunks):
        fetch(i).start()
    params = [(mix_ref, mats.at[0]), (w_in_ref, mats.at[1]), (w_out_ref, mats.at[2])]
    params += [(fx_ref, facs.at[0]), (fy_ref, facs.at[1]), (fz_ref, facs.at[2])]
    params += [(gain_ref, vecs.at[0]), (bias_ref, vecs.at[1]), (b_in_ref, vecs.at[2]), (b_out_ref, vecs.at[3])]
    param_copies = [pltpu.make_async_copy(a, b, par_sem.at[i]) for i, (a, b) in enumerate(params)]
    for copy in param_copies:
        copy.start()

    def coef(j):
        low_k = jnp.where(j == 1, half, j >> 1)
        low_s = jnp.where(j == 1, 0, j & 1)
        high_k = (j + 1) >> 1
        high_s = 1 - (j & 1)
        return jnp.where(j < kz, low_k, high_k), jnp.where(j < kz, low_s, high_s)

    def basis(j, z):
        k, s = coef(j)
        value = cosine((k * z + s * (3 * nz // 4)) & (nz - 1), nz)
        edge = (k == 0) | (k == nz // 2)
        return value * jnp.where(edge, math.sqrt(1.0 / nz), math.sqrt(2.0 / nz))

    def g_entry(rows, columns):
        y_in, z = rows >> log2(nz), rows & (nz - 1)
        j, y_out = columns >> lane_y, columns & (y_local - 1)
        return jnp.where(y_in == y_out, basis(j, z), 0.0)

    size = nz * y_local
    stepr = LANES

    def build_g(i):
        rows = pl.ds(pl.multiple_of(i * stepr, stepr), stepr)
        a = iota((stepr, size), 0) + i * stepr
        b = iota((stepr, size), 1)
        g_hi[rows], g_lo[rows] = split(g_entry(a, b))
        gi_hi[rows], gi_lo[rows] = split(g_entry(b, a))

    loop(size // stepr, build_g)

    lane = iota((1, LANES), 1)

    def e_copy(xc, k):
        w = (me_wide + k) % wide
        xs = pl.ds(xc * xc_size, xc_size)
        return pltpu.make_async_remote_copy(
            src_ref=se.at[w, :, xs],
            dst_ref=re.at[:, xs, pl.ds(pl.multiple_of(me_wide * own, own), own)],
            send_sem=e_send.at[xc, k],
            recv_sem=e_recv.at[xc, k],
            device_id=place(w, me_sub),
            device_id_type=MESH,
        )

    hchunks = h_send.shape[0]
    hc_size = x_local // hchunks

    def h_copy(hc, k):
        w = (me_wide + k) % wide
        xs = pl.ds(hc * hc_size, hc_size)
        return pltpu.make_async_remote_copy(
            src_ref=sh.at[w, xs],
            dst_ref=rh.at[xs, :, pl.ds(pl.multiple_of(me_wide * own, own), own)],
            send_sem=h_send.at[hc, k],
            recv_sem=h_recv.at[hc, k],
            device_id=place(w, me_sub),
            device_id_type=MESH,
        )

    def peers(make, what, n=wide):
        def step(k, carry):
            getattr(make(k), what)()
            return carry

        lax.fori_loop(1, n, step, 0)

    zero = jnp.zeros((own, LANES), jnp.float32)

    def transform(xc, squares):
        fetch(xc).wait()

        def one(d, carry):
            left, sq = carry
            groups = []
            for xi in range(xc_size):
                row = (xc * xc_size + xi) * ny + d * y_local
                groups.append(jnp.concatenate([fld[:, row + y, :] for y in range(y_local)], axis=1))
            value = jnp.concatenate(groups, axis=0)
            res = dot3(split(value), (g_hi[...], g_lo[...]))
            cube = res.reshape(xc_size, own, size)
            xs = pl.ds(xc * xc_size, xc_size)
            for g in range(parts):
                se[d, g, xs] = cube[:, :, g * LANES : (g + 1) * LANES]
                part = cube[:, :, (parts + g) * LANES : (parts + g + 1) * LANES]
                sh[d, xs, g] = part
                sq = sq + jnp.sum(part * part, axis=0)
            more = pltpu.roll(res[:, LANES : 2 * LANES], d * y_local, axis=1)
            left = jnp.where((lane >> lane_y) == d, more, left)
            return left, sq

        left = jnp.zeros((xc_size * own, LANES), jnp.float32)
        left, squares = lax.fori_loop(0, wide, one, (left, squares))
        lf[pl.ds(xc * xc_size, xc_size)] = left.reshape(xc_size, own, LANES)

        @pl.when(xc == 1)
        def _():
            pl.semaphore_wait(barrier, count - 1)

        @pl.when(xc >= 1)
        def _():
            peers(lambda k: e_copy(xc - 1, k), "start")

        return squares

    squares = lax.fori_loop(0, xchunks, transform, zero)
    for copy in param_copies:
        copy.wait()

    def x_src(t, s):
        cs = pl.ds(pl.multiple_of(s * chain, 8), chain)
        return se.at[t, 0, :, cs] if t < wide else lf.at[:, cs]

    def x_dst(t):
        return pin.at[t, pl.ds(me_sub * x_local, x_local)]

    x_copies = []
    for t in range(tiles):
        for k in range(1, n_sub):
            s = (me_sub + k) % n_sub
            x_copies.append(
                pltpu.make_async_remote_copy(
                    src_ref=x_src(t, s),
                    dst_ref=x_dst(t),
                    send_sem=x_send.at[t, k],
                    recv_sem=x_recv.at[t, k],
                    device_id=place(me_wide, s),
                    device_id_type=MESH,
                )
            )
    own_chan = pl.ds(pl.multiple_of(me_wide * own, own), own)
    own_copies = [pltpu.make_async_copy(x_src(t, me_sub), x_dst(t), own_sem.at[t]) for t in range(tiles)]
    own_copies.append(pltpu.make_async_copy(se.at[me_wide], re.at[:, :, own_chan], own_sem.at[tiles]))
    own_copies.append(pltpu.make_async_copy(sh.at[me_wide], rh.at[:, :, own_chan], own_sem.at[tiles + 1]))

    def p_meta(t, r):
        jj = r >> lane_y
        k = jnp.where(jj == 1, half, jj >> 1)
        s = jnp.where(jj == 1, 0, jj & 1)
        y = t * y_local + (r & (y_local - 1))
        rest = t == wide
        k = jnp.where(rest, jnp.where(r < ny, half, -1), k)
        return k, jnp.where(rest, 1, s), jnp.where(rest, r, y)

    def m_meta(t, c):
        part = jnp.where(t >= ltile, 1, 0)
        k = (t - part * ltile) * per_tile + (c >> lane_n)
        rest = t == 2 * ltile
        seat = c & (LANES // 2 - 1)
        k = jnp.where(rest, jnp.where(seat < ny, half, -2), k)
        part = jnp.where(rest, c >> log2(LANES // 2), part)
        return k, part, c & (ny - 1)

    def y_entry(pt, mt, p, m, power):
        kp, s, y = p_meta(pt, p)
        km, part, b = m_meta(mt, m)
        value = cosine((y * b + (ny // 4) * (s + part)) & (ny - 1), ny)
        norm = jnp.where(km == 0, math.sqrt(1.0 / nz), math.sqrt(2.0 / nz))
        scale = norm if power else 1.0 / norm
        if not power:
            scale = scale * (1.0 / nz)
        else:
            scale = 1.0 / scale
        return jnp.where(kp == km, value * scale, 0.0)

    square = (LANES, LANES)
    mtiles = 2 * ltile + 1

    def build_y(i):
        rows = pl.ds(pl.multiple_of(i * LANES, LANES), LANES)
        for t in range(mtiles):
            cut = slice(t * LANES, (t + 1) * LANES)
            a, b = iota(square, 0), iota(square, 1)
            yf_hi[rows, cut], yf_lo[rows, cut] = split(y_entry(i, t, a, b, False))
            yi_hi[rows, cut], yi_lo[rows, cut] = split(y_entry(t, i, b, a, True))

    def build_x(i):
        shape = (LANES, nx * 8)
        row = iota(shape, 0) + i * LANES
        col = iota(shape, 1)
        part = row >> log2(nx * 8)
        a = (row >> 3) & (nx - 1)
        value = cosine(((a * (col >> 3)) + part * (3 * nx // 4)) & (nx - 1), nx)
        value = jnp.where((row & 7) == (col & 7), value, 0.0)
        rows = pl.ds(pl.multiple_of(i * LANES, LANES), LANES)
        xt_hi[rows], xt_lo[rows] = split(value)

    peers(lambda k: e_copy(xchunks - 1, k), "start")
    for copy in x_copies:
        copy.start()
    for copy in own_copies:
        copy.start()
    loop(tiles, build_y)
    loop(2 * nx * 8 // LANES, build_x)

    fy_t[...] = jnp.transpose(facs[1])
    fz_t[...] = jnp.transpose(facs[2])
    first = me_wide * own + me_sub * chain
    bf = jnp.bfloat16
    one_hot = lambda mask: jnp.where(mask, 1.0, 0.0).astype(bf)
    for h in range(sub8):
        base = pl.multiple_of(first + 8 * h, 8)
        a = iota((nx * 8, nx), 0) >> 3
        b = iota((nx * 8, nx), 1)
        mask = iota((nx * 8, chans), 1) == first + 8 * h + (iota((nx * 8, chans), 0) & 7)
        for sign in range(2):
            want = a if sign == 0 else (nx - a) & (nx - 1)
            spread = pick(one_hot(b == want), facs[0])
            column = jnp.sum(jnp.where(mask, spread, 0.0), axis=1, keepdims=True)
            fxs[h, sign] = jnp.broadcast_to(column * (1.0 / (nx * ny)), (nx * 8, LANES))
        fz8, fy8 = fz_t[pl.ds(base, 8), :], fy_t[pl.ds(base, 8), :]
        for t in range(ltile + 1):
            i = iota((kz, LANES), 0)
            seat = iota((kz, LANES), 1)
            k = t * per_tile + (seat >> lane_n) if t < ltile else half
            bb = seat & (ny - 1)
            plus = one_hot(i == (k if t < ltile else -1))
            minus = one_hot((i == kz - k) & (k > 0)) if t < ltile else one_hot(i == half)
            yp, ym = one_hot(i == bb), one_hot(i == ((ny - bb) & (ny - 1)))
            uv[h, 0, t] = pick_right(fz8, plus) * pick_right(fy8, yp)
            uv[h, 1, t] = pick_right(fz8, minus) * pick_right(fy8, ym)

    for copy in own_copies:
        copy.wait()
    for copy in x_copies:
        copy.wait()

    rows8 = nx * 8

    def forward_y(h):
        cs = pl.ds(pl.multiple_of(h * 8, 8), 8)
        value = jnp.concatenate([pin[t, :, cs, :].reshape(rows8, LANES) for t in range(tiles)], axis=1)
        res = dot3(split(value), (yf_hi[...], yf_lo[...]))
        for t in range(mtiles):
            mid[h, t] = res[:, t * LANES : (t + 1) * LANES]

    loop(sub8, forward_y)

    def weights(h, t):
        u = jnp.broadcast_to(uv[h, 0, t][None], (nx, 8, LANES)).reshape(rows8, LANES)
        v = jnp.broadcast_to(uv[h, 1, t][None], (nx, 8, LANES)).reshape(rows8, LANES)
        return fxs[h, 0] * u + fxs[h, 1] * v

    def along_x(value):
        return dot3((xt_hi[...], xt_lo[...]), split(value))

    def pair_x(i):
        h, t = i // ltile, i % ltile
        res = along_x(jnp.concatenate([mid[h, t], mid[h, ltile + t]], axis=1))
        c_re, c_im = res[:rows8, :LANES], res[:rows8, LANES:]
        s_re, s_im = res[rows8:, :LANES], res[rows8:, LANES:]
        w = weights(h, t)
        res = along_x(jnp.concatenate([(c_re + s_im) * w, (c_im - s_re) * w], axis=1))
        c_re, c_im = res[:rows8, :LANES], res[:rows8, LANES:]
        s_re, s_im = res[rows8:, :LANES], res[rows8:, LANES:]
        mid[h, t] = c_re - s_im
        mid[h, ltile + t] = c_im + s_re

    loop(sub8 * ltile, pair_x)

    def rest_x(h):
        sign = jnp.where(lane < LANES // 2, 1.0, -1.0)
        res = along_x(mid[h, 2 * ltile])
        modes = res[:rows8] + sign * pltpu.roll(res[rows8:], LANES // 2, axis=1)
        res = along_x(modes * weights(h, ltile))
        mid[h, 2 * ltile] = res[:rows8] - sign * pltpu.roll(res[rows8:], LANES // 2, axis=1)

    loop(sub8, rest_x)

    def back_y(h):
        cs = pl.ds(pl.multiple_of(h * 8, 8), 8)
        value = jnp.concatenate([mid[h, t] for t in range(mtiles)], axis=1)
        res = dot3(split(value), (yi_hi[...], yi_lo[...]))
        for t in range(tiles):
            cut = res[:, t * LANES : (t + 1) * LANES].reshape(nx, 8, LANES)
            if t < wide:
                bs[t, :, cs, :] = cut
            else:
                lb[:, cs, :] = cut

    loop(sub8, back_y)

    def gather_rest(s):
        def one(x, carry):
            value = lb[s * x_local + x]
            new = []
            for d in range(wide):
                moved = pltpu.roll(value, ((x - d) * y_local + LANES) & (LANES - 1), axis=1)
                new.append(jnp.where((lane >> lane_y) == x, moved, carry[d]))
            return tuple(new)

        start = tuple(jnp.zeros((chain, LANES), jnp.float32) for _ in range(wide))
        done = lax.fori_loop(0, x_local, one, start)
        for d in range(wide):
            ls[s, d] = done[d]

    loop(n_sub, gather_rest)

    b_rows = pl.ds(pl.multiple_of(first, 8), chain)

    def b_copy(k):
        index = (me + k) % count
        w, s = index // n_sub, index % n_sub
        return pltpu.make_async_remote_copy(
            src_ref=bs.at[w, pl.ds(s * x_local, x_local)],
            dst_ref=rb.at[:, b_rows],
            send_sem=b_send.at[k],
            recv_sem=b_recv.at[k],
            device_id=place(w, s),
            device_id_type=MESH,
        )

    def l_copy(k):
        index = (me + k) % count
        w, s = index // n_sub, index % n_sub
        return pltpu.make_async_remote_copy(
            src_ref=ls.at[s, w],
            dst_ref=rl.at[b_rows],
            send_sem=l_send.at[k],
            recv_sem=l_recv.at[k],
            device_id=place(w, s),
            device_id_type=MESH,
        )

    peers(b_copy, "start", count)
    own_b = pltpu.make_async_copy(bs.at[me_wide, pl.ds(me_sub * x_local, x_local)], rb.at[:, b_rows], b_send.at[0])
    own_l = pltpu.make_async_copy(ls.at[me_sub, me_wide], rl.at[b_rows], l_send.at[0])
    own_b.start()
    own_l.start()
    peers(l_copy, "start", count)
    loop(AHEAD, lambda hc: peers(lambda k: h_copy(hc, k), "start"))

    eye = iota((chans, chans), 0) == iota((chans, chans), 1)
    for i in range(4):
        column = jnp.sum(jnp.where(eye, vecs[i], 0.0), axis=1, keepdims=True)
        cols[i] = jnp.broadcast_to(column, (chans, LANES))

    own_b.wait()
    own_l.wait()
    peers(b_copy, "wait", count)
    peers(l_copy, "wait", count)
    loop(xchunks, lambda xc: peers(lambda k: e_copy(xc, k), "wait"))
    mix = split(mats[0])
    rest = dot3(mix, split(rl[...]))
    lows = lane < y_local
    blank = jnp.zeros((chans, LANES), jnp.float32)

    def low(i, carry):
        one, two = carry
        spectral = dot3(mix, split(jnp.concatenate([rb[2 * i], rb[2 * i + 1]], axis=1)))
        for j in range(2):
            x = 2 * i + j
            value = re[0, x] + spectral[:, j * LANES : (j + 1) * LANES]
            re[0, x] = value
            one = one + jnp.where(lows, value, 0.0)
            two = two + value * value
            moved = pltpu.roll(rest, (LANES - x * y_local) & (LANES - 1), axis=1)
            value = re[1, x] + jnp.where(lows, moved, 0.0)
            re[1, x] = value
            two = two + value * value
        return one, two

    one, two = lax.fori_loop(0, x_local // 2, low, (blank, blank))

    per_group = chans // GROUPS

    def row(acc, base):
        groups = acc.shape[0] // per_group
        per = jnp.sum(acc.reshape(groups, per_group, LANES), axis=1)
        per = jnp.broadcast_to(jnp.sum(per, axis=1, keepdims=True), (groups, LANES))
        seat = iota((groups, LANES), 1) == iota((groups, LANES), 0) + base
        return jnp.sum(jnp.where(seat, per, 0.0), axis=0, keepdims=True)

    tile = iota((8, LANES), 0)
    sum_one = row(one, 0) * math.sqrt(nz)
    sum_two = row(two, 0) + row(squares, me_wide * (own // per_group))
    held[0] = jnp.where(tile == 0, sum_one, jnp.where(tile == 1, sum_two, 0.0))

    def t_copy(k):
        return pltpu.make_async_remote_copy(
            src_ref=held.at[0],
            dst_ref=held.at[k],
            send_sem=t_send.at[k],
            recv_sem=t_recv.at[k],
            device_id=place_flat((me + k) % count),
            device_id_type=MESH,
        )

    peers(t_copy, "start", count)
    peers(t_copy, "wait", count)
    total = jnp.sum(held[...], axis=0)
    cells_group = per_group * nx * ny * nz
    group_mean = total[0:1] / cells_group
    group_var = total[1:2] / cells_group - group_mean * group_mean
    group_scale = lax.rsqrt(group_var + 1e-05)
    seat = iota((chans, LANES), 1) == iota((chans, LANES), 0) // per_group

    def column_of(value):
        return jnp.sum(jnp.where(seat, value, 0.0), axis=1, keepdims=True)

    scale = column_of(group_scale) * cols[0, :, 0:1]
    shift = cols[1, :, 0:1] - column_of(group_mean) * scale
    cols[4] = jnp.broadcast_to(scale, (chans, LANES))
    cols[5] = jnp.broadcast_to(shift, (chans, LANES))

    def late(hc, carry):
        peers(lambda k: h_copy(hc, k), "wait")

        @pl.when(hc + AHEAD < hchunks)
        def _():
            peers(lambda k: h_copy(hc + AHEAD, k), "start")

        w_in, w_out = split(mats[1]), split(mats[2])
        factor, offset = cols[4, :, 0:1], cols[5, :, 0:1]
        b_in, b_out = cols[2, :, 0:1], cols[3, :, 0:1]
        for j in range(hc_size):
            x = hc * hc_size + j
            value = jnp.concatenate([re[g, x] for g in range(parts)] + [rh[x, g] for g in range(parts)], axis=1)
            value = dot3(split(value), (gi_hi[...], gi_lo[...]))
            normed = value * factor + offset
            hidden = dot3(w_in, split(normed)) + b_in
            inner = math.sqrt(2.0 / math.pi) * (hidden + 0.044715 * (hidden * hidden * hidden))
            hidden = hidden * (0.5 * (1.0 + jnp.tanh(inner)))
            result = value + dot3(w_out, split(hidden)) + b_out
            for y in range(y_local):
                out_ref[:, x * y_local + y, :] = result[:, y * nz : (y + 1) * nz]
        return carry

    lax.fori_loop(0, hchunks, late, 0)


def fused(
    field, mix_weight, factor_x, factor_y, factor_z, norm_gain, norm_bias, w_in, b_in, w_out, b_out
):
    n_sp, n_sub, n_rep = (lax.axis_size(a) for a in ("sp", "sub", "rep"))
    wide, count = n_sp * n_rep, n_sp * n_rep * n_sub
    own, x_local, ny, nz = field.shape
    chans, nx, y_local = own * wide, x_local * n_sub, ny // wide
    kz = factor_z.shape[1]
    chain = own // n_sub
    sub8 = chain // 8
    tiles = wide + 1
    ltile = kz // 2 * ny // LANES
    mtiles = 2 * ltile + 1
    parts = nz * y_local // LANES // 2
    size = nz * y_local
    xchunks, hchunks = 4, x_local * y_local // 8
    f32, bf = jnp.float32, jnp.bfloat16
    vmem = lambda *shape: pltpu.VMEM(shape, f32)
    table = lambda *shape: pltpu.VMEM(shape, bf)
    dma = lambda *shape: pltpu.SemaphoreType.DMA(shape)
    scratch = [
        vmem(own, x_local * ny, nz), vmem(3, chans, chans), vmem(3, kz, chans), vmem(4, 1, chans),
        table(size, size), table(size, size), table(size, size), table(size, size),
        table(tiles * LANES, mtiles * LANES), table(tiles * LANES, mtiles * LANES),
        table(mtiles * LANES, tiles * LANES), table(mtiles * LANES, tiles * LANES),
        table(2 * nx * 8, nx * 8), table(2 * nx * 8, nx * 8),
        vmem(sub8, 2, nx * 8, LANES), vmem(sub8, 2, ltile + 1, 8, LANES), vmem(chans, kz), vmem(chans, kz),
        vmem(wide, parts, x_local, own, LANES), vmem(wide, x_local, parts, own, LANES), vmem(x_local, own, LANES),
        vmem(parts, x_local, chans, LANES), vmem(x_local, parts, chans, LANES),
        vmem(tiles, nx, chain, LANES), vmem(sub8, mtiles, nx * 8, LANES),
        vmem(wide, nx, chain, LANES), vmem(nx, chain, LANES), vmem(n_sub, wide, chain, LANES),
        vmem(x_local, chans, LANES), vmem(chans, LANES), vmem(count, 8, LANES), vmem(6, chans, LANES),
        dma(xchunks), dma(10), dma(tiles + 2), dma(xchunks, wide), dma(xchunks, wide), dma(hchunks, wide),
        dma(hchunks, wide), dma(tiles, n_sub), dma(tiles, n_sub), dma(count), dma(count), dma(count), dma(count),
        dma(count), dma(count),
    ]
    any_spec = pl.BlockSpec(memory_space=pl.ANY)
    line = lambda v: v.reshape(1, chans)
    result = pl.pallas_call(
        functools.partial(fused_kernel, (n_sp, n_sub, n_rep, kz)),
        out_shape=pltpu.VMEM((chans, x_local * y_local, nz), f32),
        in_specs=[any_spec] * 11,
        out_specs=pl.BlockSpec(memory_space=pltpu.VMEM),
        scratch_shapes=scratch,
        compiler_params=pltpu.CompilerParams(
            collective_id=0, has_side_effects=True, vmem_limit_bytes=VMEM_LIMIT
        ),
        name="fused",
    )(
        field.reshape(own, x_local * ny, nz), mix_weight, w_in, w_out, factor_x.T, factor_y.T, factor_z.T,
        line(norm_gain), line(norm_bias), line(b_in), line(b_out),
    )
    return result.reshape(chans, x_local, y_local, nz)


VMEM_LIMIT = 55 * 1024 * 1024


def fits(field, factor_x, factor_y, factor_z):
    n_sub, wide = lax.axis_size("sub"), lax.axis_size(WIDE)
    own, x_local, ny, nz = field.shape
    nx, kz = x_local * n_sub, factor_z.shape[1]
    power = all(v & (v - 1) == 0 for v in (nx, ny, nz, kz))
    if not power or nz != LANES or factor_x.shape[1] != nx or factor_y.shape[1] != ny or ny % wide:
        return False
    y_local = ny // wide
    return (
        kz * y_local == LANES
        and nz == 4 * kz
        and nx == kz == ny
        and own % (8 * n_sub) == 0
        and own % (own * wide // GROUPS) == 0
        and x_local * y_local <= LANES
        and x_local % 4 == 0
        and 8 % y_local == 0
        and (kz // 2 * ny) % LANES == 0
    )


def local(
    field, mix_weight, factor_x, factor_y, factor_z, norm_gain, norm_bias, w_in, b_in, w_out, b_out
):
    run = fused if fits(field, factor_x, factor_y, factor_z) else general
    return run(
        field, mix_weight, factor_x, factor_y, factor_z, norm_gain, norm_bias, w_in, b_in, w_out, b_out
    )


def solution(mesh):
    placed = (P(("grp", "sp", "rep"), "sub", None, None),) + (P(),) * 10
    return jax.shard_map(
        local,
        mesh=mesh,
        in_specs=placed,
        out_specs=P("grp", "sub", ("sp", "rep"), None),
        check_vma=False,
    )
```

```python
import math
import functools

import jax
import jax.numpy as jnp
from jax import lax
from jax.experimental import pallas as pl
from jax.experimental.pallas import tpu as pltpu
from jax.sharding import PartitionSpec as P

GROUPS = 32
HIGH = lax.Precision.HIGH
WIDE = ("sp", "rep")


def trig(length, freq, positions):
    phases = (freq[:, None] * positions[None, :]) % length
    angles = 2.0 * math.pi / length * phases.astype(jnp.float32)
    return jnp.cos(angles), jnp.sin(angles)


def kron_pair(cos_a, sin_a, cos_b, sin_b):
    ca, sa = cos_a.T[:, None, :, None], sin_a.T[:, None, :, None]
    cb, sb = cos_b.T[None, :, None, :], sin_b.T[None, :, None, :]
    return ca * cb - sa * sb, sa * cb + ca * sb


def split(value):
    high = value.astype(jnp.bfloat16)
    low = (value - high.astype(jnp.float32)).astype(jnp.bfloat16)
    return high, low


def dot3(left, right):
    lh, ll = left
    rh, rl = right
    d = functools.partial(jnp.dot, preferred_element_type=jnp.float32)
    return d(lh, rh) + (d(lh, rl) + d(ll, rh))


def sum_kernel(
    sizes, field_ref, modes_ref, table_ref, summed_ref, total_ref, acc1, acc2, held, send_sem, recv_sem
):
    step = pl.program_id(0)
    n_sp, n_sub, n_rep = sizes
    count = n_sp * n_sub * n_rep
    me = (lax.axis_index("sp") * n_sub + lax.axis_index("sub")) * n_rep + lax.axis_index("rep")

    def place(index):
        return {
            "sp": index // (n_sub * n_rep),
            "sub": (index // n_rep) % n_sub,
            "rep": index % n_rep,
        }

    @pl.when(step == 0)
    def _():
        barrier = pltpu.get_barrier_semaphore()

        def greet(k, carry):
            pl.semaphore_signal(
                barrier,
                inc=1,
                device_id=place((me + k) % count),
                device_id_type=pl.DeviceIdType.MESH,
            )
            return carry

        lax.fori_loop(1, count, greet, 0)

    chans, cells, width = field_ref.shape
    rank = modes_ref.shape[2]

    @pl.when(step == 0)
    def _():
        acc1[...] = jnp.zeros_like(acc1)
        acc2[...] = jnp.zeros_like(acc2)

    table = split(table_ref[...])
    chunk = 32 if chans % 32 == 0 else chans

    def body(index, carry):
        rows = pl.ds(pl.multiple_of(index * chunk, chunk), chunk)
        modes = modes_ref[rows].reshape(chunk * cells, rank)
        value = dot3(split(modes), table).reshape(chunk, cells, width) + field_ref[rows]
        summed_ref[rows] = value
        acc1[rows] += value
        acc2[rows] += value * value
        return carry

    lax.fori_loop(0, chans // chunk, body, 0)

    @pl.when(step == pl.num_programs(0) - 1)
    def _():
        def row(acc):
            per = jnp.sum(acc[...], axis=1)
            per = jnp.sum(per.reshape(GROUPS, chans // GROUPS, width), axis=1)
            per = jnp.broadcast_to(jnp.sum(per, axis=1, keepdims=True), (GROUPS, 128))
            lanes = lax.broadcasted_iota(jnp.int32, (GROUPS, 128), 1)
            rows = lax.broadcasted_iota(jnp.int32, (GROUPS, 128), 0)
            return jnp.sum(jnp.where(lanes == rows, per, 0.0), axis=0, keepdims=True)

        tile = lax.broadcasted_iota(jnp.int32, (8, 128), 0)
        held[0] = jnp.where(tile == 0, row(acc1), jnp.where(tile == 1, row(acc2), 0.0))
        pl.semaphore_wait(pltpu.get_barrier_semaphore(), count - 1)

        def copy(k):
            return pltpu.make_async_remote_copy(
                src_ref=held.at[0],
                dst_ref=held.at[k],
                send_sem=send_sem.at[k],
                recv_sem=recv_sem.at[k],
                device_id=place((me + k) % count),
                device_id_type=pl.DeviceIdType.MESH,
            )

        def launch(k, carry):
            copy(k).start()
            return carry

        def finish(k, carry):
            copy(k).wait()
            return carry

        lax.fori_loop(1, count, launch, 0)
        lax.fori_loop(1, count, finish, 0)
        total_ref[...] = jnp.sum(held[...], axis=0)


def mlp_kernel(summed_ref, vec_ref, w_in_ref, w_out_ref, out_ref):
    cells = summed_ref.shape[1]
    w_in = split(w_in_ref[...])
    w_out = split(w_out_ref[...])
    vec = vec_ref[...]
    mean, scale, bias = vec[:, 0:1], vec[:, 1:2], vec[:, 2:3]
    b_in, b_out = vec[:, 3:4], vec[:, 4:5]
    pair = 2 if cells % 2 == 0 else 1
    for start in range(0, cells, pair):
        parts = [summed_ref[:, p, :] for p in range(start, start + pair)]
        value = jnp.concatenate(parts, axis=1) if pair > 1 else parts[0]
        normed = (value - mean) * scale + bias
        hidden = dot3(w_in, split(normed)) + b_in
        inner = math.sqrt(2.0 / math.pi) * (hidden + 0.044715 * (hidden * hidden * hidden))
        hidden = hidden * (0.5 * (1.0 + jnp.tanh(inner)))
        result = value + dot3(w_out, split(hidden)) + b_out
        width = summed_ref.shape[2]
        for k in range(pair):
            out_ref[:, start + k, :] = result[:, k * width : (k + 1) * width]


def general(
    field, mix_weight, factor_x, factor_y, factor_z, norm_gain, norm_bias, w_in, b_in, w_out, b_out
):
    wide_count = lax.axis_size(WIDE)
    narrow_count = lax.axis_size("sub")
    own_chans, x_local, ny, nz = field.shape
    chans = own_chans * wide_count
    nx = x_local * narrow_count
    kx, ky, kz = factor_x.shape[1], factor_y.shape[1], factor_z.shape[1]
    y_local = ny // wide_count
    half = kz // 2
    kept = half + 1
    me_sub = lax.axis_index("sub")
    cells = x_local * y_local

    spatial = field.reshape(own_chans, x_local, wide_count, y_local, nz)
    spatial = spatial.transpose(2, 0, 1, 3, 4).reshape(wide_count, own_chans, cells, nz)
    spatial = lax.all_to_all(spatial, WIDE, split_axis=0, concat_axis=0, tiled=True)

    cos_z, sin_z = trig(nz, jnp.arange(kept), jnp.arange(nz))
    forward = jnp.concatenate([cos_z, -sin_z]) / nz
    planes = jnp.einsum("rz,cxyz->rcxy", forward, field, precision=HIGH)
    planes = planes.reshape(2 * kept * own_chans, x_local * ny)

    def freqs(length, count):
        index = jnp.arange(count)
        return jnp.where(index < count // 2, index, length - count + index)

    cos_y, sin_y = trig(ny, freqs(ny, ky), jnp.arange(ny))

    def forward_xy(values, owner):
        cos_x, sin_x = trig(nx, freqs(nx, kx), owner * x_local + jnp.arange(x_local))
        c, s = kron_pair(cos_x, sin_x, cos_y, sin_y)
        c = (c / (nx * ny)).reshape(x_local * ny, kx * ky)
        s = (s / (nx * ny)).reshape(x_local * ny, kx * ky)
        a = jnp.dot(values, jnp.concatenate([c, s], axis=1), precision=HIGH)
        a = a.reshape(2, kept * own_chans, 2, kx * ky)
        return a[0, :, 0] + a[1, :, 1], a[1, :, 0] - a[0, :, 1]

    held = planes
    real, imag = forward_xy(held, me_sub)
    for hop in range(1, narrow_count):
        held = lax.ppermute(held, "sub", [(i, (i + 1) % narrow_count) for i in range(narrow_count)])
        owner = (me_sub - hop + narrow_count) % narrow_count
        more_real, more_imag = forward_xy(held, owner)
        real, imag = real + more_real, imag + more_imag

    start = lax.axis_index(WIDE) * own_chans
    fx = lax.dynamic_slice_in_dim(factor_x, start, own_chans, 0)
    fy = lax.dynamic_slice_in_dim(factor_y, start, own_chans, 0)
    fz = lax.dynamic_slice_in_dim(factor_z, start, own_chans, 0)
    mirror_x = (-jnp.arange(kx)) % kx
    mirror_y = (-jnp.arange(ky)) % ky
    plane_a = (fx[:, :, None] * fy[:, None, :]).reshape(own_chans, kx * ky)
    plane_b = (fx[:, mirror_x][:, :, None] * fy[:, mirror_y][:, None, :]).reshape(own_chans, kx * ky)
    zero = jnp.zeros((own_chans, 1), jnp.float32)
    z_plus = jnp.concatenate([fz[:, :half], zero], axis=1).T
    z_minus = jnp.concatenate([zero, fz[:, half:][:, ::-1]], axis=1).T
    weight = z_plus[:, :, None] * plane_a[None] + z_minus[:, :, None] * plane_b[None]
    weight = weight.reshape(kept * own_chans, kx * ky)
    real, imag = real * weight, imag * weight

    cos_x, sin_x = trig(nx, freqs(nx, kx), me_sub * x_local + jnp.arange(x_local))
    c, s = kron_pair(cos_x, sin_x, cos_y, sin_y)

    def columns(t):
        t = t.reshape(x_local, wide_count, y_local, kx * ky)
        return t.transpose(3, 1, 0, 2).reshape(kx * ky, wide_count * cells)

    c, s = columns(c), columns(s)
    table_re = jnp.concatenate([c, -s])
    table_im = jnp.concatenate([s, c])
    both = jnp.concatenate([real, imag], axis=1)
    back = jnp.stack(
        [jnp.dot(both, table_re, precision=HIGH), jnp.dot(both, table_im, precision=HIGH)]
    )
    back = back.reshape(2 * kept, own_chans, wide_count, cells)
    back = back.transpose(2, 1, 0, 3).reshape(wide_count * own_chans, 2 * kept * cells)
    back, spatial = lax.optimization_barrier((back, spatial))
    back = lax.all_to_all(back, WIDE, split_axis=0, concat_axis=0, tiled=True)
    back = back.reshape(chans, 2 * kept, cells)
    mixed = jnp.einsum("oi,irp->opr", mix_weight, back, precision=HIGH)

    inverse_z = jnp.concatenate([cos_z, -sin_z])
    spatial = spatial.reshape(chans, cells, nz)
    block = 8 if cells % 8 == 0 else cells
    steps = cells // block
    cube = pl.BlockSpec((chans, block, nz), lambda i: (0, i, 0))
    whole = lambda *shape: pl.BlockSpec(shape, lambda i: (0,) * len(shape))
    sizes = (lax.axis_size("sp"), narrow_count, lax.axis_size("rep"))
    count = sizes[0] * sizes[1] * sizes[2]
    summed, stats = pl.pallas_call(
        functools.partial(sum_kernel, sizes),
        grid=(steps,),
        out_shape=(
            jax.ShapeDtypeStruct(spatial.shape, jnp.float32),
            jax.ShapeDtypeStruct((8, 128), jnp.float32),
        ),
        in_specs=[
            cube,
            pl.BlockSpec((chans, block, 2 * kept), lambda i: (0, i, 0)),
            whole(2 * kept, nz),
        ],
        out_specs=(cube, whole(8, 128)),
        scratch_shapes=[pltpu.VMEM((chans, block, nz), jnp.float32)] * 2
        + [
            pltpu.VMEM((count, 8, 128), jnp.float32),
            pltpu.SemaphoreType.DMA((count,)),
            pltpu.SemaphoreType.DMA((count,)),
        ],
        compiler_params=pltpu.CompilerParams(collective_id=0, has_side_effects=True),
        name="sum_stats",
    )(spatial, mixed, inverse_z)

    size = chans // GROUPS
    stats = stats[:2, :GROUPS]
    cells_group = size * nx * ny * nz
    group_mean = stats[0] / cells_group
    group_var = stats[1] / cells_group - group_mean * group_mean
    scale = jnp.repeat(lax.rsqrt(group_var + 1e-05), size) * norm_gain
    mean = jnp.repeat(group_mean, size)
    vec = jnp.stack([mean, scale, norm_bias, b_in, b_out] + [b_out] * 3, axis=1)

    result = pl.pallas_call(
        mlp_kernel,
        grid=(steps,),
        out_shape=jax.ShapeDtypeStruct(spatial.shape, jnp.float32),
        in_specs=[cube, whole(chans, 8), whole(*w_in.shape), whole(*w_out.shape)],
        out_specs=cube,
        name="mlp",
    )(summed, vec, w_in, w_out)
    return result.reshape(chans, x_local, y_local, nz)


MESH = pl.DeviceIdType.MESH
LANES = 128
AHEAD = 4


def cosine(index, length):
    fold = jnp.abs(index.astype(jnp.float32) * (2.0 / length) - 1.0)
    near = jnp.minimum(fold, 1.0 - fold) * math.pi
    square = near * near
    total = jnp.full_like(square, 1.0 / math.factorial(14))
    for power in range(6, -1, -1):
        term = 1.0 / math.factorial(2 * power)
        total = term - square * total
    return jnp.where(fold > 0.5, total, -total)


def log2(value):
    return value.bit_length() - 1


def split3(value):
    high = value.astype(jnp.bfloat16)
    rest = value - high.astype(jnp.float32)
    mid = rest.astype(jnp.bfloat16)
    low = (rest - mid.astype(jnp.float32)).astype(jnp.bfloat16)
    return high, mid, low


def pick(left, right):
    d = functools.partial(jnp.dot, preferred_element_type=jnp.float32)
    a, b, c = split3(right)
    return d(left, a) + (d(left, b) + d(left, c))


def pick_right(left, right):
    d = functools.partial(jnp.dot, preferred_element_type=jnp.float32)
    a, b, c = split3(left)
    return d(a, right) + (d(b, right) + d(c, right))


def iota(shape, axis):
    return lax.broadcasted_iota(jnp.int32, shape, axis)


def fused_kernel(
    dims,
    field_ref, mix_ref, w_in_ref, w_out_ref, fx_ref, fy_ref, fz_ref, gain_ref, bias_ref, b_in_ref, b_out_ref,
    out_ref,
    fld, mats, facs, vecs, g_hi, g_lo, gi_hi, gi_lo, yf_hi, yf_lo, yi_hi, yi_lo, xt_hi, xt_lo, fxs, uv, fy_t, fz_t,
    se, sh, lf, re, rh, pin, mid, bs, lb, ls, rb, rl, held, cols,
    fld_sem, par_sem, own_sem, e_send, e_recv, h_send, h_recv, x_send, x_recv, b_send, b_recv, l_send, l_recv,
    t_send, t_recv,
):
    n_sp, n_sub, n_rep, n_freq = dims
    wide = n_sp * n_rep
    count = wide * n_sub
    own, xy_rows, nz = field_ref.shape
    chans = own * wide
    parts, x_local, _, _ = se.shape[1:]
    y_local = LANES // (nz // (2 * parts))
    width = LANES // y_local
    nx = pin.shape[1]
    ny = xy_rows // x_local
    kz = n_freq
    half = kz // 2
    chain = own // n_sub
    sub8 = chain // 8
    tiles = wide + 1
    ltile = half * ny // LANES
    per_tile = LANES // ny
    lane_y, lane_n = log2(y_local), log2(ny)

    me_sub = lax.axis_index("sub")
    me_sp, me_rep = lax.axis_index("sp"), lax.axis_index("rep")
    me_wide = me_sp * n_rep + me_rep
    me = me_wide * n_sub + me_sub

    def place(w, s):
        return {"sp": w // n_rep, "sub": s, "rep": w % n_rep}

    def place_flat(index):
        return place(index // n_sub, index % n_sub)

    def wide_peer(k):
        return (me_sp + k // n_rep) % n_sp * n_rep + (me_rep + k % n_rep) % n_rep

    def flat_peer(k):
        w = (me_sp + k // (n_rep * n_sub)) % n_sp * n_rep + (me_rep + k % n_rep) % n_rep
        return w, (me_sub + k // n_rep % n_sub) % n_sub

    def turn(i, n):
        near = n // n_sp
        late = i // (n - near)
        return (1 - late) * (near + i) + late * (n - 1 - i)

    def loop(n, body):
        def step(i, carry):
            body(i)
            return carry

        lax.fori_loop(0, n, step, 0)

    barrier = pltpu.get_barrier_semaphore()

    def greet(k, carry):
        pl.semaphore_signal(barrier, inc=1, device_id=place_flat((me + k) % count), device_id_type=MESH)
        return carry

    lax.fori_loop(1, count, greet, 0)

    xchunks = fld_sem.shape[0]
    xc_size = x_local // xchunks

    def fetch(i):
        rows = pl.ds(i * (xc_size * ny), xc_size * ny)
        return pltpu.make_async_copy(field_ref.at[:, rows], fld.at[:, rows], fld_sem.at[i])

    for i in range(xchunks):
        fetch(i).start()
    params = [(mix_ref, mats.at[0]), (w_in_ref, mats.at[1]), (w_out_ref, mats.at[2])]
    params += [(fx_ref, facs.at[0]), (fy_ref, facs.at[1]), (fz_ref, facs.at[2])]
    params += [(gain_ref, vecs.at[0]), (bias_ref, vecs.at[1]), (b_in_ref, vecs.at[2]), (b_out_ref, vecs.at[3])]
    param_copies = [pltpu.make_async_copy(a, b, par_sem.at[i]) for i, (a, b) in enumerate(params)]
    for copy in param_copies:
        copy.start()

    def coef(j):
        low_k = jnp.where(j == 1, half, j >> 1)
        low_s = jnp.where(j == 1, 0, j & 1)
        high_k = (j + 1) >> 1
        high_s = 1 - (j & 1)
        return jnp.where(j < kz, low_k, high_k), jnp.where(j < kz, low_s, high_s)

    def basis(j, z):
        k, s = coef(j)
        value = cosine((k * z + s * (3 * nz // 4)) & (nz - 1), nz)
        edge = (k == 0) | (k == nz // 2)
        return value * jnp.where(edge, math.sqrt(1.0 / nz), math.sqrt(2.0 / nz))

    def g_entry(rows, columns):
        y_in, z = rows >> log2(nz), rows & (nz - 1)
        j, y_out = columns >> lane_y, columns & (y_local - 1)
        return jnp.where(y_in == y_out, basis(j, z), 0.0)

    size = nz * y_local
    stepr = LANES

    def build_g(i):
        rows = pl.ds(pl.multiple_of(i * stepr, stepr), stepr)
        a = iota((stepr, size), 0) + i * stepr
        b = iota((stepr, size), 1)
        g_hi[rows], g_lo[rows] = split(g_entry(a, b))
        gi_hi[rows], gi_lo[rows] = split(g_entry(b, a))

    loop(size // stepr, build_g)

    lane = iota((1, LANES), 1)

    def e_copy(xc, k):
        w = wide_peer(k)
        xs = pl.ds(xc * xc_size, xc_size)
        return pltpu.make_async_remote_copy(
            src_ref=se.at[w, :, xs],
            dst_ref=re.at[:, xs, pl.ds(pl.multiple_of(me_wide * own, own), own)],
            send_sem=e_send.at[xc, k],
            recv_sem=e_recv.at[xc, k],
            device_id=place(w, me_sub),
            device_id_type=MESH,
        )

    hchunks = h_send.shape[0]
    hc_size = x_local // hchunks

    def h_copy(hc, k):
        w = wide_peer(k)
        xs = pl.ds(hc * hc_size, hc_size)
        return pltpu.make_async_remote_copy(
            src_ref=sh.at[w, xs],
            dst_ref=rh.at[xs, :, pl.ds(pl.multiple_of(me_wide * own, own), own)],
            send_sem=h_send.at[hc, k],
            recv_sem=h_recv.at[hc, k],
            device_id=place(w, me_sub),
            device_id_type=MESH,
        )

    def peers(make, what, n=wide):
        def step(i, carry):
            getattr(make(turn(i, n)), what)()
            return carry

        lax.fori_loop(0, n - 1, step, 0)

    zero = jnp.zeros((own, LANES), jnp.float32)

    def transform(xc, squares):
        fetch(xc).wait()

        def one(i, carry):
            left, sq = carry
            d = wide_peer(turn(i, wide))
            groups = []
            for xi in range(xc_size):
                row = (xc * xc_size + xi) * ny + d * y_local
                groups.append(jnp.concatenate([fld[:, row + y, :] for y in range(y_local)], axis=1))
            value = jnp.concatenate(groups, axis=0)
            res = dot3(split(value), (g_hi[...], g_lo[...]))
            cube = res.reshape(xc_size, own, size)
            xs = pl.ds(xc * xc_size, xc_size)
            for g in range(parts):
                se[d, g, xs] = cube[:, :, g * LANES : (g + 1) * LANES]
                part = cube[:, :, (parts + g) * LANES : (parts + g + 1) * LANES]
                sh[d, xs, g] = part
                sq = sq + jnp.sum(part * part, axis=0)
            more = pltpu.roll(res[:, LANES : 2 * LANES], d * y_local, axis=1)
            left = jnp.where((lane >> lane_y) == d, more, left)

            @pl.when(jnp.logical_and(xc == 0, i == 1))
            def _():
                pl.semaphore_wait(barrier, count - 1)

            @pl.when(i >= 1)
            def _():
                e_copy(xc, turn(i - 1, wide)).start()

            return left, sq

        left = jnp.zeros((xc_size * own, LANES), jnp.float32)
        left, squares = lax.fori_loop(0, wide, one, (left, squares))
        lf[pl.ds(xc * xc_size, xc_size)] = left.reshape(xc_size, own, LANES)

        return squares

    squares = lax.fori_loop(0, xchunks, transform, zero)
    for copy in param_copies:
        copy.wait()

    def x_src(t, s):
        cs = pl.ds(pl.multiple_of(s * chain, 8), chain)
        return se.at[t, 0, :, cs] if t < wide else lf.at[:, cs]

    def x_dst(t):
        return pin.at[t, pl.ds(me_sub * x_local, x_local)]

    x_copies = []
    for t in range(tiles):
        for k in range(1, n_sub):
            s = (me_sub + k) % n_sub
            x_copies.append(
                pltpu.make_async_remote_copy(
                    src_ref=x_src(t, s),
                    dst_ref=x_dst(t),
                    send_sem=x_send.at[t, k],
                    recv_sem=x_recv.at[t, k],
                    device_id=place(me_wide, s),
                    device_id_type=MESH,
                )
            )
    own_chan = pl.ds(pl.multiple_of(me_wide * own, own), own)
    own_copies = [pltpu.make_async_copy(x_src(t, me_sub), x_dst(t), own_sem.at[t]) for t in range(tiles)]
    own_copies.append(pltpu.make_async_copy(se.at[me_wide], re.at[:, :, own_chan], own_sem.at[tiles]))
    own_copies.append(pltpu.make_async_copy(sh.at[me_wide], rh.at[:, :, own_chan], own_sem.at[tiles + 1]))

    def p_meta(t, r):
        jj = r >> lane_y
        k = jnp.where(jj == 1, half, jj >> 1)
        s = jnp.where(jj == 1, 0, jj & 1)
        y = t * y_local + (r & (y_local - 1))
        rest = t == wide
        k = jnp.where(rest, jnp.where(r < ny, half, -1), k)
        return k, jnp.where(rest, 1, s), jnp.where(rest, r, y)

    def m_meta(t, c):
        part = jnp.where(t >= ltile, 1, 0)
        k = (t - part * ltile) * per_tile + (c >> lane_n)
        rest = t == 2 * ltile
        seat = c & (LANES // 2 - 1)
        k = jnp.where(rest, jnp.where(seat < ny, half, -2), k)
        part = jnp.where(rest, c >> log2(LANES // 2), part)
        return k, part, c & (ny - 1)

    def y_entry(pt, mt, p, m, forward):
        kp, s, y = p_meta(pt, p)
        km, part, b = m_meta(mt, m)
        value = cosine((y * b + (ny // 4) * (s + part)) & (ny - 1), ny)
        scale = jnp.where(km == 0, math.sqrt(nz), math.sqrt(nz / 2.0))
        if forward:
            scale = scale * (1.0 / nz)
        return jnp.where(kp == km, value * scale, 0.0)

    square = (LANES, LANES)
    mtiles = 2 * ltile + 1

    def build_y(i):
        rows = pl.ds(pl.multiple_of(i * LANES, LANES), LANES)
        for t in range(mtiles):
            cut = slice(t * LANES, (t + 1) * LANES)
            a, b = iota(square, 0), iota(square, 1)
            yf_hi[rows, cut], yf_lo[rows, cut] = split(y_entry(i, t, a, b, True))
            yi_hi[rows, cut], yi_lo[rows, cut] = split(y_entry(t, i, b, a, False))

    def build_x(i):
        shape = (LANES, nx * 8)
        row = iota(shape, 0) + i * LANES
        col = iota(shape, 1)
        part = row >> log2(nx * 8)
        a = (row >> 3) & (nx - 1)
        value = cosine(((a * (col >> 3)) + part * (3 * nx // 4)) & (nx - 1), nx)
        value = jnp.where((row & 7) == (col & 7), value, 0.0)
        rows = pl.ds(pl.multiple_of(i * LANES, LANES), LANES)
        xt_hi[rows], xt_lo[rows] = split(value)

    for copy in x_copies:
        copy.start()
    for copy in own_copies:
        copy.start()
    loop(tiles, build_y)
    loop(2 * nx * 8 // LANES, build_x)

    fy_t[...] = jnp.transpose(facs[1])
    fz_t[...] = jnp.transpose(facs[2])
    first = me_wide * own + me_sub * chain
    bf = jnp.bfloat16
    one_hot = lambda mask: jnp.where(mask, 1.0, 0.0).astype(bf)
    for h in range(sub8):
        base = pl.multiple_of(first + 8 * h, 8)
        a = iota((nx * 8, nx), 0) >> 3
        b = iota((nx * 8, nx), 1)
        mask = iota((nx * 8, chans), 1) == first + 8 * h + (iota((nx * 8, chans), 0) & 7)
        for sign in range(2):
            want = a if sign == 0 else (nx - a) & (nx - 1)
            spread = pick(one_hot(b == want), facs[0])
            column = jnp.sum(jnp.where(mask, spread, 0.0), axis=1, keepdims=True)
            fxs[h, sign] = jnp.broadcast_to(column * (1.0 / (nx * ny)), (nx * 8, LANES))
        fz8, fy8 = fz_t[pl.ds(base, 8), :], fy_t[pl.ds(base, 8), :]
        for t in range(ltile + 1):
            i = iota((kz, LANES), 0)
            seat = iota((kz, LANES), 1)
            k = t * per_tile + (seat >> lane_n) if t < ltile else half
            bb = seat & (ny - 1)
            plus = one_hot(i == (k if t < ltile else -1))
            minus = one_hot((i == kz - k) & (k > 0)) if t < ltile else one_hot(i == half)
            yp, ym = one_hot(i == bb), one_hot(i == ((ny - bb) & (ny - 1)))
            uv[h, 0, t] = pick_right(fz8, plus) * pick_right(fy8, yp)
            uv[h, 1, t] = pick_right(fz8, minus) * pick_right(fy8, ym)

    for copy in own_copies:
        copy.wait()
    for copy in x_copies:
        copy.wait()

    rows8 = nx * 8

    def forward_y(h):
        cs = pl.ds(pl.multiple_of(h * 8, 8), 8)
        value = jnp.concatenate([pin[t, :, cs, :].reshape(rows8, LANES) for t in range(tiles)], axis=1)
        res = dot3(split(value), (yf_hi[...], yf_lo[...]))
        for t in range(mtiles):
            mid[h, t] = res[:, t * LANES : (t + 1) * LANES]

    loop(sub8, forward_y)

    def weights(h, t):
        u = jnp.broadcast_to(uv[h, 0, t][None], (nx, 8, LANES)).reshape(rows8, LANES)
        v = jnp.broadcast_to(uv[h, 1, t][None], (nx, 8, LANES)).reshape(rows8, LANES)
        return fxs[h, 0] * u + fxs[h, 1] * v

    def along_x(value):
        return dot3((xt_hi[...], xt_lo[...]), split(value))

    def pair_x(i):
        h, t = i // ltile, i % ltile
        res = along_x(jnp.concatenate([mid[h, t], mid[h, ltile + t]], axis=1))
        c_re, c_im = res[:rows8, :LANES], res[:rows8, LANES:]
        s_re, s_im = res[rows8:, :LANES], res[rows8:, LANES:]
        w = weights(h, t)
        res = along_x(jnp.concatenate([(c_re + s_im) * w, (c_im - s_re) * w], axis=1))
        c_re, c_im = res[:rows8, :LANES], res[:rows8, LANES:]
        s_re, s_im = res[rows8:, :LANES], res[rows8:, LANES:]
        mid[h, t] = c_re - s_im
        mid[h, ltile + t] = c_im + s_re

    loop(sub8 * ltile, pair_x)

    def rest_x(h):
        sign = jnp.where(lane < LANES // 2, 1.0, -1.0)
        res = along_x(mid[h, 2 * ltile])
        modes = res[:rows8] + sign * pltpu.roll(res[rows8:], LANES // 2, axis=1)
        res = along_x(modes * weights(h, ltile))
        mid[h, 2 * ltile] = res[:rows8] - sign * pltpu.roll(res[rows8:], LANES // 2, axis=1)

    loop(sub8, rest_x)

    def back_y(h):
        cs = pl.ds(pl.multiple_of(h * 8, 8), 8)
        value = jnp.concatenate([mid[h, t] for t in range(mtiles)], axis=1)
        res = dot3(split(value), (yi_hi[...], yi_lo[...]))
        for t in range(tiles):
            cut = res[:, t * LANES : (t + 1) * LANES].reshape(nx, 8, LANES)
            if t < wide:
                bs[t, :, cs, :] = cut
            else:
                lb[:, cs, :] = cut

    loop(sub8, back_y)

    def gather_rest(s):
        def one(x, carry):
            value = lb[s * x_local + x]
            new = []
            for d in range(wide):
                moved = pltpu.roll(value, ((x - d) * y_local + LANES) & (LANES - 1), axis=1)
                new.append(jnp.where((lane >> lane_y) == x, moved, carry[d]))
            return tuple(new)

        start = tuple(jnp.zeros((chain, LANES), jnp.float32) for _ in range(wide))
        done = lax.fori_loop(0, x_local, one, start)
        for d in range(wide):
            other = pltpu.roll(done[d][chain // 2 :], LANES // 2, axis=1)
            ls[s, d] = jnp.where(lane < LANES // 2, done[d][: chain // 2], other)

    loop(n_sub, gather_rest)

    b_rows = pl.ds(pl.multiple_of(first, 8), chain)

    def b_copy(k):
        w, s = flat_peer(k)
        return pltpu.make_async_remote_copy(
            src_ref=bs.at[w, pl.ds(s * x_local, x_local)],
            dst_ref=rb.at[:, b_rows],
            send_sem=b_send.at[k],
            recv_sem=b_recv.at[k],
            device_id=place(w, s),
            device_id_type=MESH,
        )

    def l_copy(k):
        w, s = flat_peer(k)
        return pltpu.make_async_remote_copy(
            src_ref=ls.at[s, w],
            dst_ref=rl.at[me],
            send_sem=l_send.at[k],
            recv_sem=l_recv.at[k],
            device_id=place(w, s),
            device_id_type=MESH,
        )

    peers(b_copy, "start", count)
    own_b = pltpu.make_async_copy(bs.at[me_wide, pl.ds(me_sub * x_local, x_local)], rb.at[:, b_rows], b_send.at[0])
    own_l = pltpu.make_async_copy(ls.at[me_sub, me_wide], rl.at[me], l_send.at[0])
    own_b.start()
    own_l.start()
    peers(l_copy, "start", count)
    loop(AHEAD, lambda hc: peers(lambda k: h_copy(hc, k), "start"))

    eye = iota((chans, chans), 0) == iota((chans, chans), 1)
    for i in range(4):
        column = jnp.sum(jnp.where(eye, vecs[i], 0.0), axis=1, keepdims=True)
        cols[i] = jnp.broadcast_to(column, (chans, LANES))

    own_b.wait()
    own_l.wait()
    peers(b_copy, "wait", count)
    peers(l_copy, "wait", count)
    loop(xchunks, lambda xc: peers(lambda k: e_copy(xc, k), "wait"))
    mix = split(mats[0])
    packed = rl[...].reshape(chans // 2, LANES)
    other = pltpu.roll(packed, LANES // 2, axis=1).reshape(rl.shape)
    rest = jnp.concatenate([rl[...], other], axis=1).reshape(chans, LANES)
    rest = dot3(mix, split(rest))
    lows = lane < y_local
    blank = jnp.zeros((chans, LANES), jnp.float32)

    def low(i, carry):
        one, two = carry
        spectral = dot3(mix, split(jnp.concatenate([rb[2 * i], rb[2 * i + 1]], axis=1)))
        for j in range(2):
            x = 2 * i + j
            value = re[0, x] + spectral[:, j * LANES : (j + 1) * LANES]
            re[0, x] = value
            one = one + jnp.where(lows, value, 0.0)
            two = two + value * value
            moved = pltpu.roll(rest, (LANES - x * y_local) & (LANES - 1), axis=1)
            value = re[1, x] + jnp.where(lows, moved, 0.0)
            re[1, x] = value
            two = two + value * value
        return one, two

    one, two = lax.fori_loop(0, x_local // 2, low, (blank, blank))

    per_group = chans // GROUPS

    def row(acc, base):
        groups = acc.shape[0] // per_group
        per = jnp.sum(acc.reshape(groups, per_group, LANES), axis=1)
        per = jnp.broadcast_to(jnp.sum(per, axis=1, keepdims=True), (groups, LANES))
        seat = iota((groups, LANES), 1) == iota((groups, LANES), 0) + base
        return jnp.sum(jnp.where(seat, per, 0.0), axis=0, keepdims=True)

    tile = iota((8, LANES), 0)
    sum_one = row(one, 0) * math.sqrt(nz)
    sum_two = row(two, 0) + row(squares, me_wide * (own // per_group))
    held[0] = jnp.where(tile == 0, sum_one, jnp.where(tile == 1, sum_two, 0.0))

    def t_copy(k):
        return pltpu.make_async_remote_copy(
            src_ref=held.at[0],
            dst_ref=held.at[k],
            send_sem=t_send.at[k],
            recv_sem=t_recv.at[k],
            device_id=place(*flat_peer(k)),
            device_id_type=MESH,
        )

    peers(t_copy, "start", count)
    peers(t_copy, "wait", count)
    total = jnp.sum(held[...], axis=0)
    cells_group = per_group * nx * ny * nz
    group_mean = total[0:1] / cells_group
    group_var = total[1:2] / cells_group - group_mean * group_mean
    group_scale = lax.rsqrt(group_var + 1e-05)
    seat = iota((chans, LANES), 1) == iota((chans, LANES), 0) // per_group

    def column_of(value):
        return jnp.sum(jnp.where(seat, value, 0.0), axis=1, keepdims=True)

    scale = column_of(group_scale) * cols[0, :, 0:1]
    shift = cols[1, :, 0:1] - column_of(group_mean) * scale
    cols[4] = jnp.broadcast_to(scale, (chans, LANES))
    cols[5] = jnp.broadcast_to(shift, (chans, LANES))

    def late(hc, carry):
        peers(lambda k: h_copy(hc, k), "wait")

        @pl.when(hc + AHEAD < hchunks)
        def _():
            peers(lambda k: h_copy(hc + AHEAD, k), "start")

        w_in, w_out = split(mats[1]), split(mats[2])
        factor, offset = cols[4, :, 0:1], cols[5, :, 0:1]
        b_in, b_out = cols[2, :, 0:1], cols[3, :, 0:1]
        for j in range(hc_size):
            x = hc * hc_size + j
            value = jnp.concatenate([re[g, x] for g in range(parts)] + [rh[x, g] for g in range(parts)], axis=1)
            value = dot3(split(value), (gi_hi[...], gi_lo[...]))
            normed = value * factor + offset
            hidden = dot3(w_in, split(normed)) + b_in
            inner = math.sqrt(2.0 / math.pi) * (hidden + 0.044715 * (hidden * hidden * hidden))
            hidden = hidden * (0.5 * (1.0 + jnp.tanh(inner)))
            result = value + dot3(w_out, split(hidden)) + b_out
            for y in range(y_local):
                out_ref[:, x * y_local + y, :] = result[:, y * nz : (y + 1) * nz]
        return carry

    lax.fori_loop(0, hchunks, late, 0)


def fused(
    field, mix_weight, factor_x, factor_y, factor_z, norm_gain, norm_bias, w_in, b_in, w_out, b_out
):
    n_sp, n_sub, n_rep = (lax.axis_size(a) for a in ("sp", "sub", "rep"))
    wide, count = n_sp * n_rep, n_sp * n_rep * n_sub
    own, x_local, ny, nz = field.shape
    chans, nx, y_local = own * wide, x_local * n_sub, ny // wide
    kz = factor_z.shape[1]
    chain = own // n_sub
    sub8 = chain // 8
    tiles = wide + 1
    ltile = kz // 2 * ny // LANES
    mtiles = 2 * ltile + 1
    parts = nz * y_local // LANES // 2
    size = nz * y_local
    xchunks, hchunks = 4, x_local // 1
    f32, bf = jnp.float32, jnp.bfloat16
    vmem = lambda *shape: pltpu.VMEM(shape, f32)
    table = lambda *shape: pltpu.VMEM(shape, bf)
    dma = lambda *shape: pltpu.SemaphoreType.DMA(shape)
    scratch = [
        vmem(own, x_local * ny, nz), vmem(3, chans, chans), vmem(3, kz, chans), vmem(4, 1, chans),
        table(size, size), table(size, size), table(size, size), table(size, size),
        table(tiles * LANES, mtiles * LANES), table(tiles * LANES, mtiles * LANES),
        table(mtiles * LANES, tiles * LANES), table(mtiles * LANES, tiles * LANES),
        table(2 * nx * 8, nx * 8), table(2 * nx * 8, nx * 8),
        vmem(sub8, 2, nx * 8, LANES), vmem(sub8, 2, ltile + 1, 8, LANES), vmem(chans, kz), vmem(chans, kz),
        vmem(wide, parts, x_local, own, LANES), vmem(wide, x_local, parts, own, LANES), vmem(x_local, own, LANES),
        vmem(parts, x_local, chans, LANES), vmem(x_local, parts, chans, LANES),
        vmem(tiles, nx, chain, LANES), vmem(sub8, mtiles, nx * 8, LANES),
        vmem(wide, nx, chain, LANES), vmem(nx, chain, LANES), vmem(n_sub, wide, chain // 2, LANES),
        vmem(x_local, chans, LANES), vmem(count, chain // 2, LANES), vmem(count, 8, LANES), vmem(6, chans, LANES),
        dma(xchunks), dma(10), dma(tiles + 2), dma(xchunks, wide), dma(xchunks, wide), dma(hchunks, wide),
        dma(hchunks, wide), dma(tiles, n_sub), dma(tiles, n_sub), dma(count), dma(count), dma(count), dma(count),
        dma(count), dma(count),
    ]
    any_spec = pl.BlockSpec(memory_space=pl.ANY)
    line = lambda v: v.reshape(1, chans)
    result = pl.pallas_call(
        functools.partial(fused_kernel, (n_sp, n_sub, n_rep, kz)),
        out_shape=pltpu.VMEM((chans, x_local * y_local, nz), f32),
        in_specs=[any_spec] * 11,
        out_specs=pl.BlockSpec(memory_space=pltpu.VMEM),
        scratch_shapes=scratch,
        compiler_params=pltpu.CompilerParams(
            collective_id=0, has_side_effects=True, vmem_limit_bytes=VMEM_LIMIT
        ),
        name="fused",
    )(
        field.reshape(own, x_local * ny, nz), mix_weight, w_in, w_out, factor_x.T, factor_y.T, factor_z.T,
        line(norm_gain), line(norm_bias), line(b_in), line(b_out),
    )
    return result.reshape(chans, x_local, y_local, nz)


VMEM_LIMIT = 55 * 1024 * 1024


def fits(field, factor_x, factor_y, factor_z):
    n_sub, wide = lax.axis_size("sub"), lax.axis_size(WIDE)
    own, x_local, ny, nz = field.shape
    nx, kz = x_local * n_sub, factor_z.shape[1]
    power = all(v & (v - 1) == 0 for v in (nx, ny, nz, kz))
    if not power or nz != LANES or factor_x.shape[1] != nx or factor_y.shape[1] != ny or ny % wide:
        return False
    y_local = ny // wide
    return (
        kz * y_local == LANES
        and nz == 4 * kz
        and nx == kz == ny
        and own % (16 * n_sub) == 0
        and lax.axis_size("sp") > 1
        and own % (own * wide // GROUPS) == 0
        and 2 * x_local * y_local <= LANES
        and x_local % 4 == 0
        and (kz // 2 * ny) % LANES == 0
    )


def local(
    field, mix_weight, factor_x, factor_y, factor_z, norm_gain, norm_bias, w_in, b_in, w_out, b_out
):
    run = fused if fits(field, factor_x, factor_y, factor_z) else general
    return run(
        field, mix_weight, factor_x, factor_y, factor_z, norm_gain, norm_bias, w_in, b_in, w_out, b_out
    )


def solution(mesh):
    placed = (P(("grp", "sp", "rep"), "sub", None, None),) + (P(),) * 10
    return jax.shard_map(
        local,
        mesh=mesh,
        in_specs=placed,
        out_specs=P("grp", "sub", ("sp", "rep"), None),
        check_vma=False,
    )
```

```python
import math
import functools

import jax
import jax.numpy as jnp
from jax import lax
from jax.experimental import pallas as pl
from jax.experimental.pallas import tpu as pltpu
from jax.sharding import PartitionSpec as P

GROUPS = 32
HIGH = lax.Precision.HIGH
WIDE = ("sp", "rep")


def trig(length, freq, positions):
    phases = (freq[:, None] * positions[None, :]) % length
    angles = 2.0 * math.pi / length * phases.astype(jnp.float32)
    return jnp.cos(angles), jnp.sin(angles)


def kron_pair(cos_a, sin_a, cos_b, sin_b):
    ca, sa = cos_a.T[:, None, :, None], sin_a.T[:, None, :, None]
    cb, sb = cos_b.T[None, :, None, :], sin_b.T[None, :, None, :]
    return ca * cb - sa * sb, sa * cb + ca * sb


def split(value):
    high = value.astype(jnp.bfloat16)
    low = (value - high.astype(jnp.float32)).astype(jnp.bfloat16)
    return high, low


def dot3(left, right):
    lh, ll = left
    rh, rl = right
    d = functools.partial(jnp.dot, preferred_element_type=jnp.float32)
    return d(lh, rh) + (d(lh, rl) + d(ll, rh))


def sum_kernel(
    sizes, field_ref, modes_ref, table_ref, summed_ref, total_ref, acc1, acc2, held, send_sem, recv_sem
):
    step = pl.program_id(0)
    n_sp, n_sub, n_rep = sizes
    count = n_sp * n_sub * n_rep
    me = (lax.axis_index("sp") * n_sub + lax.axis_index("sub")) * n_rep + lax.axis_index("rep")

    def place(index):
        return {
            "sp": index // (n_sub * n_rep),
            "sub": (index // n_rep) % n_sub,
            "rep": index % n_rep,
        }

    @pl.when(step == 0)
    def _():
        barrier = pltpu.get_barrier_semaphore()

        def greet(k, carry):
            pl.semaphore_signal(
                barrier,
                inc=1,
                device_id=place((me + k) % count),
                device_id_type=pl.DeviceIdType.MESH,
            )
            return carry

        lax.fori_loop(1, count, greet, 0)

    chans, cells, width = field_ref.shape
    rank = modes_ref.shape[2]

    @pl.when(step == 0)
    def _():
        acc1[...] = jnp.zeros_like(acc1)
        acc2[...] = jnp.zeros_like(acc2)

    table = split(table_ref[...])
    chunk = 32 if chans % 32 == 0 else chans

    def body(index, carry):
        rows = pl.ds(pl.multiple_of(index * chunk, chunk), chunk)
        modes = modes_ref[rows].reshape(chunk * cells, rank)
        value = dot3(split(modes), table).reshape(chunk, cells, width) + field_ref[rows]
        summed_ref[rows] = value
        acc1[rows] += value
        acc2[rows] += value * value
        return carry

    lax.fori_loop(0, chans // chunk, body, 0)

    @pl.when(step == pl.num_programs(0) - 1)
    def _():
        def row(acc):
            per = jnp.sum(acc[...], axis=1)
            per = jnp.sum(per.reshape(GROUPS, chans // GROUPS, width), axis=1)
            per = jnp.broadcast_to(jnp.sum(per, axis=1, keepdims=True), (GROUPS, 128))
            lanes = lax.broadcasted_iota(jnp.int32, (GROUPS, 128), 1)
            rows = lax.broadcasted_iota(jnp.int32, (GROUPS, 128), 0)
            return jnp.sum(jnp.where(lanes == rows, per, 0.0), axis=0, keepdims=True)

        tile = lax.broadcasted_iota(jnp.int32, (8, 128), 0)
        held[0] = jnp.where(tile == 0, row(acc1), jnp.where(tile == 1, row(acc2), 0.0))
        pl.semaphore_wait(pltpu.get_barrier_semaphore(), count - 1)

        def copy(k):
            return pltpu.make_async_remote_copy(
                src_ref=held.at[0],
                dst_ref=held.at[k],
                send_sem=send_sem.at[k],
                recv_sem=recv_sem.at[k],
                device_id=place((me + k) % count),
                device_id_type=pl.DeviceIdType.MESH,
            )

        def launch(k, carry):
            copy(k).start()
            return carry

        def finish(k, carry):
            copy(k).wait()
            return carry

        lax.fori_loop(1, count, launch, 0)
        lax.fori_loop(1, count, finish, 0)
        total_ref[...] = jnp.sum(held[...], axis=0)


def mlp_kernel(summed_ref, vec_ref, w_in_ref, w_out_ref, out_ref):
    cells = summed_ref.shape[1]
    w_in = split(w_in_ref[...])
    w_out = split(w_out_ref[...])
    vec = vec_ref[...]
    mean, scale, bias = vec[:, 0:1], vec[:, 1:2], vec[:, 2:3]
    b_in, b_out = vec[:, 3:4], vec[:, 4:5]
    pair = 2 if cells % 2 == 0 else 1
    for start in range(0, cells, pair):
        parts = [summed_ref[:, p, :] for p in range(start, start + pair)]
        value = jnp.concatenate(parts, axis=1) if pair > 1 else parts[0]
        normed = (value - mean) * scale + bias
        hidden = dot3(w_in, split(normed)) + b_in
        inner = math.sqrt(2.0 / math.pi) * (hidden + 0.044715 * (hidden * hidden * hidden))
        hidden = hidden * (0.5 * (1.0 + jnp.tanh(inner)))
        result = value + dot3(w_out, split(hidden)) + b_out
        width = summed_ref.shape[2]
        for k in range(pair):
            out_ref[:, start + k, :] = result[:, k * width : (k + 1) * width]


def general(
    field, mix_weight, factor_x, factor_y, factor_z, norm_gain, norm_bias, w_in, b_in, w_out, b_out
):
    wide_count = lax.axis_size(WIDE)
    narrow_count = lax.axis_size("sub")
    own_chans, x_local, ny, nz = field.shape
    chans = own_chans * wide_count
    nx = x_local * narrow_count
    kx, ky, kz = factor_x.shape[1], factor_y.shape[1], factor_z.shape[1]
    y_local = ny // wide_count
    half = kz // 2
    kept = half + 1
    me_sub = lax.axis_index("sub")
    cells = x_local * y_local

    spatial = field.reshape(own_chans, x_local, wide_count, y_local, nz)
    spatial = spatial.transpose(2, 0, 1, 3, 4).reshape(wide_count, own_chans, cells, nz)
    spatial = lax.all_to_all(spatial, WIDE, split_axis=0, concat_axis=0, tiled=True)

    cos_z, sin_z = trig(nz, jnp.arange(kept), jnp.arange(nz))
    forward = jnp.concatenate([cos_z, -sin_z]) / nz
    planes = jnp.einsum("rz,cxyz->rcxy", forward, field, precision=HIGH)
    planes = planes.reshape(2 * kept * own_chans, x_local * ny)

    def freqs(length, count):
        index = jnp.arange(count)
        return jnp.where(index < count // 2, index, length - count + index)

    cos_y, sin_y = trig(ny, freqs(ny, ky), jnp.arange(ny))

    def forward_xy(values, owner):
        cos_x, sin_x = trig(nx, freqs(nx, kx), owner * x_local + jnp.arange(x_local))
        c, s = kron_pair(cos_x, sin_x, cos_y, sin_y)
        c = (c / (nx * ny)).reshape(x_local * ny, kx * ky)
        s = (s / (nx * ny)).reshape(x_local * ny, kx * ky)
        a = jnp.dot(values, jnp.concatenate([c, s], axis=1), precision=HIGH)
        a = a.reshape(2, kept * own_chans, 2, kx * ky)
        return a[0, :, 0] + a[1, :, 1], a[1, :, 0] - a[0, :, 1]

    held = planes
    real, imag = forward_xy(held, me_sub)
    for hop in range(1, narrow_count):
        held = lax.ppermute(held, "sub", [(i, (i + 1) % narrow_count) for i in range(narrow_count)])
        owner = (me_sub - hop + narrow_count) % narrow_count
        more_real, more_imag = forward_xy(held, owner)
        real, imag = real + more_real, imag + more_imag

    start = lax.axis_index(WIDE) * own_chans
    fx = lax.dynamic_slice_in_dim(factor_x, start, own_chans, 0)
    fy = lax.dynamic_slice_in_dim(factor_y, start, own_chans, 0)
    fz = lax.dynamic_slice_in_dim(factor_z, start, own_chans, 0)
    mirror_x = (-jnp.arange(kx)) % kx
    mirror_y = (-jnp.arange(ky)) % ky
    plane_a = (fx[:, :, None] * fy[:, None, :]).reshape(own_chans, kx * ky)
    plane_b = (fx[:, mirror_x][:, :, None] * fy[:, mirror_y][:, None, :]).reshape(own_chans, kx * ky)
    zero = jnp.zeros((own_chans, 1), jnp.float32)
    z_plus = jnp.concatenate([fz[:, :half], zero], axis=1).T
    z_minus = jnp.concatenate([zero, fz[:, half:][:, ::-1]], axis=1).T
    weight = z_plus[:, :, None] * plane_a[None] + z_minus[:, :, None] * plane_b[None]
    weight = weight.reshape(kept * own_chans, kx * ky)
    real, imag = real * weight, imag * weight

    cos_x, sin_x = trig(nx, freqs(nx, kx), me_sub * x_local + jnp.arange(x_local))
    c, s = kron_pair(cos_x, sin_x, cos_y, sin_y)

    def columns(t):
        t = t.reshape(x_local, wide_count, y_local, kx * ky)
        return t.transpose(3, 1, 0, 2).reshape(kx * ky, wide_count * cells)

    c, s = columns(c), columns(s)
    table_re = jnp.concatenate([c, -s])
    table_im = jnp.concatenate([s, c])
    both = jnp.concatenate([real, imag], axis=1)
    back = jnp.stack(
        [jnp.dot(both, table_re, precision=HIGH), jnp.dot(both, table_im, precision=HIGH)]
    )
    back = back.reshape(2 * kept, own_chans, wide_count, cells)
    back = back.transpose(2, 1, 0, 3).reshape(wide_count * own_chans, 2 * kept * cells)
    back, spatial = lax.optimization_barrier((back, spatial))
    back = lax.all_to_all(back, WIDE, split_axis=0, concat_axis=0, tiled=True)
    back = back.reshape(chans, 2 * kept, cells)
    mixed = jnp.einsum("oi,irp->opr", mix_weight, back, precision=HIGH)

    inverse_z = jnp.concatenate([cos_z, -sin_z])
    spatial = spatial.reshape(chans, cells, nz)
    block = 8 if cells % 8 == 0 else cells
    steps = cells // block
    cube = pl.BlockSpec((chans, block, nz), lambda i: (0, i, 0))
    whole = lambda *shape: pl.BlockSpec(shape, lambda i: (0,) * len(shape))
    sizes = (lax.axis_size("sp"), narrow_count, lax.axis_size("rep"))
    count = sizes[0] * sizes[1] * sizes[2]
    summed, stats = pl.pallas_call(
        functools.partial(sum_kernel, sizes),
        grid=(steps,),
        out_shape=(
            jax.ShapeDtypeStruct(spatial.shape, jnp.float32),
            jax.ShapeDtypeStruct((8, 128), jnp.float32),
        ),
        in_specs=[
            cube,
            pl.BlockSpec((chans, block, 2 * kept), lambda i: (0, i, 0)),
            whole(2 * kept, nz),
        ],
        out_specs=(cube, whole(8, 128)),
        scratch_shapes=[pltpu.VMEM((chans, block, nz), jnp.float32)] * 2
        + [
            pltpu.VMEM((count, 8, 128), jnp.float32),
            pltpu.SemaphoreType.DMA((count,)),
            pltpu.SemaphoreType.DMA((count,)),
        ],
        compiler_params=pltpu.CompilerParams(collective_id=0, has_side_effects=True),
        name="sum_stats",
    )(spatial, mixed, inverse_z)

    size = chans // GROUPS
    stats = stats[:2, :GROUPS]
    cells_group = size * nx * ny * nz
    group_mean = stats[0] / cells_group
    group_var = stats[1] / cells_group - group_mean * group_mean
    scale = jnp.repeat(lax.rsqrt(group_var + 1e-05), size) * norm_gain
    mean = jnp.repeat(group_mean, size)
    vec = jnp.stack([mean, scale, norm_bias, b_in, b_out] + [b_out] * 3, axis=1)

    result = pl.pallas_call(
        mlp_kernel,
        grid=(steps,),
        out_shape=jax.ShapeDtypeStruct(spatial.shape, jnp.float32),
        in_specs=[cube, whole(chans, 8), whole(*w_in.shape), whole(*w_out.shape)],
        out_specs=cube,
        name="mlp",
    )(summed, vec, w_in, w_out)
    return result.reshape(chans, x_local, y_local, nz)


MESH = pl.DeviceIdType.MESH
LANES = 128
AHEAD = 4
PUMP = 4


def cosine(index, length):
    fold = jnp.abs(index.astype(jnp.float32) * (2.0 / length) - 1.0)
    near = jnp.minimum(fold, 1.0 - fold) * math.pi
    square = near * near
    total = jnp.full_like(square, 1.0 / math.factorial(14))
    for power in range(6, -1, -1):
        term = 1.0 / math.factorial(2 * power)
        total = term - square * total
    return jnp.where(fold > 0.5, total, -total)


def log2(value):
    return value.bit_length() - 1


def split3(value):
    high = value.astype(jnp.bfloat16)
    rest = value - high.astype(jnp.float32)
    mid = rest.astype(jnp.bfloat16)
    low = (rest - mid.astype(jnp.float32)).astype(jnp.bfloat16)
    return high, mid, low


def pick(left, right):
    d = functools.partial(jnp.dot, preferred_element_type=jnp.float32)
    a, b, c = split3(right)
    return d(left, a) + (d(left, b) + d(left, c))


def pick_right(left, right):
    d = functools.partial(jnp.dot, preferred_element_type=jnp.float32)
    a, b, c = split3(left)
    return d(a, right) + (d(b, right) + d(c, right))


def iota(shape, axis):
    return lax.broadcasted_iota(jnp.int32, shape, axis)


def fused_kernel(
    dims,
    field_ref, mix_ref, w_in_ref, w_out_ref, fx_ref, fy_ref, fz_ref, gain_ref, bias_ref, b_in_ref, b_out_ref,
    out_ref,
    fld, mats, facs, vecs, g_hi, g_lo, gi_hi, gi_lo, yf_hi, yf_lo, yi_hi, yi_lo, xt_hi, xt_lo, fxs, uv, fy_t, fz_t,
    se, sh, lf, re, rh, pin, mid, bs, lb, ls, rb, rl, held, cols,
    fld_sem, par_sem, own_sem, e_send, e_recv, h_send, h_recv, x_send, x_recv, b_send, b_recv, l_send, l_recv,
    t_send, t_recv,
):
    n_sp, n_sub, n_rep, n_freq = dims
    wide = n_sp * n_rep
    count = wide * n_sub
    own, xy_rows, nz = field_ref.shape
    chans = own * wide
    parts, x_local, _, _ = se.shape[1:]
    y_local = LANES // (nz // (2 * parts))
    width = LANES // y_local
    nx = pin.shape[1]
    ny = xy_rows // x_local
    kz = n_freq
    half = kz // 2
    chain = own // n_sub
    sub8 = chain // 8
    tiles = wide + 1
    ltile = half * ny // LANES
    per_tile = LANES // ny
    lane_y, lane_n = log2(y_local), log2(ny)

    me_sub = lax.axis_index("sub")
    me_sp, me_rep = lax.axis_index("sp"), lax.axis_index("rep")
    me_wide = me_sp * n_rep + me_rep
    me = me_wide * n_sub + me_sub

    def place(w, s):
        return {"sp": w // n_rep, "sub": s, "rep": w % n_rep}

    def place_flat(index):
        return place(index // n_sub, index % n_sub)

    def wide_peer(k):
        return (me_sp + k // n_rep) % n_sp * n_rep + (me_rep + k % n_rep) % n_rep

    def flat_peer(k):
        w = (me_sp + k // (n_rep * n_sub)) % n_sp * n_rep + (me_rep + k % n_rep) % n_rep
        return w, (me_sub + k // n_rep % n_sub) % n_sub

    def turn(i, n):
        near = n // n_sp
        late = i // (n - near)
        return (1 - late) * (near + i) + late * (n - 1 - i)

    def loop(n, body):
        def step(i, carry):
            body(i)
            return carry

        lax.fori_loop(0, n, step, 0)

    barrier = pltpu.get_barrier_semaphore()

    def greet(k, carry):
        pl.semaphore_signal(barrier, inc=1, device_id=place_flat((me + k) % count), device_id_type=MESH)
        return carry

    lax.fori_loop(1, count, greet, 0)

    xchunks = fld_sem.shape[0]
    xc_size = x_local // xchunks

    def fetch(i):
        rows = pl.ds(i * (xc_size * ny), xc_size * ny)
        return pltpu.make_async_copy(field_ref.at[:, rows], fld.at[:, rows], fld_sem.at[i])

    fetch(0).start()
    params = [(mix_ref, mats.at[0]), (w_in_ref, mats.at[1]), (w_out_ref, mats.at[2])]
    params += [(fx_ref, facs.at[0]), (fy_ref, facs.at[1]), (fz_ref, facs.at[2])]
    params += [(gain_ref, vecs.at[0]), (bias_ref, vecs.at[1]), (b_in_ref, vecs.at[2]), (b_out_ref, vecs.at[3])]
    param_copies = [pltpu.make_async_copy(a, b, par_sem.at[i]) for i, (a, b) in enumerate(params)]
    def coef(j):
        low_k = jnp.where(j == 1, half, j >> 1)
        low_s = jnp.where(j == 1, 0, j & 1)
        high_k = (j + 1) >> 1
        high_s = 1 - (j & 1)
        return jnp.where(j < kz, low_k, high_k), jnp.where(j < kz, low_s, high_s)

    def basis(j, z):
        k, s = coef(j)
        value = cosine((k * z + s * (3 * nz // 4)) & (nz - 1), nz)
        edge = (k == 0) | (k == nz // 2)
        return value * jnp.where(edge, math.sqrt(1.0 / nz), math.sqrt(2.0 / nz))

    def g_entry(rows, columns):
        y_in, z = rows >> log2(nz), rows & (nz - 1)
        j, y_out = columns >> lane_y, columns & (y_local - 1)
        return jnp.where(y_in == y_out, basis(j, z), 0.0)

    size = nz * y_local
    stepr = LANES

    def build_g(i):
        rows = pl.ds(pl.multiple_of(i * stepr, stepr), stepr)
        a = iota((stepr, size), 0) + i * stepr
        b = iota((stepr, size), 1)
        g_hi[rows], g_lo[rows] = split(g_entry(a, b))

    def build_back(i):
        rows = pl.ds(pl.multiple_of(i * stepr, stepr), stepr)
        a = iota((stepr, size), 0) + i * stepr
        b = iota((stepr, size), 1)
        gi_hi[rows], gi_lo[rows] = split(g_entry(b, a))

    loop(size // stepr, build_g)

    lane = iota((1, LANES), 1)

    def e_copy(xc, k):
        w = wide_peer(k)
        xs = pl.ds(xc * xc_size, xc_size)
        return pltpu.make_async_remote_copy(
            src_ref=se.at[w, :, xs],
            dst_ref=re.at[:, xs, pl.ds(pl.multiple_of(me_wide * own, own), own)],
            send_sem=e_send.at[xc, k],
            recv_sem=e_recv.at[xc, k],
            device_id=place(w, me_sub),
            device_id_type=MESH,
        )

    hchunks = h_send.shape[0]
    hc_size = x_local // hchunks

    def h_copy(hc, k):
        w = wide_peer(k)
        xs = pl.ds(hc * hc_size, hc_size)
        return pltpu.make_async_remote_copy(
            src_ref=sh.at[w, xs],
            dst_ref=rh.at[xs, :, pl.ds(pl.multiple_of(me_wide * own, own), own)],
            send_sem=h_send.at[hc, k],
            recv_sem=h_recv.at[hc, k],
            device_id=place(w, me_sub),
            device_id_type=MESH,
        )

    def peers(make, what, n=wide):
        def step(i, carry):
            getattr(make(turn(i, n)), what)()
            return carry

        lax.fori_loop(0, n - 1, step, 0)

    zero = jnp.zeros((own, LANES), jnp.float32)

    def transform(xc, squares):
        fetch(xc).wait()

        @pl.when(xc + 1 < xchunks)
        def _():
            fetch(xc + 1).start()


        def one(i, carry):
            left, sq = carry
            d = wide_peer(turn(i, wide))
            groups = []
            for xi in range(xc_size):
                row = (xc * xc_size + xi) * ny + d * y_local
                groups.append(jnp.concatenate([fld[:, row + y, :] for y in range(y_local)], axis=1))
            value = jnp.concatenate(groups, axis=0)
            res = dot3(split(value), (g_hi[...], g_lo[...]))
            cube = res.reshape(xc_size, own, size)
            xs = pl.ds(xc * xc_size, xc_size)
            for g in range(parts):
                se[d, g, xs] = cube[:, :, g * LANES : (g + 1) * LANES]
                part = cube[:, :, (parts + g) * LANES : (parts + g + 1) * LANES]
                sh[d, xs, g] = part
                sq = sq + jnp.sum(part * part, axis=0)
            more = pltpu.roll(res[:, LANES : 2 * LANES], d * y_local, axis=1)
            left = jnp.where((lane >> lane_y) == d, more, left)

            @pl.when(jnp.logical_and(xc == 0, i == 1))
            def _():
                pl.semaphore_wait(barrier, count - 1)

            @pl.when(i >= 1)
            def _():
                e_copy(xc, turn(i - 1, wide)).start()

            return left, sq

        left = jnp.zeros((xc_size * own, LANES), jnp.float32)
        left, squares = lax.fori_loop(0, wide, one, (left, squares))
        lf[pl.ds(xc * xc_size, xc_size)] = left.reshape(xc_size, own, LANES)

        return squares

    squares = lax.fori_loop(0, xchunks, transform, zero)
    for copy in param_copies:
        copy.start()

    def x_src(t, s):
        cs = pl.ds(pl.multiple_of(s * chain, 8), chain)
        return se.at[t, 0, :, cs] if t < wide else lf.at[:, cs]

    def x_dst(t):
        return pin.at[t, pl.ds(me_sub * x_local, x_local)]

    x_copies = []
    for t in range(tiles):
        for k in range(1, n_sub):
            s = (me_sub + k) % n_sub
            x_copies.append(
                pltpu.make_async_remote_copy(
                    src_ref=x_src(t, s),
                    dst_ref=x_dst(t),
                    send_sem=x_send.at[t, k],
                    recv_sem=x_recv.at[t, k],
                    device_id=place(me_wide, s),
                    device_id_type=MESH,
                )
            )
    own_chan = pl.ds(pl.multiple_of(me_wide * own, own), own)
    own_copies = [pltpu.make_async_copy(x_src(t, me_sub), x_dst(t), own_sem.at[t]) for t in range(tiles)]
    own_copies.append(pltpu.make_async_copy(se.at[me_wide], re.at[:, :, own_chan], own_sem.at[tiles]))
    own_copies.append(pltpu.make_async_copy(sh.at[me_wide], rh.at[:, :, own_chan], own_sem.at[tiles + 1]))

    def p_meta(t, r):
        jj = r >> lane_y
        k = jnp.where(jj == 1, half, jj >> 1)
        s = jnp.where(jj == 1, 0, jj & 1)
        y = t * y_local + (r & (y_local - 1))
        rest = t == wide
        k = jnp.where(rest, jnp.where(r < ny, half, -1), k)
        return k, jnp.where(rest, 1, s), jnp.where(rest, r, y)

    def m_meta(t, c):
        part = jnp.where(t >= ltile, 1, 0)
        k = (t - part * ltile) * per_tile + (c >> lane_n)
        rest = t == 2 * ltile
        seat = c & (LANES // 2 - 1)
        k = jnp.where(rest, jnp.where(seat < ny, half, -2), k)
        part = jnp.where(rest, c >> log2(LANES // 2), part)
        return k, part, c & (ny - 1)

    def y_entry(pt, mt, p, m, forward):
        kp, s, y = p_meta(pt, p)
        km, part, b = m_meta(mt, m)
        value = cosine((y * b + (ny // 4) * (s + part)) & (ny - 1), ny)
        scale = jnp.where(km == 0, math.sqrt(nz), math.sqrt(nz / 2.0))
        if forward:
            scale = scale * (1.0 / nz)
        return jnp.where(kp == km, value * scale, 0.0)

    square = (LANES, LANES)
    mtiles = 2 * ltile + 1

    def build_y(i):
        rows = pl.ds(pl.multiple_of(i * LANES, LANES), LANES)
        for t in range(mtiles):
            cut = slice(t * LANES, (t + 1) * LANES)
            a, b = iota(square, 0), iota(square, 1)
            yf_hi[rows, cut], yf_lo[rows, cut] = split(y_entry(i, t, a, b, True))
            yi_hi[rows, cut], yi_lo[rows, cut] = split(y_entry(t, i, b, a, False))

    def build_x(i):
        shape = (LANES, nx * 8)
        row = iota(shape, 0) + i * LANES
        col = iota(shape, 1)
        part = row >> log2(nx * 8)
        a = (row >> 3) & (nx - 1)
        value = cosine(((a * (col >> 3)) + part * (3 * nx // 4)) & (nx - 1), nx)
        value = jnp.where((row & 7) == (col & 7), value, 0.0)
        rows = pl.ds(pl.multiple_of(i * LANES, LANES), LANES)
        xt_hi[rows], xt_lo[rows] = split(value)

    for copy in x_copies:
        copy.start()
    for copy in own_copies:
        copy.start()
    loop(tiles, build_y)
    loop(size // stepr, build_back)
    loop(2 * nx * 8 // LANES, build_x)

    for copy in param_copies:
        copy.wait()
    fy_t[...] = jnp.transpose(facs[1])
    fz_t[...] = jnp.transpose(facs[2])
    first = me_wide * own + me_sub * chain
    bf = jnp.bfloat16
    one_hot = lambda mask: jnp.where(mask, 1.0, 0.0).astype(bf)
    for h in range(sub8):
        base = pl.multiple_of(first + 8 * h, 8)
        a = iota((nx * 8, nx), 0) >> 3
        b = iota((nx * 8, nx), 1)
        mask = iota((nx * 8, chans), 1) == first + 8 * h + (iota((nx * 8, chans), 0) & 7)
        for sign in range(2):
            want = a if sign == 0 else (nx - a) & (nx - 1)
            spread = pick(one_hot(b == want), facs[0])
            column = jnp.sum(jnp.where(mask, spread, 0.0), axis=1, keepdims=True)
            fxs[h, sign] = jnp.broadcast_to(column * (1.0 / (nx * ny)), (nx * 8, LANES))
        fz8, fy8 = fz_t[pl.ds(base, 8), :], fy_t[pl.ds(base, 8), :]
        for t in range(ltile + 1):
            i = iota((kz, LANES), 0)
            seat = iota((kz, LANES), 1)
            k = t * per_tile + (seat >> lane_n) if t < ltile else half
            bb = seat & (ny - 1)
            plus = one_hot(i == (k if t < ltile else -1))
            minus = one_hot((i == kz - k) & (k > 0)) if t < ltile else one_hot(i == half)
            yp, ym = one_hot(i == bb), one_hot(i == ((ny - bb) & (ny - 1)))
            uv[h, 0, t] = pick_right(fz8, plus) * pick_right(fy8, yp)
            uv[h, 1, t] = pick_right(fz8, minus) * pick_right(fy8, ym)

    for copy in own_copies:
        copy.wait()
    for copy in x_copies:
        copy.wait()

    rows8 = nx * 8

    def forward_y(h):
        cs = pl.ds(pl.multiple_of(h * 8, 8), 8)
        value = jnp.concatenate([pin[t, :, cs, :].reshape(rows8, LANES) for t in range(tiles)], axis=1)
        res = dot3(split(value), (yf_hi[...], yf_lo[...]))
        for t in range(mtiles):
            mid[h, t] = res[:, t * LANES : (t + 1) * LANES]

    loop(sub8, forward_y)

    def weights(h, t):
        u = jnp.broadcast_to(uv[h, 0, t][None], (nx, 8, LANES)).reshape(rows8, LANES)
        v = jnp.broadcast_to(uv[h, 1, t][None], (nx, 8, LANES)).reshape(rows8, LANES)
        return fxs[h, 0] * u + fxs[h, 1] * v

    def along_x(value):
        return dot3((xt_hi[...], xt_lo[...]), split(value))

    def pair_x(i):
        h, t = i // ltile, i % ltile
        res = along_x(jnp.concatenate([mid[h, t], mid[h, ltile + t]], axis=1))
        c_re, c_im = res[:rows8, :LANES], res[:rows8, LANES:]
        s_re, s_im = res[rows8:, :LANES], res[rows8:, LANES:]
        w = weights(h, t)
        res = along_x(jnp.concatenate([(c_re + s_im) * w, (c_im - s_re) * w], axis=1))
        c_re, c_im = res[:rows8, :LANES], res[:rows8, LANES:]
        s_re, s_im = res[rows8:, :LANES], res[rows8:, LANES:]
        mid[h, t] = c_re - s_im
        mid[h, ltile + t] = c_im + s_re

    loop(sub8 * ltile, pair_x)

    def rest_x(h):
        sign = jnp.where(lane < LANES // 2, 1.0, -1.0)
        res = along_x(mid[h, 2 * ltile])
        modes = res[:rows8] + sign * pltpu.roll(res[rows8:], LANES // 2, axis=1)
        res = along_x(modes * weights(h, ltile))
        mid[h, 2 * ltile] = res[:rows8] - sign * pltpu.roll(res[rows8:], LANES // 2, axis=1)

    loop(sub8, rest_x)

    def back_y(h):
        cs = pl.ds(pl.multiple_of(h * 8, 8), 8)
        value = jnp.concatenate([mid[h, t] for t in range(mtiles)], axis=1)
        res = dot3(split(value), (yi_hi[...], yi_lo[...]))
        for t in range(tiles):
            cut = res[:, t * LANES : (t + 1) * LANES].reshape(nx, 8, LANES)
            if t < wide:
                bs[t, :, cs, :] = cut
            else:
                lb[:, cs, :] = cut

    loop(sub8, back_y)

    def gather_rest(s):
        def one(x, carry):
            value = lb[s * x_local + x]
            new = []
            for d in range(wide):
                moved = pltpu.roll(value, ((x - d) * y_local + LANES) & (LANES - 1), axis=1)
                new.append(jnp.where((lane >> lane_y) == x, moved, carry[d]))
            return tuple(new)

        start = tuple(jnp.zeros((chain, LANES), jnp.float32) for _ in range(wide))
        done = lax.fori_loop(0, x_local, one, start)
        for d in range(wide):
            other = pltpu.roll(done[d][chain // 2 :], LANES // 2, axis=1)
            ls[s, d] = jnp.where(lane < LANES // 2, done[d][: chain // 2], other)

    loop(n_sub, gather_rest)

    b_rows = pl.ds(pl.multiple_of(first, 8), chain)

    def b_copy(k):
        w, s = flat_peer(k)
        return pltpu.make_async_remote_copy(
            src_ref=bs.at[w, pl.ds(s * x_local, x_local)],
            dst_ref=rb.at[:, b_rows],
            send_sem=b_send.at[k],
            recv_sem=b_recv.at[k],
            device_id=place(w, s),
            device_id_type=MESH,
        )

    def l_copy(k):
        w, s = flat_peer(k)
        return pltpu.make_async_remote_copy(
            src_ref=ls.at[s, w],
            dst_ref=rl.at[me],
            send_sem=l_send.at[k],
            recv_sem=l_recv.at[k],
            device_id=place(w, s),
            device_id_type=MESH,
        )

    peers(b_copy, "start", count)
    own_b = pltpu.make_async_copy(bs.at[me_wide, pl.ds(me_sub * x_local, x_local)], rb.at[:, b_rows], b_send.at[0])
    own_l = pltpu.make_async_copy(ls.at[me_sub, me_wide], rl.at[me], l_send.at[0])
    own_b.start()
    own_l.start()
    peers(l_copy, "start", count)
    loop(AHEAD, lambda hc: peers(lambda k: h_copy(hc, k), "start"))

    eye = iota((chans, chans), 0) == iota((chans, chans), 1)
    for i in range(4):
        column = jnp.sum(jnp.where(eye, vecs[i], 0.0), axis=1, keepdims=True)
        cols[i] = jnp.broadcast_to(column, (chans, LANES))

    own_b.wait()
    own_l.wait()
    peers(b_copy, "wait", count)
    peers(l_copy, "wait", count)
    loop(xchunks, lambda xc: peers(lambda k: e_copy(xc, k), "wait"))
    mix = split(mats[0])
    packed = rl[...].reshape(chans // 2, LANES)
    other = pltpu.roll(packed, LANES // 2, axis=1).reshape(rl.shape)
    rest = jnp.concatenate([rl[...], other], axis=1).reshape(chans, LANES)
    rest = dot3(mix, split(rest))
    lows = lane < y_local
    blank = jnp.zeros((chans, LANES), jnp.float32)

    def low(i, carry):
        one, two = carry
        spectral = dot3(mix, split(jnp.concatenate([rb[2 * i], rb[2 * i + 1]], axis=1)))
        for j in range(2):
            x = 2 * i + j
            value = re[0, x] + spectral[:, j * LANES : (j + 1) * LANES]
            re[0, x] = value
            one = one + jnp.where(lows, value, 0.0)
            two = two + value * value
            moved = pltpu.roll(rest, (LANES - x * y_local) & (LANES - 1), axis=1)
            value = re[1, x] + jnp.where(lows, moved, 0.0)
            re[1, x] = value
            two = two + value * value
        return one, two

    one, two = lax.fori_loop(0, x_local // 2, low, (blank, blank))

    per_group = chans // GROUPS

    def row(acc, base):
        groups = acc.shape[0] // per_group
        per = jnp.sum(acc.reshape(groups, per_group, LANES), axis=1)
        per = jnp.broadcast_to(jnp.sum(per, axis=1, keepdims=True), (groups, LANES))
        seat = iota((groups, LANES), 1) == iota((groups, LANES), 0) + base
        return jnp.sum(jnp.where(seat, per, 0.0), axis=0, keepdims=True)

    tile = iota((8, LANES), 0)
    sum_one = row(one, 0) * math.sqrt(nz)
    sum_two = row(two, 0) + row(squares, me_wide * (own // per_group))
    held[0] = jnp.where(tile == 0, sum_one, jnp.where(tile == 1, sum_two, 0.0))

    def t_copy(k):
        return pltpu.make_async_remote_copy(
            src_ref=held.at[0],
            dst_ref=held.at[k],
            send_sem=t_send.at[k],
            recv_sem=t_recv.at[k],
            device_id=place(*flat_peer(k)),
            device_id_type=MESH,
        )

    def arrive(hc):
        peers(lambda k: h_copy(hc, k), "wait")

        @pl.when(hc + AHEAD < hchunks)
        def _():
            peers(lambda k: h_copy(hc + AHEAD, k), "start")

    peers(t_copy, "start", count)
    loop(PUMP, arrive)
    peers(t_copy, "wait", count)
    total = jnp.sum(held[...], axis=0)
    cells_group = per_group * nx * ny * nz
    group_mean = total[0:1] / cells_group
    group_var = total[1:2] / cells_group - group_mean * group_mean
    group_scale = lax.rsqrt(group_var + 1e-05)
    seat = iota((chans, LANES), 1) == iota((chans, LANES), 0) // per_group

    def column_of(value):
        return jnp.sum(jnp.where(seat, value, 0.0), axis=1, keepdims=True)

    scale = column_of(group_scale) * cols[0, :, 0:1]
    shift = cols[1, :, 0:1] - column_of(group_mean) * scale
    cols[4] = jnp.broadcast_to(scale, (chans, LANES))
    cols[5] = jnp.broadcast_to(shift, (chans, LANES))

    def late(hc, carry):
        pl.when(hc >= PUMP)(functools.partial(arrive, hc))
        w_in, w_out = split(mats[1]), split(mats[2])
        factor, offset = cols[4, :, 0:1], cols[5, :, 0:1]
        b_in, b_out = cols[2, :, 0:1], cols[3, :, 0:1]
        for j in range(hc_size):
            x = hc * hc_size + j
            value = jnp.concatenate([re[g, x] for g in range(parts)] + [rh[x, g] for g in range(parts)], axis=1)
            value = dot3(split(value), (gi_hi[...], gi_lo[...]))
            normed = value * factor + offset
            hidden = dot3(w_in, split(normed)) + b_in
            inner = math.sqrt(2.0 / math.pi) * (hidden + 0.044715 * (hidden * hidden * hidden))
            hidden = hidden * (0.5 * (1.0 + jnp.tanh(inner)))
            result = value + dot3(w_out, split(hidden)) + b_out
            for y in range(y_local):
                out_ref[:, x * y_local + y, :] = result[:, y * nz : (y + 1) * nz]
        return carry

    lax.fori_loop(0, hchunks, late, 0)


def fused(
    field, mix_weight, factor_x, factor_y, factor_z, norm_gain, norm_bias, w_in, b_in, w_out, b_out
):
    n_sp, n_sub, n_rep = (lax.axis_size(a) for a in ("sp", "sub", "rep"))
    wide, count = n_sp * n_rep, n_sp * n_rep * n_sub
    own, x_local, ny, nz = field.shape
    chans, nx, y_local = own * wide, x_local * n_sub, ny // wide
    kz = factor_z.shape[1]
    chain = own // n_sub
    sub8 = chain // 8
    tiles = wide + 1
    ltile = kz // 2 * ny // LANES
    mtiles = 2 * ltile + 1
    parts = nz * y_local // LANES // 2
    size = nz * y_local
    xchunks, hchunks = 4, x_local
    f32, bf = jnp.float32, jnp.bfloat16
    vmem = lambda *shape: pltpu.VMEM(shape, f32)
    table = lambda *shape: pltpu.VMEM(shape, bf)
    dma = lambda *shape: pltpu.SemaphoreType.DMA(shape)
    scratch = [
        vmem(own, x_local * ny, nz), vmem(3, chans, chans), vmem(3, kz, chans), vmem(4, 1, chans),
        table(size, size), table(size, size), table(size, size), table(size, size),
        table(tiles * LANES, mtiles * LANES), table(tiles * LANES, mtiles * LANES),
        table(mtiles * LANES, tiles * LANES), table(mtiles * LANES, tiles * LANES),
        table(2 * nx * 8, nx * 8), table(2 * nx * 8, nx * 8),
        vmem(sub8, 2, nx * 8, LANES), vmem(sub8, 2, ltile + 1, 8, LANES), vmem(chans, kz), vmem(chans, kz),
        vmem(wide, parts, x_local, own, LANES), vmem(wide, x_local, parts, own, LANES), vmem(x_local, own, LANES),
        vmem(parts, x_local, chans, LANES), vmem(x_local, parts, chans, LANES),
        vmem(tiles, nx, chain, LANES), vmem(sub8, mtiles, nx * 8, LANES),
        vmem(wide, nx, chain, LANES), vmem(nx, chain, LANES), vmem(n_sub, wide, chain // 2, LANES),
        vmem(x_local, chans, LANES), vmem(count, chain // 2, LANES), vmem(count, 8, LANES), vmem(6, chans, LANES),
        dma(xchunks), dma(10), dma(tiles + 2), dma(xchunks, wide), dma(xchunks, wide), dma(hchunks, wide),
        dma(hchunks, wide), dma(tiles, n_sub), dma(tiles, n_sub), dma(count), dma(count), dma(count), dma(count),
        dma(count), dma(count),
    ]
    any_spec = pl.BlockSpec(memory_space=pl.ANY)
    line = lambda v: v.reshape(1, chans)
    result = pl.pallas_call(
        functools.partial(fused_kernel, (n_sp, n_sub, n_rep, kz)),
        out_shape=pltpu.VMEM((chans, x_local * y_local, nz), f32),
        in_specs=[any_spec] * 11,
        out_specs=pl.BlockSpec(memory_space=pltpu.VMEM),
        scratch_shapes=scratch,
        compiler_params=pltpu.CompilerParams(
            collective_id=0, has_side_effects=True, vmem_limit_bytes=VMEM_LIMIT
        ),
        name="fused",
    )(
        field.reshape(own, x_local * ny, nz), mix_weight, w_in, w_out, factor_x.T, factor_y.T, factor_z.T,
        line(norm_gain), line(norm_bias), line(b_in), line(b_out),
    )
    return result.reshape(chans, x_local, y_local, nz)


VMEM_LIMIT = 55 * 1024 * 1024


def fits(field, factor_x, factor_y, factor_z):
    n_sub, wide = lax.axis_size("sub"), lax.axis_size(WIDE)
    own, x_local, ny, nz = field.shape
    nx, kz = x_local * n_sub, factor_z.shape[1]
    power = all(v & (v - 1) == 0 for v in (nx, ny, nz, kz))
    if not power or nz != LANES or factor_x.shape[1] != nx or factor_y.shape[1] != ny or ny % wide:
        return False
    y_local = ny // wide
    return (
        kz * y_local == LANES
        and nz == 4 * kz
        and nx == kz == ny
        and own % (16 * n_sub) == 0
        and lax.axis_size("sp") > 1
        and own % (own * wide // GROUPS) == 0
        and 2 * x_local * y_local <= LANES
        and x_local % 4 == 0
        and (kz // 2 * ny) % LANES == 0
    )


def local(
    field, mix_weight, factor_x, factor_y, factor_z, norm_gain, norm_bias, w_in, b_in, w_out, b_out
):
    run = fused if fits(field, factor_x, factor_y, factor_z) else general
    return run(
        field, mix_weight, factor_x, factor_y, factor_z, norm_gain, norm_bias, w_in, b_in, w_out, b_out
    )


def solution(mesh):
    placed = (P(("grp", "sp", "rep"), "sub", None, None),) + (P(),) * 10
    return jax.shard_map(
        local,
        mesh=mesh,
        in_specs=placed,
        out_specs=P("grp", "sub", ("sp", "rep"), None),
        check_vma=False,
    )
```

```python
import math
import functools

import jax
import jax.numpy as jnp
from jax import lax
from jax.experimental import pallas as pl
from jax.experimental.pallas import tpu as pltpu
from jax.sharding import PartitionSpec as P

GROUPS = 32
HIGH = lax.Precision.HIGH
WIDE = ("sp", "rep")


def trig(length, freq, positions):
    phases = (freq[:, None] * positions[None, :]) % length
    angles = 2.0 * math.pi / length * phases.astype(jnp.float32)
    return jnp.cos(angles), jnp.sin(angles)


def kron_pair(cos_a, sin_a, cos_b, sin_b):
    ca, sa = cos_a.T[:, None, :, None], sin_a.T[:, None, :, None]
    cb, sb = cos_b.T[None, :, None, :], sin_b.T[None, :, None, :]
    return ca * cb - sa * sb, sa * cb + ca * sb


def split(value):
    high = value.astype(jnp.bfloat16)
    low = (value - high.astype(jnp.float32)).astype(jnp.bfloat16)
    return high, low


def dot3(left, right):
    lh, ll = left
    rh, rl = right
    d = functools.partial(jnp.dot, preferred_element_type=jnp.float32)
    return d(lh, rh) + (d(lh, rl) + d(ll, rh))


def sum_kernel(
    sizes, field_ref, modes_ref, table_ref, summed_ref, total_ref, acc1, acc2, held, send_sem, recv_sem
):
    step = pl.program_id(0)
    n_sp, n_sub, n_rep = sizes
    count = n_sp * n_sub * n_rep
    me = (lax.axis_index("sp") * n_sub + lax.axis_index("sub")) * n_rep + lax.axis_index("rep")

    def place(index):
        return {
            "sp": index // (n_sub * n_rep),
            "sub": (index // n_rep) % n_sub,
            "rep": index % n_rep,
        }

    @pl.when(step == 0)
    def _():
        barrier = pltpu.get_barrier_semaphore()

        def greet(k, carry):
            pl.semaphore_signal(
                barrier,
                inc=1,
                device_id=place((me + k) % count),
                device_id_type=pl.DeviceIdType.MESH,
            )
            return carry

        lax.fori_loop(1, count, greet, 0)

    chans, cells, width = field_ref.shape
    rank = modes_ref.shape[2]

    @pl.when(step == 0)
    def _():
        acc1[...] = jnp.zeros_like(acc1)
        acc2[...] = jnp.zeros_like(acc2)

    table = split(table_ref[...])
    chunk = 32 if chans % 32 == 0 else chans

    def body(index, carry):
        rows = pl.ds(pl.multiple_of(index * chunk, chunk), chunk)
        modes = modes_ref[rows].reshape(chunk * cells, rank)
        value = dot3(split(modes), table).reshape(chunk, cells, width) + field_ref[rows]
        summed_ref[rows] = value
        acc1[rows] += value
        acc2[rows] += value * value
        return carry

    lax.fori_loop(0, chans // chunk, body, 0)

    @pl.when(step == pl.num_programs(0) - 1)
    def _():
        def row(acc):
            per = jnp.sum(acc[...], axis=1)
            per = jnp.sum(per.reshape(GROUPS, chans // GROUPS, width), axis=1)
            per = jnp.broadcast_to(jnp.sum(per, axis=1, keepdims=True), (GROUPS, 128))
            lanes = lax.broadcasted_iota(jnp.int32, (GROUPS, 128), 1)
            rows = lax.broadcasted_iota(jnp.int32, (GROUPS, 128), 0)
            return jnp.sum(jnp.where(lanes == rows, per, 0.0), axis=0, keepdims=True)

        tile = lax.broadcasted_iota(jnp.int32, (8, 128), 0)
        held[0] = jnp.where(tile == 0, row(acc1), jnp.where(tile == 1, row(acc2), 0.0))
        pl.semaphore_wait(pltpu.get_barrier_semaphore(), count - 1)

        def copy(k):
            return pltpu.make_async_remote_copy(
                src_ref=held.at[0],
                dst_ref=held.at[k],
                send_sem=send_sem.at[k],
                recv_sem=recv_sem.at[k],
                device_id=place((me + k) % count),
                device_id_type=pl.DeviceIdType.MESH,
            )

        def launch(k, carry):
            copy(k).start()
            return carry

        def finish(k, carry):
            copy(k).wait()
            return carry

        lax.fori_loop(1, count, launch, 0)
        lax.fori_loop(1, count, finish, 0)
        total_ref[...] = jnp.sum(held[...], axis=0)


def mlp_kernel(summed_ref, vec_ref, w_in_ref, w_out_ref, out_ref):
    cells = summed_ref.shape[1]
    w_in = split(w_in_ref[...])
    w_out = split(w_out_ref[...])
    vec = vec_ref[...]
    mean, scale, bias = vec[:, 0:1], vec[:, 1:2], vec[:, 2:3]
    b_in, b_out = vec[:, 3:4], vec[:, 4:5]
    pair = 2 if cells % 2 == 0 else 1
    for start in range(0, cells, pair):
        parts = [summed_ref[:, p, :] for p in range(start, start + pair)]
        value = jnp.concatenate(parts, axis=1) if pair > 1 else parts[0]
        normed = (value - mean) * scale + bias
        hidden = dot3(w_in, split(normed)) + b_in
        inner = math.sqrt(2.0 / math.pi) * (hidden + 0.044715 * (hidden * hidden * hidden))
        hidden = hidden * (0.5 * (1.0 + jnp.tanh(inner)))
        result = value + dot3(w_out, split(hidden)) + b_out
        width = summed_ref.shape[2]
        for k in range(pair):
            out_ref[:, start + k, :] = result[:, k * width : (k + 1) * width]


def general(
    field, mix_weight, factor_x, factor_y, factor_z, norm_gain, norm_bias, w_in, b_in, w_out, b_out
):
    wide_count = lax.axis_size(WIDE)
    narrow_count = lax.axis_size("sub")
    own_chans, x_local, ny, nz = field.shape
    chans = own_chans * wide_count
    nx = x_local * narrow_count
    kx, ky, kz = factor_x.shape[1], factor_y.shape[1], factor_z.shape[1]
    y_local = ny // wide_count
    half = kz // 2
    kept = half + 1
    me_sub = lax.axis_index("sub")
    cells = x_local * y_local

    spatial = field.reshape(own_chans, x_local, wide_count, y_local, nz)
    spatial = spatial.transpose(2, 0, 1, 3, 4).reshape(wide_count, own_chans, cells, nz)
    spatial = lax.all_to_all(spatial, WIDE, split_axis=0, concat_axis=0, tiled=True)

    cos_z, sin_z = trig(nz, jnp.arange(kept), jnp.arange(nz))
    forward = jnp.concatenate([cos_z, -sin_z]) / nz
    planes = jnp.einsum("rz,cxyz->rcxy", forward, field, precision=HIGH)
    planes = planes.reshape(2 * kept * own_chans, x_local * ny)

    def freqs(length, count):
        index = jnp.arange(count)
        return jnp.where(index < count // 2, index, length - count + index)

    cos_y, sin_y = trig(ny, freqs(ny, ky), jnp.arange(ny))

    def forward_xy(values, owner):
        cos_x, sin_x = trig(nx, freqs(nx, kx), owner * x_local + jnp.arange(x_local))
        c, s = kron_pair(cos_x, sin_x, cos_y, sin_y)
        c = (c / (nx * ny)).reshape(x_local * ny, kx * ky)
        s = (s / (nx * ny)).reshape(x_local * ny, kx * ky)
        a = jnp.dot(values, jnp.concatenate([c, s], axis=1), precision=HIGH)
        a = a.reshape(2, kept * own_chans, 2, kx * ky)
        return a[0, :, 0] + a[1, :, 1], a[1, :, 0] - a[0, :, 1]

    held = planes
    real, imag = forward_xy(held, me_sub)
    for hop in range(1, narrow_count):
        held = lax.ppermute(held, "sub", [(i, (i + 1) % narrow_count) for i in range(narrow_count)])
        owner = (me_sub - hop + narrow_count) % narrow_count
        more_real, more_imag = forward_xy(held, owner)
        real, imag = real + more_real, imag + more_imag

    start = lax.axis_index(WIDE) * own_chans
    fx = lax.dynamic_slice_in_dim(factor_x, start, own_chans, 0)
    fy = lax.dynamic_slice_in_dim(factor_y, start, own_chans, 0)
    fz = lax.dynamic_slice_in_dim(factor_z, start, own_chans, 0)
    mirror_x = (-jnp.arange(kx)) % kx
    mirror_y = (-jnp.arange(ky)) % ky
    plane_a = (fx[:, :, None] * fy[:, None, :]).reshape(own_chans, kx * ky)
    plane_b = (fx[:, mirror_x][:, :, None] * fy[:, mirror_y][:, None, :]).reshape(own_chans, kx * ky)
    zero = jnp.zeros((own_chans, 1), jnp.float32)
    z_plus = jnp.concatenate([fz[:, :half], zero], axis=1).T
    z_minus = jnp.concatenate([zero, fz[:, half:][:, ::-1]], axis=1).T
    weight = z_plus[:, :, None] * plane_a[None] + z_minus[:, :, None] * plane_b[None]
    weight = weight.reshape(kept * own_chans, kx * ky)
    real, imag = real * weight, imag * weight

    cos_x, sin_x = trig(nx, freqs(nx, kx), me_sub * x_local + jnp.arange(x_local))
    c, s = kron_pair(cos_x, sin_x, cos_y, sin_y)

    def columns(t):
        t = t.reshape(x_local, wide_count, y_local, kx * ky)
        return t.transpose(3, 1, 0, 2).reshape(kx * ky, wide_count * cells)

    c, s = columns(c), columns(s)
    table_re = jnp.concatenate([c, -s])
    table_im = jnp.concatenate([s, c])
    both = jnp.concatenate([real, imag], axis=1)
    back = jnp.stack(
        [jnp.dot(both, table_re, precision=HIGH), jnp.dot(both, table_im, precision=HIGH)]
    )
    back = back.reshape(2 * kept, own_chans, wide_count, cells)
    back = back.transpose(2, 1, 0, 3).reshape(wide_count * own_chans, 2 * kept * cells)
    back, spatial = lax.optimization_barrier((back, spatial))
    back = lax.all_to_all(back, WIDE, split_axis=0, concat_axis=0, tiled=True)
    back = back.reshape(chans, 2 * kept, cells)
    mixed = jnp.einsum("oi,irp->opr", mix_weight, back, precision=HIGH)

    inverse_z = jnp.concatenate([cos_z, -sin_z])
    spatial = spatial.reshape(chans, cells, nz)
    block = 8 if cells % 8 == 0 else cells
    steps = cells // block
    cube = pl.BlockSpec((chans, block, nz), lambda i: (0, i, 0))
    whole = lambda *shape: pl.BlockSpec(shape, lambda i: (0,) * len(shape))
    sizes = (lax.axis_size("sp"), narrow_count, lax.axis_size("rep"))
    count = sizes[0] * sizes[1] * sizes[2]
    summed, stats = pl.pallas_call(
        functools.partial(sum_kernel, sizes),
        grid=(steps,),
        out_shape=(
            jax.ShapeDtypeStruct(spatial.shape, jnp.float32),
            jax.ShapeDtypeStruct((8, 128), jnp.float32),
        ),
        in_specs=[
            cube,
            pl.BlockSpec((chans, block, 2 * kept), lambda i: (0, i, 0)),
            whole(2 * kept, nz),
        ],
        out_specs=(cube, whole(8, 128)),
        scratch_shapes=[pltpu.VMEM((chans, block, nz), jnp.float32)] * 2
        + [
            pltpu.VMEM((count, 8, 128), jnp.float32),
            pltpu.SemaphoreType.DMA((count,)),
            pltpu.SemaphoreType.DMA((count,)),
        ],
        compiler_params=pltpu.CompilerParams(collective_id=0, has_side_effects=True),
        name="sum_stats",
    )(spatial, mixed, inverse_z)

    size = chans // GROUPS
    stats = stats[:2, :GROUPS]
    cells_group = size * nx * ny * nz
    group_mean = stats[0] / cells_group
    group_var = stats[1] / cells_group - group_mean * group_mean
    scale = jnp.repeat(lax.rsqrt(group_var + 1e-05), size) * norm_gain
    mean = jnp.repeat(group_mean, size)
    vec = jnp.stack([mean, scale, norm_bias, b_in, b_out] + [b_out] * 3, axis=1)

    result = pl.pallas_call(
        mlp_kernel,
        grid=(steps,),
        out_shape=jax.ShapeDtypeStruct(spatial.shape, jnp.float32),
        in_specs=[cube, whole(chans, 8), whole(*w_in.shape), whole(*w_out.shape)],
        out_specs=cube,
        name="mlp",
    )(summed, vec, w_in, w_out)
    return result.reshape(chans, x_local, y_local, nz)


MESH = pl.DeviceIdType.MESH
LANES = 128
AHEAD = 4
PUMP = 4


def cosine(index, length):
    fold = jnp.abs(index.astype(jnp.float32) * (2.0 / length) - 1.0)
    near = jnp.minimum(fold, 1.0 - fold) * math.pi
    square = near * near
    total = jnp.full_like(square, 1.0 / math.factorial(14))
    for power in range(6, -1, -1):
        term = 1.0 / math.factorial(2 * power)
        total = term - square * total
    return jnp.where(fold > 0.5, total, -total)


def log2(value):
    return value.bit_length() - 1


def split3(value):
    high = value.astype(jnp.bfloat16)
    rest = value - high.astype(jnp.float32)
    mid = rest.astype(jnp.bfloat16)
    low = (rest - mid.astype(jnp.float32)).astype(jnp.bfloat16)
    return high, mid, low


def pick(left, right):
    d = functools.partial(jnp.dot, preferred_element_type=jnp.float32)
    a, b, c = split3(right)
    return d(left, a) + (d(left, b) + d(left, c))


def pick_right(left, right):
    d = functools.partial(jnp.dot, preferred_element_type=jnp.float32)
    a, b, c = split3(left)
    return d(a, right) + (d(b, right) + d(c, right))


def iota(shape, axis):
    return lax.broadcasted_iota(jnp.int32, shape, axis)


def fused_kernel(
    dims,
    field_ref, mix_ref, w_in_ref, w_out_ref, fx_ref, fy_ref, fz_ref, gain_ref, bias_ref, b_in_ref, b_out_ref,
    out_ref,
    fld, mats, facs, vecs, g_hi, g_lo, gi_hi, gi_lo, yf_hi, yf_lo, yi_hi, yi_lo, xt_hi, xt_lo, fxs, uv, fy_t, fz_t,
    se, sh, lf, re, rh, pin, mid, bs, lb, ls, rb, rl, held, cols,
    fld_sem, par_sem, own_sem, e_send, e_recv, h_send, h_recv, x_send, x_recv, b_send, b_recv, l_send, l_recv,
    t_send, t_recv,
):
    n_sp, n_sub, n_rep, n_freq = dims
    wide = n_sp * n_rep
    count = wide * n_sub
    own, xy_rows, nz = field_ref.shape
    chans = own * wide
    parts, x_local, _, _ = se.shape[1:]
    y_local = LANES // (nz // (2 * parts))
    width = LANES // y_local
    nx = pin.shape[1]
    ny = xy_rows // x_local
    kz = n_freq
    half = kz // 2
    chain = own // n_sub
    sub8 = chain // 8
    tiles = wide + 1
    ltile = half * ny // LANES
    per_tile = LANES // ny
    lane_y, lane_n = log2(y_local), log2(ny)

    me_sub = lax.axis_index("sub")
    me_sp, me_rep = lax.axis_index("sp"), lax.axis_index("rep")
    me_wide = me_sp * n_rep + me_rep
    me = me_wide * n_sub + me_sub

    def place(w, s):
        return {"sp": w // n_rep, "sub": s, "rep": w % n_rep}

    def place_flat(index):
        return place(index // n_sub, index % n_sub)

    def wide_peer(k):
        return (me_sp + k // n_rep) % n_sp * n_rep + (me_rep + k % n_rep) % n_rep

    def flat_peer(k):
        w = (me_sp + k // (n_rep * n_sub)) % n_sp * n_rep + (me_rep + k % n_rep) % n_rep
        return w, (me_sub + k // n_rep % n_sub) % n_sub

    def turn(i, n):
        near = n // n_sp
        late = i // (n - near)
        far = near + (i + near * (n_sp // 2 - 1)) % (n - near)
        return (1 - late) * far + late * (n - 1 - i)

    def loop(n, body):
        def step(i, carry):
            body(i)
            return carry

        lax.fori_loop(0, n, step, 0)

    barrier = pltpu.get_barrier_semaphore()

    def greet(k, carry):
        pl.semaphore_signal(barrier, inc=1, device_id=place_flat((me + k) % count), device_id_type=MESH)
        return carry

    lax.fori_loop(1, count, greet, 0)

    xchunks = fld_sem.shape[0]
    xc_size = x_local // xchunks

    def fetch(i):
        rows = pl.ds(i * (xc_size * ny), xc_size * ny)
        return pltpu.make_async_copy(field_ref.at[:, rows], fld.at[:, rows], fld_sem.at[i])

    fetch(0).start()
    params = [(mix_ref, mats.at[0]), (w_in_ref, mats.at[1]), (w_out_ref, mats.at[2])]
    params += [(fx_ref, facs.at[0]), (fy_ref, facs.at[1]), (fz_ref, facs.at[2])]
    params += [(gain_ref, vecs.at[0]), (bias_ref, vecs.at[1]), (b_in_ref, vecs.at[2]), (b_out_ref, vecs.at[3])]
    param_copies = [pltpu.make_async_copy(a, b, par_sem.at[i]) for i, (a, b) in enumerate(params)]
    def coef(j):
        low_k = jnp.where(j == 1, half, j >> 1)
        low_s = jnp.where(j == 1, 0, j & 1)
        high_k = (j + 1) >> 1
        high_s = 1 - (j & 1)
        return jnp.where(j < kz, low_k, high_k), jnp.where(j < kz, low_s, high_s)

    def basis(j, z):
        k, s = coef(j)
        value = cosine((k * z + s * (3 * nz // 4)) & (nz - 1), nz)
        edge = (k == 0) | (k == nz // 2)
        return value * jnp.where(edge, math.sqrt(1.0 / nz), math.sqrt(2.0 / nz))

    def g_entry(rows, columns):
        y_in, z = rows >> log2(nz), rows & (nz - 1)
        j, y_out = columns >> lane_y, columns & (y_local - 1)
        return jnp.where(y_in == y_out, basis(j, z), 0.0)

    size = nz * y_local
    stepr = LANES

    def build_g(i):
        rows = pl.ds(pl.multiple_of(i * stepr, stepr), stepr)
        a = iota((stepr, size), 0) + i * stepr
        b = iota((stepr, size), 1)
        g_hi[rows], g_lo[rows] = split(g_entry(a, b))

    def build_back(i):
        rows = pl.ds(pl.multiple_of(i * stepr, stepr), stepr)
        a = iota((stepr, size), 0) + i * stepr
        b = iota((stepr, size), 1)
        gi_hi[rows], gi_lo[rows] = split(g_entry(b, a))

    loop(size // stepr, build_g)

    lane = iota((1, LANES), 1)

    def e_copy(xc, k):
        w = wide_peer(k)
        xs = pl.ds(xc * xc_size, xc_size)
        return pltpu.make_async_remote_copy(
            src_ref=se.at[w, :, xs],
            dst_ref=re.at[:, xs, pl.ds(pl.multiple_of(me_wide * own, own), own)],
            send_sem=e_send.at[xc, k],
            recv_sem=e_recv.at[xc, k],
            device_id=place(w, me_sub),
            device_id_type=MESH,
        )

    hchunks = h_send.shape[0]
    hc_size = x_local // hchunks

    def h_copy(hc, k):
        w = wide_peer(k)
        xs = pl.ds(hc * hc_size, hc_size)
        return pltpu.make_async_remote_copy(
            src_ref=sh.at[w, xs],
            dst_ref=rh.at[xs, :, pl.ds(pl.multiple_of(me_wide * own, own), own)],
            send_sem=h_send.at[hc, k],
            recv_sem=h_recv.at[hc, k],
            device_id=place(w, me_sub),
            device_id_type=MESH,
        )

    def peers(make, what, n=wide):
        def step(i, carry):
            getattr(make(turn(i, n)), what)()
            return carry

        lax.fori_loop(0, n - 1, step, 0)

    zero = jnp.zeros((own, LANES), jnp.float32)

    def transform(xc, squares):
        fetch(xc).wait()

        @pl.when(xc + 1 < xchunks)
        def _():
            fetch(xc + 1).start()


        def one(i, carry):
            left, sq = carry
            d = wide_peer(turn(i, wide))
            groups = []
            for xi in range(xc_size):
                row = (xc * xc_size + xi) * ny + d * y_local
                groups.append(jnp.concatenate([fld[:, row + y, :] for y in range(y_local)], axis=1))
            value = jnp.concatenate(groups, axis=0)
            res = dot3(split(value), (g_hi[...], g_lo[...]))
            cube = res.reshape(xc_size, own, size)
            xs = pl.ds(xc * xc_size, xc_size)
            for g in range(parts):
                se[d, g, xs] = cube[:, :, g * LANES : (g + 1) * LANES]
                part = cube[:, :, (parts + g) * LANES : (parts + g + 1) * LANES]
                sh[d, xs, g] = part
                sq = sq + jnp.sum(part * part, axis=0)
            more = pltpu.roll(res[:, LANES : 2 * LANES], d * y_local, axis=1)
            left = jnp.where((lane >> lane_y) == d, more, left)

            @pl.when(jnp.logical_and(xc == 0, i == 1))
            def _():
                pl.semaphore_wait(barrier, count - 1)

            @pl.when(i >= 1)
            def _():
                e_copy(xc, turn(i - 1, wide)).start()

            return left, sq

        left = jnp.zeros((xc_size * own, LANES), jnp.float32)
        left, squares = lax.fori_loop(0, wide, one, (left, squares))
        lf[pl.ds(xc * xc_size, xc_size)] = left.reshape(xc_size, own, LANES)

        return squares

    squares = lax.fori_loop(0, xchunks, transform, zero)
    for copy in param_copies:
        copy.start()

    def x_src(t, s):
        cs = pl.ds(pl.multiple_of(s * chain, 8), chain)
        return se.at[t, 0, :, cs] if t < wide else lf.at[:, cs]

    def x_dst(t):
        return pin.at[t, pl.ds(me_sub * x_local, x_local)]

    x_copies = []
    for t in range(tiles):
        for k in range(1, n_sub):
            s = (me_sub + k) % n_sub
            x_copies.append(
                pltpu.make_async_remote_copy(
                    src_ref=x_src(t, s),
                    dst_ref=x_dst(t),
                    send_sem=x_send.at[t, k],
                    recv_sem=x_recv.at[t, k],
                    device_id=place(me_wide, s),
                    device_id_type=MESH,
                )
            )
    own_chan = pl.ds(pl.multiple_of(me_wide * own, own), own)
    own_copies = [pltpu.make_async_copy(x_src(t, me_sub), x_dst(t), own_sem.at[t]) for t in range(tiles)]
    own_copies.append(pltpu.make_async_copy(se.at[me_wide], re.at[:, :, own_chan], own_sem.at[tiles]))
    own_copies.append(pltpu.make_async_copy(sh.at[me_wide], rh.at[:, :, own_chan], own_sem.at[tiles + 1]))

    def p_meta(t, r):
        jj = r >> lane_y
        k = jnp.where(jj == 1, half, jj >> 1)
        s = jnp.where(jj == 1, 0, jj & 1)
        y = t * y_local + (r & (y_local - 1))
        rest = t == wide
        k = jnp.where(rest, jnp.where(r < ny, half, -1), k)
        return k, jnp.where(rest, 1, s), jnp.where(rest, r, y)

    def m_meta(t, c):
        part = jnp.where(t >= ltile, 1, 0)
        k = (t - part * ltile) * per_tile + (c >> lane_n)
        rest = t == 2 * ltile
        seat = c & (LANES // 2 - 1)
        k = jnp.where(rest, jnp.where(seat < ny, half, -2), k)
        part = jnp.where(rest, c >> log2(LANES // 2), part)
        return k, part, c & (ny - 1)

    def y_entry(pt, mt, p, m, forward):
        kp, s, y = p_meta(pt, p)
        km, part, b = m_meta(mt, m)
        value = cosine((y * b + (ny // 4) * (s + part)) & (ny - 1), ny)
        scale = jnp.where(km == 0, math.sqrt(nz), math.sqrt(nz / 2.0))
        if forward:
            scale = scale * (1.0 / nz)
        return jnp.where(kp == km, value * scale, 0.0)

    square = (LANES, LANES)
    mtiles = 2 * ltile + 1

    def build_y(i):
        rows = pl.ds(pl.multiple_of(i * LANES, LANES), LANES)
        for t in range(mtiles):
            cut = slice(t * LANES, (t + 1) * LANES)
            a, b = iota(square, 0), iota(square, 1)
            yf_hi[rows, cut], yf_lo[rows, cut] = split(y_entry(i, t, a, b, True))
            yi_hi[rows, cut], yi_lo[rows, cut] = split(y_entry(t, i, b, a, False))

    def build_x(i):
        shape = (LANES, nx * 8)
        row = iota(shape, 0) + i * LANES
        col = iota(shape, 1)
        part = row >> log2(nx * 8)
        a = (row >> 3) & (nx - 1)
        value = cosine(((a * (col >> 3)) + part * (3 * nx // 4)) & (nx - 1), nx)
        value = jnp.where((row & 7) == (col & 7), value, 0.0)
        rows = pl.ds(pl.multiple_of(i * LANES, LANES), LANES)
        xt_hi[rows], xt_lo[rows] = split(value)

    loop(2 * nx * 8 // LANES, build_x)
    for copy in x_copies:
        copy.start()
    for copy in own_copies:
        copy.start()
    loop(tiles, build_y)
    loop(size // stepr, build_back)

    for copy in param_copies:
        copy.wait()
    fy_t[...] = jnp.transpose(facs[1])
    fz_t[...] = jnp.transpose(facs[2])
    first = me_wide * own + me_sub * chain
    bf = jnp.bfloat16
    one_hot = lambda mask: jnp.where(mask, 1.0, 0.0).astype(bf)
    for h in range(sub8):
        base = pl.multiple_of(first + 8 * h, 8)
        a = iota((nx * 8, nx), 0) >> 3
        b = iota((nx * 8, nx), 1)
        mask = iota((nx * 8, chans), 1) == first + 8 * h + (iota((nx * 8, chans), 0) & 7)
        for sign in range(2):
            want = a if sign == 0 else (nx - a) & (nx - 1)
            spread = pick(one_hot(b == want), facs[0])
            column = jnp.sum(jnp.where(mask, spread, 0.0), axis=1, keepdims=True)
            fxs[h, sign] = jnp.broadcast_to(column * (1.0 / (nx * ny)), (nx * 8, LANES))
        fz8, fy8 = fz_t[pl.ds(base, 8), :], fy_t[pl.ds(base, 8), :]
        for t in range(ltile + 1):
            i = iota((kz, LANES), 0)
            seat = iota((kz, LANES), 1)
            k = t * per_tile + (seat >> lane_n) if t < ltile else half
            bb = seat & (ny - 1)
            plus = one_hot(i == (k if t < ltile else -1))
            minus = one_hot((i == kz - k) & (k > 0)) if t < ltile else one_hot(i == half)
            yp, ym = one_hot(i == bb), one_hot(i == ((ny - bb) & (ny - 1)))
            uv[h, 0, t] = pick_right(fz8, plus) * pick_right(fy8, yp)
            uv[h, 1, t] = pick_right(fz8, minus) * pick_right(fy8, ym)

    for copy in own_copies:
        copy.wait()
    for copy in x_copies:
        copy.wait()

    rows8 = nx * 8

    def forward_y(h):
        cs = pl.ds(pl.multiple_of(h * 8, 8), 8)
        value = jnp.concatenate([pin[t, :, cs, :].reshape(rows8, LANES) for t in range(tiles)], axis=1)
        res = dot3(split(value), (yf_hi[...], yf_lo[...]))
        for t in range(mtiles):
            mid[h, t] = res[:, t * LANES : (t + 1) * LANES]

    loop(sub8, forward_y)

    def weights(h, t):
        u = jnp.broadcast_to(uv[h, 0, t][None], (nx, 8, LANES)).reshape(rows8, LANES)
        v = jnp.broadcast_to(uv[h, 1, t][None], (nx, 8, LANES)).reshape(rows8, LANES)
        return fxs[h, 0] * u + fxs[h, 1] * v

    def along_x(value):
        return dot3((xt_hi[...], xt_lo[...]), split(value))

    def pair_x(i):
        h, t = i // ltile, i % ltile
        res = along_x(jnp.concatenate([mid[h, t], mid[h, ltile + t]], axis=1))
        c_re, c_im = res[:rows8, :LANES], res[:rows8, LANES:]
        s_re, s_im = res[rows8:, :LANES], res[rows8:, LANES:]
        w = weights(h, t)
        res = along_x(jnp.concatenate([(c_re + s_im) * w, (c_im - s_re) * w], axis=1))
        c_re, c_im = res[:rows8, :LANES], res[:rows8, LANES:]
        s_re, s_im = res[rows8:, :LANES], res[rows8:, LANES:]
        mid[h, t] = c_re - s_im
        mid[h, ltile + t] = c_im + s_re

    loop(sub8 * ltile, pair_x)

    def rest_x(h):
        sign = jnp.where(lane < LANES // 2, 1.0, -1.0)
        res = along_x(mid[h, 2 * ltile])
        modes = res[:rows8] + sign * pltpu.roll(res[rows8:], LANES // 2, axis=1)
        res = along_x(modes * weights(h, ltile))
        mid[h, 2 * ltile] = res[:rows8] - sign * pltpu.roll(res[rows8:], LANES // 2, axis=1)

    loop(sub8, rest_x)

    def back_y(h):
        cs = pl.ds(pl.multiple_of(h * 8, 8), 8)
        value = jnp.concatenate([mid[h, t] for t in range(mtiles)], axis=1)
        res = dot3(split(value), (yi_hi[...], yi_lo[...]))
        for t in range(tiles):
            cut = res[:, t * LANES : (t + 1) * LANES].reshape(nx, 8, LANES)
            if t < wide:
                bs[t, :, cs, :] = cut
            else:
                lb[:, cs, :] = cut

    loop(sub8, back_y)

    def gather_rest(s):
        def one(x, carry):
            value = lb[s * x_local + x]
            new = []
            for d in range(wide):
                moved = pltpu.roll(value, ((x - d) * y_local + LANES) & (LANES - 1), axis=1)
                new.append(jnp.where((lane >> lane_y) == x, moved, carry[d]))
            return tuple(new)

        start = tuple(jnp.zeros((chain, LANES), jnp.float32) for _ in range(wide))
        done = lax.fori_loop(0, x_local, one, start)
        for d in range(wide):
            other = pltpu.roll(done[d][chain // 2 :], LANES // 2, axis=1)
            ls[s, d] = jnp.where(lane < LANES // 2, done[d][: chain // 2], other)

    loop(n_sub, gather_rest)

    b_rows = pl.ds(pl.multiple_of(first, 8), chain)

    def b_copy(k):
        w, s = flat_peer(k)
        return pltpu.make_async_remote_copy(
            src_ref=bs.at[w, pl.ds(s * x_local, x_local)],
            dst_ref=rb.at[:, b_rows],
            send_sem=b_send.at[k],
            recv_sem=b_recv.at[k],
            device_id=place(w, s),
            device_id_type=MESH,
        )

    def l_copy(k):
        w, s = flat_peer(k)
        return pltpu.make_async_remote_copy(
            src_ref=ls.at[s, w],
            dst_ref=rl.at[me],
            send_sem=l_send.at[k],
            recv_sem=l_recv.at[k],
            device_id=place(w, s),
            device_id_type=MESH,
        )

    peers(b_copy, "start", count)
    own_b = pltpu.make_async_copy(bs.at[me_wide, pl.ds(me_sub * x_local, x_local)], rb.at[:, b_rows], b_send.at[0])
    own_l = pltpu.make_async_copy(ls.at[me_sub, me_wide], rl.at[me], l_send.at[0])
    own_b.start()
    own_l.start()
    peers(l_copy, "start", count)
    loop(AHEAD, lambda hc: peers(lambda k: h_copy(hc, k), "start"))

    eye = iota((chans, chans), 0) == iota((chans, chans), 1)
    for i in range(4):
        column = jnp.sum(jnp.where(eye, vecs[i], 0.0), axis=1, keepdims=True)
        cols[i] = jnp.broadcast_to(column, (chans, LANES))

    own_b.wait()
    own_l.wait()
    peers(b_copy, "wait", count)
    peers(l_copy, "wait", count)
    loop(xchunks, lambda xc: peers(lambda k: e_copy(xc, k), "wait"))
    mix = split(mats[0])
    packed = rl[...].reshape(chans // 2, LANES)
    other = pltpu.roll(packed, LANES // 2, axis=1).reshape(rl.shape)
    rest = jnp.concatenate([rl[...], other], axis=1).reshape(chans, LANES)
    rest = dot3(mix, split(rest))
    lows = lane < y_local
    blank = jnp.zeros((chans, LANES), jnp.float32)

    def low(i, carry):
        one, two = carry
        spectral = dot3(mix, split(jnp.concatenate([rb[2 * i], rb[2 * i + 1]], axis=1)))
        for j in range(2):
            x = 2 * i + j
            value = re[0, x] + spectral[:, j * LANES : (j + 1) * LANES]
            re[0, x] = value
            one = one + jnp.where(lows, value, 0.0)
            two = two + value * value
            moved = pltpu.roll(rest, (LANES - x * y_local) & (LANES - 1), axis=1)
            value = re[1, x] + jnp.where(lows, moved, 0.0)
            re[1, x] = value
            two = two + value * value
        return one, two

    one, two = lax.fori_loop(0, x_local // 2, low, (blank, blank))

    per_group = chans // GROUPS

    def row(acc, base):
        groups = acc.shape[0] // per_group
        per = jnp.sum(acc.reshape(groups, per_group, LANES), axis=1)
        per = jnp.broadcast_to(jnp.sum(per, axis=1, keepdims=True), (groups, LANES))
        seat = iota((groups, LANES), 1) == iota((groups, LANES), 0) + base
        return jnp.sum(jnp.where(seat, per, 0.0), axis=0, keepdims=True)

    tile = iota((8, LANES), 0)
    sum_one = row(one, 0) * math.sqrt(nz)
    sum_two = row(two, 0) + row(squares, me_wide * (own // per_group))
    held[0] = jnp.where(tile == 0, sum_one, jnp.where(tile == 1, sum_two, 0.0))

    def t_copy(k):
        return pltpu.make_async_remote_copy(
            src_ref=held.at[0],
            dst_ref=held.at[k],
            send_sem=t_send.at[k],
            recv_sem=t_recv.at[k],
            device_id=place(*flat_peer(k)),
            device_id_type=MESH,
        )

    def arrive(hc):
        peers(lambda k: h_copy(hc, k), "wait")

        @pl.when(hc + AHEAD < hchunks)
        def _():
            peers(lambda k: h_copy(hc + AHEAD, k), "start")

    peers(t_copy, "start", count)
    loop(PUMP, arrive)
    peers(t_copy, "wait", count)
    total = jnp.sum(held[...], axis=0)
    cells_group = per_group * nx * ny * nz
    group_mean = total[0:1] / cells_group
    group_var = total[1:2] / cells_group - group_mean * group_mean
    group_scale = lax.rsqrt(group_var + 1e-05)
    seat = iota((chans, LANES), 1) == iota((chans, LANES), 0) // per_group

    def column_of(value):
        return jnp.sum(jnp.where(seat, value, 0.0), axis=1, keepdims=True)

    scale = column_of(group_scale) * cols[0, :, 0:1]
    shift = cols[1, :, 0:1] - column_of(group_mean) * scale
    cols[4] = jnp.broadcast_to(scale, (chans, LANES))
    cols[5] = jnp.broadcast_to(shift, (chans, LANES))

    def late(hc, carry):
        pl.when(hc >= PUMP)(functools.partial(arrive, hc))
        w_in, w_out = split(mats[1]), split(mats[2])
        factor, offset = cols[4, :, 0:1], cols[5, :, 0:1]
        b_in, b_out = cols[2, :, 0:1], cols[3, :, 0:1]
        for j in range(hc_size):
            x = hc * hc_size + j
            value = jnp.concatenate([re[g, x] for g in range(parts)] + [rh[x, g] for g in range(parts)], axis=1)
            value = dot3(split(value), (gi_hi[...], gi_lo[...]))
            normed = value * factor + offset
            hidden = dot3(w_in, split(normed)) + b_in
            inner = math.sqrt(2.0 / math.pi) * (hidden + 0.044715 * (hidden * hidden * hidden))
            hidden = hidden * (0.5 * (1.0 + jnp.tanh(inner)))
            result = value + dot3(w_out, split(hidden)) + b_out
            for y in range(y_local):
                out_ref[:, x * y_local + y, :] = result[:, y * nz : (y + 1) * nz]
        return carry

    lax.fori_loop(0, hchunks, late, 0)


def fused(
    field, mix_weight, factor_x, factor_y, factor_z, norm_gain, norm_bias, w_in, b_in, w_out, b_out
):
    n_sp, n_sub, n_rep = (lax.axis_size(a) for a in ("sp", "sub", "rep"))
    wide, count = n_sp * n_rep, n_sp * n_rep * n_sub
    own, x_local, ny, nz = field.shape
    chans, nx, y_local = own * wide, x_local * n_sub, ny // wide
    kz = factor_z.shape[1]
    chain = own // n_sub
    sub8 = chain // 8
    tiles = wide + 1
    ltile = kz // 2 * ny // LANES
    mtiles = 2 * ltile + 1
    parts = nz * y_local // LANES // 2
    size = nz * y_local
    xchunks, hchunks = 4, x_local
    f32, bf = jnp.float32, jnp.bfloat16
    vmem = lambda *shape: pltpu.VMEM(shape, f32)
    table = lambda *shape: pltpu.VMEM(shape, bf)
    dma = lambda *shape: pltpu.SemaphoreType.DMA(shape)
    scratch = [
        vmem(own, x_local * ny, nz), vmem(3, chans, chans), vmem(3, kz, chans), vmem(4, 1, chans),
        table(size, size), table(size, size), table(size, size), table(size, size),
        table(tiles * LANES, mtiles * LANES), table(tiles * LANES, mtiles * LANES),
        table(mtiles * LANES, tiles * LANES), table(mtiles * LANES, tiles * LANES),
        table(2 * nx * 8, nx * 8), table(2 * nx * 8, nx * 8),
        vmem(sub8, 2, nx * 8, LANES), vmem(sub8, 2, ltile + 1, 8, LANES), vmem(chans, kz), vmem(chans, kz),
        vmem(wide, parts, x_local, own, LANES), vmem(wide, x_local, parts, own, LANES), vmem(x_local, own, LANES),
        vmem(parts, x_local, chans, LANES), vmem(x_local, parts, chans, LANES),
        vmem(tiles, nx, chain, LANES), vmem(sub8, mtiles, nx * 8, LANES),
        vmem(wide, nx, chain, LANES), vmem(nx, chain, LANES), vmem(n_sub, wide, chain // 2, LANES),
        vmem(x_local, chans, LANES), vmem(count, chain // 2, LANES), vmem(count, 8, LANES), vmem(6, chans, LANES),
        dma(xchunks), dma(10), dma(tiles + 2), dma(xchunks, wide), dma(xchunks, wide), dma(hchunks, wide),
        dma(hchunks, wide), dma(tiles, n_sub), dma(tiles, n_sub), dma(count), dma(count), dma(count), dma(count),
        dma(count), dma(count),
    ]
    any_spec = pl.BlockSpec(memory_space=pl.ANY)
    line = lambda v: v.reshape(1, chans)
    result = pl.pallas_call(
        functools.partial(fused_kernel, (n_sp, n_sub, n_rep, kz)),
        out_shape=pltpu.VMEM((chans, x_local * y_local, nz), f32),
        in_specs=[any_spec] * 11,
        out_specs=pl.BlockSpec(memory_space=pltpu.VMEM),
        scratch_shapes=scratch,
        compiler_params=pltpu.CompilerParams(
            collective_id=0, has_side_effects=True, vmem_limit_bytes=VMEM_LIMIT
        ),
        name="fused",
    )(
        field.reshape(own, x_local * ny, nz), mix_weight, w_in, w_out, factor_x.T, factor_y.T, factor_z.T,
        line(norm_gain), line(norm_bias), line(b_in), line(b_out),
    )
    return result.reshape(chans, x_local, y_local, nz)


VMEM_LIMIT = 55 * 1024 * 1024


def fits(field, factor_x, factor_y, factor_z):
    n_sub, wide = lax.axis_size("sub"), lax.axis_size(WIDE)
    own, x_local, ny, nz = field.shape
    nx, kz = x_local * n_sub, factor_z.shape[1]
    power = all(v & (v - 1) == 0 for v in (nx, ny, nz, kz))
    if not power or nz != LANES or factor_x.shape[1] != nx or factor_y.shape[1] != ny or ny % wide:
        return False
    y_local = ny // wide
    return (
        kz * y_local == LANES
        and nz == 4 * kz
        and nx == kz == ny
        and own % (16 * n_sub) == 0
        and lax.axis_size("sp") > 1
        and own % (own * wide // GROUPS) == 0
        and 2 * x_local * y_local <= LANES
        and x_local % 4 == 0
        and (kz // 2 * ny) % LANES == 0
    )


def local(
    field, mix_weight, factor_x, factor_y, factor_z, norm_gain, norm_bias, w_in, b_in, w_out, b_out
):
    run = fused if fits(field, factor_x, factor_y, factor_z) else general
    return run(
        field, mix_weight, factor_x, factor_y, factor_z, norm_gain, norm_bias, w_in, b_in, w_out, b_out
    )


def solution(mesh):
    placed = (P(("grp", "sp", "rep"), "sub", None, None),) + (P(),) * 10
    return jax.shard_map(
        local,
        mesh=mesh,
        in_specs=placed,
        out_specs=P("grp", "sub", ("sp", "rep"), None),
        check_vma=False,
    )
```
